32 devices in a mesh: boxes: 32 (over z, y, x, core).
Axes of the slice: x: 2, y: 2, z: 4, core: 2. Of those that a mesh axis runs over, the one named last changes fastest.
Arguments:
- conserved: float32 [32, 5, 16, 32, 128], P('boxes'), may hold values from -6 to 6
- volume_fraction: float32 [32, 16, 32, 128], P('boxes'), may hold values from 0.05 to 1
- cut_mask: int32 [32, 16, 32, 128], P('boxes'), may hold values 0 or 1
- merge_code: int32 [32, 16, 32, 128], P('boxes'), may hold values from 0 to 26
Outputs:
- redistributed: float32 [32, 5, 16, 32, 128], P('boxes')
The draws below stay inside these ranges and needn't reach their ends.
All inputs are finite; a program needn't handle non-finite values. No bound on the sum of `cut_mask` on one device may be relied on, other than what follows from the above.
Results may differ from the reference program's by a relative error of at most 0.0003.
Values sent between devices are 32-bit elements; how exact they have to be, the bound alone decides.
No kernel may reach another device: no remote copies, remote signals or barrier semaphores. Data moves between devices by JAX's collectives and lax.ppermute only.
A program may use at most 64 MiB of HBM per device.

```python
import math
import jax
import jax.numpy as jnp
from jax import lax

FIELDS = 5
CX = 16
CY = 32
CZ = 128
NBY = 4
NBZ = 4
NBOXES = 32
NBX = 2
NX = 32
NY = 128
NZ = 512


def plant(array, stream_key, least, high):
    shape = array.shape
    spot = [jax.random.randint(jax.random.fold_in(stream_key, axis), (), 0, shape[axis]) for axis in range(len(shape))]
    array = array.at[tuple(spot)].set(least)
    longest = shape.index(max(shape))
    spot[longest] = (spot[longest] + 1) % shape[longest]
    return array.at[tuple(spot)].set(high)


def levels(key, dims, split, least, high):
    loudness, own = 1.0, jax.random.fold_in(key, 6)
    for dim, parts in split:
        steps = jnp.exp(jax.random.uniform(jax.random.fold_in(own, dim), (parts,), jnp.float32, least / len(split), high / len(split)))
        loudness = loudness * jnp.repeat(steps, dims[dim] // parts).reshape([-1 if axis == dim else 1 for axis in range(len(dims))])
    return loudness


def bell_draw(key, shape, width, limit, cuts=(), held_as=jnp.bfloat16):
    gain = levels(key, shape, cuts, -0.22, 0.18) if cuts else 1.0
    array = jax.random.normal(key, shape, jnp.float32) * width * gain
    return jnp.minimum(jnp.maximum(array, -limit), limit).astype(held_as)


def setup_inputs(seed: int = 0) -> dict:
    arg_keys = jax.random.split(jax.random.key(seed), 5)
    return {
        "conserved": bell_draw(arg_keys[0], (NBOXES, FIELDS, CX, CY, CZ), 1.0, 6.0, ((0, 32),), jnp.float32),
        "volume_fraction": jnp.clip(jnp.exp(math.log(1.0) - 2.9957323 * jax.random.uniform(arg_keys[1], (NBOXES, CX, CY, CZ), jnp.float32) ** levels(arg_keys[1], (NBOXES, CX, CY, CZ), ((0, 32),), -0.2, 0.2)), 0.05, 1.0),
        "cut_mask": plant((jax.random.randint(arg_keys[2], (NBOXES, CX, CY, CZ), 0, 2) < 1).astype(jnp.int32), jax.random.fold_in(arg_keys[2], 1), 0, 1),
        "merge_code": plant(jax.random.randint(arg_keys[3], (NBOXES, CX, CY, CZ), 0, 27), jax.random.fold_in(arg_keys[3], 1), 0, 26).astype(jnp.int32),
    }


OFFSETS = [(first, second, third) for first in (-1, 0, 1) for second in (-1, 0, 1) for third in (-1, 0, 1) if (first, second, third) != (0, 0, 0)]


def decode(code_field):
    sign_parts = (code_field // 9 - 1, (code_field // 3) % 3 - 1, code_field % 3 - 1)
    members = []
    for offset in OFFSETS:
        inside = jnp.ones(code_field.shape, jnp.bool_)
        for direction, component in zip(sign_parts, offset):
            if component != 0:
                inside = inside & (direction == component)
        members.append(inside)
    return members


def placed(values, offset):
    spread = [(0, 0)] * (values.ndim - 3) + [(1 + component, 1 - component) for component in offset]
    return jnp.pad(values, spread)


def count_members(members):
    running = placed(jnp.ones(members[0].shape, jnp.float32), (0, 0, 0))
    for offset, inside in zip(OFFSETS, members):
        running = running + placed(inside.astype(jnp.float32), offset)
    return running


def window(weighted, offset, interior):
    starts = [0] + [1 + component for component in offset]
    limits = [weighted.shape[0]] + [anchor + extent for anchor, extent in zip(starts[1:], interior)]
    return lax.slice(weighted, starts, limits)


def neighbour_average(weighted, members):
    interior = [extent - 2 for extent in weighted.shape[1:]]
    running = window(weighted, (0, 0, 0), interior)
    for offset, inside in zip(OFFSETS, members):
        running = running + jnp.where(inside[None], window(weighted, offset, interior), 0.0)
    return running[1:] / running[0:1]


def spread_back(average, members):
    running = placed(average, (0, 0, 0))
    for offset, inside in zip(OFFSETS, members):
        running = running + placed(jnp.where(inside[None], average, 0.0), offset)
    return running


def to_grid(boxed):
    channels = boxed.shape[1]
    shaped = boxed.reshape(NBX, NBY, NBZ, channels, CX, CY, CZ)
    return shaped.transpose(3, 0, 4, 1, 5, 2, 6).reshape(channels, NX, NY, NZ)


def from_grid(gridded):
    channels = gridded.shape[0]
    shaped = gridded.reshape(channels, NBX, CX, NBY, CY, NBZ, CZ)
    return shaped.transpose(1, 3, 5, 0, 2, 4, 6).reshape(NBOXES, channels, CX, CY, CZ)


def reference(conserved, volume_fraction, cut_mask, merge_code):
    fields = to_grid(conserved)
    fraction = to_grid(volume_fraction[:, None])[0]
    code_field = jnp.where(to_grid(cut_mask[:, None])[0] == 1, to_grid(merge_code[:, None])[0], 13)
    members = decode(code_field)
    counts = count_members(members)[1:-1, 1:-1, 1:-1]
    weight = fraction / counts
    weighted = jnp.concatenate([weight[None], weight[None] * fields], axis=0)
    weighted = jnp.pad(weighted, ((0, 0), (1, 1), (1, 1), (1, 1)))
    average = neighbour_average(weighted, members)
    gathered = spread_back(average, members)[:, 1:-1, 1:-1, 1:-1]
    return from_grid(gathered / counts[None])
```

```python
import functools

import jax
import jax.numpy as jnp
from jax import lax
from jax.experimental import pallas as pl
from jax.experimental.pallas import tpu as pltpu
from jax.sharding import PartitionSpec as P

NBY = 4
NBZ = 4
AXIS = "boxes"

NFIELD = 5
VF = 5
C1 = 6
C2 = 7
NF = 8
ZU, ZD, YU, YD, XU, XD = 16, 256, 4, 4096, 1 << 28, 1 << 29
LOW = (1 << 24) - 1
EDGE = 13.0


def pairing(stride, extent, devices, odd):
    pairs = []
    for i in range(devices):
        c = i // stride % extent
        partner = ((c + 1) ^ 1) - 1 if odd else c ^ 1
        pairs.append((i, i + (partner % extent - c) * stride))
    return pairs


def lanes_of(shape):
    return lax.broadcasted_iota(jnp.int32, shape, len(shape) - 1)


def roll(value, shift, axis=1):
    if isinstance(shift, int):
        shift %= value.shape[axis]
        if shift == 0:
            return value
    return pltpu.roll(value, shift, axis)


def place():
    me = lax.axis_index(AXIS)
    return me // (NBY * NBZ), me // NBZ % NBY, me % NBZ


def pack_kernel(cx, cy, two_x, u, vf, mask, code, zp, y_a, y_b, *xs):
    bx, by, bz = place()
    lane = lanes_of((cy, 128))
    slot = ((lane + 1) & 127) >> 1
    low_lane = (lane & 1) == 0

    def codes(rows):
        return jnp.where(mask[rows, :] == 1, code[rows, :], 13).astype(jnp.float32)

    for g in range(2):
        acc = jnp.zeros((cy, 128), jnp.float32)
        for k in range(4):
            f = 4 * g + k
            for x in range(cx):
                m = cx * k + x
                rows = pl.ds(x * cy, cy)
                if f < NFIELD:
                    part = roll(u[pl.ds((f * cx + x) * cy, cy), :], 2 * m)
                elif f == VF:
                    part = roll(vf[rows, :], 2 * m)
                elif f == C1:
                    part = roll(codes(rows), 2 * m)
                else:
                    c = codes(rows)
                    part = jnp.where(low_lane, roll(c, 2 * m - 1), roll(c, 2 * m + 1))
                acc = jnp.where(slot == m, part, acc)
        zp[g * cy : (g + 1) * cy, :] = acc

    def y_face(out, high):
        rim = jnp.where(high, cy - 1, 0)
        second = jnp.where(high, cy - 2, 1)

        def column(ref, base, row):
            return ref[pl.ds(base + row, cx, stride=cy), :]

        def code_column(row):
            return jnp.where(column(mask, 0, row) == 1, column(code, 0, row), 13).astype(jnp.float32)

        for f in range(NFIELD):
            out[f * cx : (f + 1) * cx, :] = column(u, f * cx * cy, rim)
        out[VF * cx : (VF + 1) * cx, :] = column(vf, 0, rim)
        out[C1 * cx : (C1 + 1) * cx, :] = code_column(rim)
        out[C2 * cx : (C2 + 1) * cx, :] = code_column(second)

    y_face(y_a, by % 2 == 0)
    y_face(y_b, by % 2 == 1)

    def x_face(out, high):
        rim = jnp.where(high, cx - 1, 0) * cy
        second = jnp.where(high, cx - 2, 1) * cy

        def rows(base, start):
            return pl.ds(pl.multiple_of(base + start, 8), cy)

        for f in range(NFIELD):
            out[f * cy : (f + 1) * cy, :] = u[rows(f * cx * cy, rim), :]
        out[VF * cy : (VF + 1) * cy, :] = vf[rows(0, rim), :]
        out[C1 * cy : (C1 + 1) * cy, :] = codes(rows(0, rim))
        out[C2 * cy : (C2 + 1) * cy, :] = codes(rows(0, second))

    x_face(xs[0], bx % 2 == 0)
    if two_x:
        x_face(xs[1], bx % 2 == 1)


def z_merge_kernel(cx, cy, r_a, r_b, ya_in, yb_in, zh, y_a, y_b):
    bx, by, bz = place()
    odd = bz % 2 == 1
    lane = lanes_of((cy, 128))
    low_lane = (lane & 1) == 0
    codes = (lane >= 63) & (lane <= 126)
    for g in range(2):
        rows = slice(g * cy, (g + 1) * cy)
        a, b = r_a[rows, :], r_b[rows, :]
        edge = jnp.where(codes, EDGE, 0.0) if g else jnp.zeros((cy, 128), jnp.float32)
        low = jnp.where(bz > 0, roll(jnp.where(odd, a, b), 1), edge)
        high = jnp.where(bz < NBZ - 1, roll(jnp.where(odd, b, a), -1), edge)
        zh[rows, :] = jnp.where(low_lane, low, high)
    n = NF * cx

    def finish(out, main, high):
        out[:n, :] = main[...]
        rim = jnp.where(high, cy - 1, 0)
        second = jnp.where(high, cy - 2, 1)
        for g in range(2):
            out[n + 2 * g : n + 2 * g + 1, :] = zh[pl.ds(g * cy + rim, 1), :]
            out[n + 2 * g + 1 : n + 2 * g + 2, :] = zh[pl.ds(g * cy + second, 1), :]
        out[n + 4 : n + 8, :] = jnp.zeros((4, 128), jnp.float32)

    finish(y_a, ya_in, by % 2 == 0)
    finish(y_b, yb_in, by % 2 == 1)


def z_edge_rows(cx):
    n = NF * cx
    row = lax.broadcasted_iota(jnp.int32, (n + 8, 128), 0)
    lane = lanes_of((n + 8, 128))
    codes = ((row >= C1 * cx) & (row < n)) | ((row >= n + 2) & (lane >= 63) & (lane <= 126))
    return jnp.where(codes, EDGE, 0.0)


def y_merge_kernel(cx, cy, two_x, r_a, r_b, zh, y_lo, y_hi, *xs):
    bx, by, bz = place()
    odd = by % 2 == 1
    edge = z_edge_rows(cx)
    a, b = r_a[...], r_b[...]
    y_lo[...] = jnp.where(by > 0, jnp.where(odd, a, b), edge)
    y_hi[...] = jnp.where(by < NBY - 1, jnp.where(odd, b, a), edge)
    n = NF * cx

    def x_rim(out, high):
        rim = jnp.where(high, cx - 1, 0)
        second = jnp.where(high, cx - 2, 1)
        out[: 2 * cy, :] = zh[...]
        at = 2 * cy
        for y in (y_lo, y_hi):
            out[at : at + 4, :] = y[n : n + 4, :]
            at += 4
        for y in (y_lo, y_hi):
            for f in range(NF):
                out[at : at + 1, :] = y[pl.ds(f * cx + rim, 1), :]
                at += 1
            for f in (C1, C2):
                out[at : at + 1, :] = y[pl.ds(f * cx + second, 1), :]
                at += 1
        out[at:, :] = jnp.zeros((out.shape[0] - at, 128), jnp.float32)

    x_rim(xs[0], bx % 2 == 0)
    if two_x:
        x_rim(xs[1], bx % 2 == 1)


def decode(code):
    qx = (code * 57) >> 9
    rest = code - 9 * qx
    qy = (rest * 11) >> 5
    qz = rest - 3 * qy
    word = 1 + jnp.where(qz == 2, ZU, 0) + jnp.where(qz == 0, ZD, 0)
    word = word * jnp.where(qy == 2, 1 + YU, jnp.where(qy == 0, 1 + YD, 1))
    return word | jnp.where(qx == 2, XU, jnp.where(qx == 0, XD, 0))


def on(word, bits):
    return (word & bits) == bits


def ring_store(ref, lead, value):
    n = value.shape[0]
    ref[(*lead, slice(8, 8 + n), slice(None))] = value
    ref[(*lead, slice(0, 8), slice(None))] = value[n - 8 :]
    ref[(*lead, slice(8 + n, 16 + n), slice(None))] = value[:8]


def main_kernel(
    cx, cy, nbx, u, vf, mask, code, zh, y_lo, y_hi, xa, xb, sa, sb, out,
    cw, ht, hz, zf, ow, tmp_i, tmp_f, i1, zw, zi, h0, hm, hp, rc, av, dz,
):
    bx, by, bz = place()
    x_odd = bx % 2 == 1
    has_lo, has_hi = bx > 0, bx < nbx - 1
    n = NF * cx
    rows = cy + 8
    tiles = rows // 8
    tile_lane = lanes_of((8, 128))
    lane = lanes_of((rows, 128))
    first_lane, last_lane = lane == 0, lane == 127
    even = (lane & 1) == 0

    def lower(a, b):
        return jnp.where(x_odd, a, b)

    def upper(a, b):
        return jnp.where(x_odd, b, a)

    def x_raw(f, side):
        part = slice(f * cy, (f + 1) * cy)
        edge = EDGE if f >= C1 else 0.0
        if side == 0:
            return jnp.where(has_lo, lower(xa[part, :], xb[part, :]), edge)
        return jnp.where(has_hi, upper(xa[part, :], xb[part, :]), edge)

    ht[...] = jnp.zeros(ht.shape, jnp.float32)
    at = 2 * cy + 8
    for f in range(C2):
        for x in range(cx):
            ht[f, x + 2, 0:1, :] = y_hi[f * cx + x : f * cx + x + 1, :]
            ht[f, x + 2, 7:8, :] = y_lo[f * cx + x : f * cx + x + 1, :]
    for x in range(cx):
        ht[C1, x + 2, 1:2, :] = y_hi[C2 * cx + x : C2 * cx + x + 1, :]
        ht[C1, x + 2, 6:7, :] = y_lo[C2 * cx + x : C2 * cx + x + 1, :]
    for side, layer, second in ((0, 1, 0), (1, cx + 2, cx + 3)):
        present = has_lo if side == 0 else has_hi
        pick = lower if side == 0 else upper
        for y, row1, row2 in ((0, 7, 6), (1, 0, 1)):

            def rim(i, base=at + 10 * y, pick=pick, present=present, edge=0.0):
                return jnp.where(present, pick(sa[base + i : base + i + 1, :], sb[base + i : base + i + 1, :]), edge)

            for f in range(C1):
                ht[f, layer, row1 : row1 + 1, :] = rim(f)
            ht[C1, layer, row1 : row1 + 1, :] = rim(C1, edge=EDGE)
            ht[C1, layer, row2 : row2 + 1, :] = rim(C2, edge=EDGE)
            ht[C1, second, row1 : row1 + 1, :] = rim(NF, edge=EDGE)
            ht[C1, second, row2 : row2 + 1, :] = rim(NF + 1, edge=EDGE)

    def words(own, layer):
        both = jnp.concatenate([own, ht[C1, layer].astype(jnp.int32)], axis=0)
        ring_store(cw, (layer,), decode(both))

    def own_words(x, _):
        part = pl.ds(pl.multiple_of(x * cy, 8), cy)
        words(jnp.where(mask[part, :] == 1, code[part, :], 13), x + 2)
        return 0

    lax.fori_loop(0, cx, own_words, 0)
    words(x_raw(C2, 0).astype(jnp.int32), 0)
    words(x_raw(C1, 0).astype(jnp.int32), 1)
    words(x_raw(C1, 1).astype(jnp.int32), cx + 2)
    words(x_raw(C2, 1).astype(jnp.int32), cx + 3)

    zrow = 2 * cy
    for g in range(2):
        for i, row in enumerate((0, 1)):
            hz[0, g, row : row + 1, :] = y_hi[n + 2 * g + i : n + 2 * g + i + 1, :]
            hz[0, g, 7 - row : 8 - row, :] = y_lo[n + 2 * g + i : n + 2 * g + i + 1, :]
            for side, pick in ((1, lower), (2, upper)):
                hi, lo = zrow + 4 + 2 * g + i, zrow + 2 * g + i
                hz[side, g, row : row + 1, :] = pick(sa[hi : hi + 1, :], sb[hi : hi + 1, :])
                hz[side, g, 7 - row : 8 - row, :] = pick(sa[lo : lo + 1, :], sb[lo : lo + 1, :])
    below = (lane == 127) | (lane <= 2)
    above = (lane >= 2 * cx + 3) & (lane <= 2 * cx + 6)
    for f in range(NF):
        g, k = f // 4, f % 4
        part = slice(g * cy, (g + 1) * cy)
        edge = EDGE if f >= C1 else 0.0
        own = jnp.concatenate([zh[part, :], hz[0, g]], axis=0)
        lo = jnp.concatenate([lower(sa[part, :], sb[part, :]), hz[1, g]], axis=0)
        hi = jnp.concatenate([upper(sa[part, :], sb[part, :]), hz[2, g]], axis=0)
        base = 4 - 2 * cx * k
        lo = jnp.where(has_lo, roll(lo, base - 2 * cx), edge)
        hi = jnp.where(has_hi, roll(hi, base + 2 * cx), edge)
        zf[f] = jnp.where(below, lo, jnp.where(above, hi, roll(own, base)))

    def lane_pair(layer):
        return (lane == 2 * layer) | (lane == 2 * layer - 1) | ((lane == 127) & (layer == 0))

    def collect(layer, acc):
        return jnp.where(lane_pair(layer), roll(cw[layer, 8 : 8 + rows, :], 2 * layer), acc)

    inner = lax.fori_loop(0, cx + 4, collect, jnp.ones((rows, 128), jnp.int32))
    outer1 = decode(zf[C1].astype(jnp.int32))
    outer2 = decode(zf[C2].astype(jnp.int32))
    ring_store(ow, (), outer1)
    inward = jnp.where(even, ZU, ZD)
    outward = jnp.where(even, ZD, ZU)

    def spread_counts(planes):
        mid = up = down = jnp.zeros((rows, 128), jnp.int32)
        for word, bits in planes:
            v = 1 + ((word & YU) << 6) + ((word & YD) << 4)
            if bits is not None:
                v = jnp.where((word & bits) != 0, v, 0)
            mid = mid + v
            up = up + jnp.where((word & XU) != 0, v, 0)
            down = down + jnp.where((word & XD) != 0, v, 0)
        total = mid + roll(up, 2) + roll(down, -2)
        ring_store(tmp_i, (), total)
        before, after = tmp_i[7 : 7 + rows, :], tmp_i[9 : 9 + rows, :]
        return (total & 255) + ((before >> 8) & 255) + ((after >> 16) & 255)

    z_count = spread_counts(((outer1, None), (outer2, inward), (inner, outward)))
    i1[...] = spread_counts(((outer1, inward),))
    z_weight = zf[VF] / z_count.astype(jnp.float32)
    zw[0] = z_weight
    for f in range(NFIELD):
        zw[f + 1] = z_weight * zf[f]

    zi[...] = jnp.zeros(zi.shape, jnp.float32)

    def weigh(layer, field):
        mid, left, right = (cw[layer + d, 8 : 8 + rows, :] for d in (0, -1, 1))
        total = (mid & LOW) + jnp.where((left & XU) != 0, left & LOW, 0) + jnp.where((right & XD) != 0, right & LOW, 0)
        ring_store(tmp_i, (), total)
        before, after = tmp_i[7 : 7 + rows, :], tmp_i[9 : 9 + rows, :]
        total = (total & 0x333) + ((before >> 2) & 0x333) + ((after >> 12) & 0x333)
        back = 128 - 2 * layer
        extra = roll(i1[...], back)
        count = (total & 15) + jnp.where(first_lane, extra, (roll(total, 1) >> 4) & 15)
        count = count + jnp.where(last_lane, extra, (roll(total, -1) >> 8) & 15)
        inverse = 1.0 / count.astype(jnp.float32)
        rc[layer] = inverse[:cy]
        weight = field(VF) * inverse
        pair = lane_pair(layer)
        for f in range(NFIELD + 1):
            w = weight * field(f - 1) if f else weight
            halo = roll(zw[f], back)
            ring_store(h0, (f, layer), w)
            ring_store(hm, (f, layer), w + jnp.where(first_lane, halo, roll(w, 1)))
            ring_store(hp, (f, layer), w + jnp.where(last_lane, halo, roll(w, -1)))
            zi[f] = jnp.where(pair, roll(w, 2 * layer), zi[f])

    def own_field(x, f):
        base = (f * cx + x if f < NFIELD else x) * cy
        ref = u if f < NFIELD else vf
        return jnp.concatenate([ref[pl.ds(pl.multiple_of(base, 8), cy), :], ht[f, x + 2]], axis=0)

    def own_weigh(x, _):
        weigh(x + 2, functools.partial(own_field, x))
        return 0

    lax.fori_loop(0, cx, own_weigh, 0)
    weigh(1, lambda f: jnp.concatenate([x_raw(f, 0), ht[f, 1]], axis=0))
    weigh(cx + 2, lambda f: jnp.concatenate([x_raw(f, 1), ht[f, cx + 2]], axis=0))

    word = ow[8 : 8 + rows, :]
    sums = []
    for f in range(NFIELD + 1):
        ring_store(tmp_f, (), zw[f] + zi[f])
        mid, before, after = (tmp_f[s : s + rows, :] for s in (8, 7, 9))
        parts = []
        for d in (0, 1, -1):
            m, b, a = (roll(v, -2 * d) for v in (mid, before, after))
            parts.append(m + jnp.where((word & YU) != 0, a, jnp.where((word & YD) != 0, b, 0.0)))
        sums.append(parts[0] + jnp.where((word & XU) != 0, parts[1], jnp.where((word & XD) != 0, parts[2], 0.0)))
    inverse = 1.0 / sums[0]
    for f in range(NFIELD):
        v = jnp.where((word & inward) != 0, sums[f + 1] * inverse, 0.0)
        spread = []
        for bits in (0, YU, YD):
            w = jnp.where((word & bits) != 0, v, 0.0) if bits else v
            up, down = jnp.where((word & XU) != 0, w, 0.0), jnp.where((word & XD) != 0, w, 0.0)
            spread.append(w + roll(up, 2) + roll(down, -2))
        ring_store(tmp_f, (), spread[1])
        total = spread[0] + tmp_f[7 : 7 + rows, :]
        ring_store(tmp_f, (), spread[2])
        dz[f] = total + tmp_f[9 : 9 + rows, :]

    def average(layer, _):
        for t in range(tiles):
            at = 8 + 8 * t
            word = cw[layer, at : at + 8, :]
            zu, zd = (word & ZU) != 0, (word & ZD) != 0
            yu, yd = (word & YU) != 0, (word & YD) != 0
            xu, xd = (word & XU) != 0, (word & XD) != 0
            sums = []
            for f in range(NFIELD + 1):
                parts = []
                for d in (0, 1, -1):
                    line = []
                    for e in (0, 1, -1):
                        at_e = slice(at + e, at + e + 8)
                        v0, vm, vp = (r[f, layer + d, at_e, :] for r in (h0, hm, hp))
                        line.append(jnp.where(zu, vp, jnp.where(zd, vm, v0)))
                    parts.append(line[0] + jnp.where(yu, line[1], jnp.where(yd, line[2], 0.0)))
                sums.append(parts[0] + jnp.where(xu, parts[1], jnp.where(xd, parts[2], 0.0)))
            inverse = 1.0 / sums[0]
            for f in range(NFIELD):
                a = sums[f + 1] * inverse
                av[f, layer, at : at + 8, :] = a
                if t == 0:
                    av[f, layer, 8 + rows : 16 + rows, :] = a
                if t == tiles - 1:
                    av[f, layer, 0:8, :] = a
        return 0

    lax.fori_loop(1, cx + 3, average, 0)

    tile_first, tile_last = tile_lane == 0, tile_lane == 127

    def spread(x, _):
        layer = x + 2
        back = 128 - 2 * layer
        for t in range(tiles - 1):
            at = 8 + 8 * t
            base = [av[f, layer, at : at + 8, :] for f in range(NFIELD)]
            word = cw[layer, at : at + 8, :]
            up = [jnp.where((word & ZU) != 0, a, 0.0) for a in base]
            down = [jnp.where((word & ZD) != 0, a, 0.0) for a in base]
            for d in (0, 1, -1):
                for e in (0, 1, -1):
                    if d == 0 and e == 0:
                        continue
                    at_e = slice(at - e, at - e + 8)
                    word = cw[layer - d, at_e, :]
                    bits = (0, XU, XD)[d] | (0, YU, YD)[e]
                    here = on(word, bits)
                    here_up, here_down = on(word, bits | ZU), on(word, bits | ZD)
                    for f in range(NFIELD):
                        a = av[f, layer - d, at_e, :]
                        base[f] = base[f] + jnp.where(here, a, 0.0)
                        up[f] = up[f] + jnp.where(here_up, a, 0.0)
                        down[f] = down[f] + jnp.where(here_down, a, 0.0)
            inverse = rc[layer, 8 * t : 8 * t + 8, :]
            for f in range(NFIELD):
                halo = roll(dz[f, 8 * t : 8 * t + 8, :], back)
                total = base[f] + jnp.where(tile_first, halo, roll(up[f], 1))
                total = total + jnp.where(tile_last, halo, roll(down[f], -1))
                out[pl.ds(pl.multiple_of((f * cx + x) * cy + 8 * t, 8), 8), :] = total * inverse
        return 0

    lax.fori_loop(0, cx, spread, 0)


def call(kernel, outs, scratch=(), name=None):
    return pl.pallas_call(
        kernel,
        out_shape=tuple(jax.ShapeDtypeStruct(s, jnp.float32) for s in outs),
        scratch_shapes=scratch,
        name=name,
    )


def per_device(conserved, volume_fraction, cut_mask, merge_code):
    _, cx, cy, cz = cut_mask.shape
    devices = lax.axis_size(AXIS)
    nbx = devices // (NBY * NBZ)
    two_x = nbx > 2
    u = conserved.reshape(NFIELD * cx * cy, cz)
    vf, mask, code = (a.reshape(cx * cy, cz) for a in (volume_fraction, cut_mask, merge_code))

    def swap(value, stride, extent, odd):
        return lax.ppermute(value, AXIS, pairing(stride, extent, devices, odd))

    def x_swap(parts):
        got = [swap(p, NBY * NBZ, nbx, odd) for odd, p in enumerate(parts)]
        return got if two_x else got * 2

    n = NF * cx
    face, z_shape, y_shape, x_shape = (n, cz), (2 * cy, cz), (n + 8, cz), (NF * cy, cz)
    rim_shape = (2 * cy + 32, cz)
    copies = 2 if two_x else 1
    zp, ya, yb, *xs = call(
        functools.partial(pack_kernel, cx, cy, two_x), [z_shape, face, face] + [x_shape] * copies, name="pack"
    )(u, vf, mask, code)
    xa, xb = x_swap(xs)
    zh, ya, yb = call(functools.partial(z_merge_kernel, cx, cy), [z_shape, y_shape, y_shape], name="z_merge")(
        swap(zp, 1, NBZ, False), swap(zp, 1, NBZ, True), ya, yb
    )
    y_lo, y_hi, *rims = call(
        functools.partial(y_merge_kernel, cx, cy, two_x), [y_shape, y_shape] + [rim_shape] * copies, name="y_merge"
    )(swap(ya, NBZ, NBY, False), swap(yb, NBZ, NBY, True), zh)
    sa, sb = x_swap(rims)

    rows, ring = cy + 8, cy + 24
    layers = cx + 4
    f32, i32 = jnp.float32, jnp.int32
    scratch = [
        pltpu.VMEM((layers, ring, cz), i32),
        pltpu.VMEM((C2, layers, 8, cz), f32),
        pltpu.VMEM((3, 2, 8, cz), f32),
        pltpu.VMEM((NF, rows, cz), f32),
        pltpu.VMEM((ring, cz), i32),
        pltpu.VMEM((ring, cz), i32),
        pltpu.VMEM((ring, cz), f32),
        pltpu.VMEM((rows, cz), i32),
        pltpu.VMEM((NFIELD + 1, rows, cz), f32),
        pltpu.VMEM((NFIELD + 1, rows, cz), f32),
        pltpu.VMEM((NFIELD + 1, layers, ring, cz), f32),
        pltpu.VMEM((NFIELD + 1, layers, ring, cz), f32),
        pltpu.VMEM((NFIELD + 1, layers, ring, cz), f32),
        pltpu.VMEM((layers, cy, cz), f32),
        pltpu.VMEM((NFIELD, layers, ring, cz), f32),
        pltpu.VMEM((NFIELD, rows, cz), f32),
    ]
    (out,) = call(functools.partial(main_kernel, cx, cy, nbx), [(NFIELD * cx * cy, cz)], scratch, name="redistribute")(
        u, vf, mask, code, zh, y_lo, y_hi, xa, xb, sa, sb
    )
    return out.reshape(conserved.shape)


def solution(mesh):
    return jax.shard_map(
        per_device,
        mesh=mesh,
        in_specs=(
            P(AXIS, None, None, None, None),
            P(AXIS, None, None, None),
            P(AXIS, None, None, None),
            P(AXIS, None, None, None),
        ),
        out_specs=P(AXIS, None, None, None, None),
        check_vma=False,
    )
```

```python
import functools

import jax
import jax.numpy as jnp
from jax import lax
from jax.experimental import pallas as pl
from jax.experimental.pallas import tpu as pltpu
from jax.sharding import PartitionSpec as P

NBY = 4
NBZ = 4
AXIS = "boxes"

NFIELD = 5
VF = 5
C1 = 6
C2 = 7
NF = 8
ZU, ZD, YU, YD, XU, XD = 16, 256, 4, 4096, 1 << 28, 1 << 29
LOW = (1 << 24) - 1
EDGE = 13.0


def pairing(stride, extent, devices, odd):
    pairs = []
    for i in range(devices):
        c = i // stride % extent
        partner = ((c + 1) ^ 1) - 1 if odd else c ^ 1
        pairs.append((i, i + (partner % extent - c) * stride))
    return pairs


def lanes_of(shape):
    return lax.broadcasted_iota(jnp.int32, shape, len(shape) - 1)


def roll(value, shift, axis=1):
    if isinstance(shift, int):
        shift %= value.shape[axis]
        if shift == 0:
            return value
    return pltpu.roll(value, shift, axis)


def place():
    me = lax.axis_index(AXIS)
    return me // (NBY * NBZ), me // NBZ % NBY, me % NBZ


def pack_kernel(cx, cy, two_x, u, vf, mask, code, zp, y_a, y_b, *xs):
    bx, by, bz = place()
    lane = lanes_of((cy, 128))
    slot = ((lane + 1) & 127) >> 1
    low_lane = (lane & 1) == 0

    def codes(rows):
        return jnp.where(mask[rows, :] == 1, code[rows, :], 13).astype(jnp.float32)

    for g in range(2):
        acc = jnp.zeros((cy, 128), jnp.float32)
        for k in range(4):
            f = 4 * g + k
            for x in range(cx):
                m = cx * k + x
                rows = pl.ds(x * cy, cy)
                if f < NFIELD:
                    part = roll(u[pl.ds((f * cx + x) * cy, cy), :], 2 * m)
                elif f == VF:
                    part = roll(vf[rows, :], 2 * m)
                elif f == C1:
                    part = roll(codes(rows), 2 * m)
                else:
                    c = codes(rows)
                    part = jnp.where(low_lane, roll(c, 2 * m - 1), roll(c, 2 * m + 1))
                acc = jnp.where(slot == m, part, acc)
        zp[g * cy : (g + 1) * cy, :] = acc

    def y_face(out, high):
        rim = jnp.where(high, cy - 1, 0)
        second = jnp.where(high, cy - 2, 1)

        def column(ref, base, row):
            return ref[pl.ds(base + row, cx, stride=cy), :]

        def code_column(row):
            return jnp.where(column(mask, 0, row) == 1, column(code, 0, row), 13).astype(jnp.float32)

        for f in range(NFIELD):
            out[f * cx : (f + 1) * cx, :] = column(u, f * cx * cy, rim)
        out[VF * cx : (VF + 1) * cx, :] = column(vf, 0, rim)
        out[C1 * cx : (C1 + 1) * cx, :] = code_column(rim)
        out[C2 * cx : (C2 + 1) * cx, :] = code_column(second)

    y_face(y_a, by % 2 == 0)
    y_face(y_b, by % 2 == 1)

    def x_face(out, high):
        rim = jnp.where(high, cx - 1, 0) * cy
        second = jnp.where(high, cx - 2, 1) * cy

        def rows(base, start):
            return pl.ds(pl.multiple_of(base + start, 8), cy)

        for f in range(NFIELD):
            out[f * cy : (f + 1) * cy, :] = u[rows(f * cx * cy, rim), :]
        out[VF * cy : (VF + 1) * cy, :] = vf[rows(0, rim), :]
        out[C1 * cy : (C1 + 1) * cy, :] = codes(rows(0, rim))
        out[C2 * cy : (C2 + 1) * cy, :] = codes(rows(0, second))

    x_face(xs[0], bx % 2 == 0)
    if two_x:
        x_face(xs[1], bx % 2 == 1)


def z_merge_kernel(cx, cy, r_a, r_b, ya_in, yb_in, zh, y_a, y_b):
    bx, by, bz = place()
    odd = bz % 2 == 1
    lane = lanes_of((cy, 128))
    low_lane = (lane & 1) == 0
    codes = (lane >= 63) & (lane <= 126)
    for g in range(2):
        rows = slice(g * cy, (g + 1) * cy)
        a, b = r_a[rows, :], r_b[rows, :]
        edge = jnp.where(codes, EDGE, 0.0) if g else jnp.zeros((cy, 128), jnp.float32)
        low = jnp.where(bz > 0, roll(jnp.where(odd, a, b), 1), edge)
        high = jnp.where(bz < NBZ - 1, roll(jnp.where(odd, b, a), -1), edge)
        zh[rows, :] = jnp.where(low_lane, low, high)
    n = NF * cx

    def finish(out, main, high):
        out[:n, :] = main[...]
        rim = jnp.where(high, cy - 1, 0)
        second = jnp.where(high, cy - 2, 1)
        for g in range(2):
            out[n + 2 * g : n + 2 * g + 1, :] = zh[pl.ds(g * cy + rim, 1), :]
            out[n + 2 * g + 1 : n + 2 * g + 2, :] = zh[pl.ds(g * cy + second, 1), :]
        out[n + 4 : n + 8, :] = jnp.zeros((4, 128), jnp.float32)

    finish(y_a, ya_in, by % 2 == 0)
    finish(y_b, yb_in, by % 2 == 1)


def z_edge_rows(cx):
    n = NF * cx
    row = lax.broadcasted_iota(jnp.int32, (n + 8, 128), 0)
    lane = lanes_of((n + 8, 128))
    codes = ((row >= C1 * cx) & (row < n)) | ((row >= n + 2) & (lane >= 63) & (lane <= 126))
    return jnp.where(codes, EDGE, 0.0)


def y_merge_kernel(cx, cy, two_x, r_a, r_b, zh, y_lo, y_hi, *xs):
    bx, by, bz = place()
    odd = by % 2 == 1
    edge = z_edge_rows(cx)
    a, b = r_a[...], r_b[...]
    y_lo[...] = jnp.where(by > 0, jnp.where(odd, a, b), edge)
    y_hi[...] = jnp.where(by < NBY - 1, jnp.where(odd, b, a), edge)
    n = NF * cx

    def x_rim(out, high):
        rim = jnp.where(high, cx - 1, 0)
        second = jnp.where(high, cx - 2, 1)
        out[: 2 * cy, :] = zh[...]
        at = 2 * cy
        for y in (y_lo, y_hi):
            out[at : at + 4, :] = y[n : n + 4, :]
            at += 4
        for y in (y_lo, y_hi):
            for f in range(NF):
                out[at : at + 1, :] = y[pl.ds(f * cx + rim, 1), :]
                at += 1
            for f in (C1, C2):
                out[at : at + 1, :] = y[pl.ds(f * cx + second, 1), :]
                at += 1
        out[at:, :] = jnp.zeros((out.shape[0] - at, 128), jnp.float32)

    x_rim(xs[0], bx % 2 == 0)
    if two_x:
        x_rim(xs[1], bx % 2 == 1)


def decode(code):
    qx = (code * 57) >> 9
    rest = code - 9 * qx
    qy = (rest * 11) >> 5
    qz = rest - 3 * qy
    word = 1 + jnp.where(qz == 2, ZU, 0) + jnp.where(qz == 0, ZD, 0)
    word = word * jnp.where(qy == 2, 1 + YU, jnp.where(qy == 0, 1 + YD, 1))
    return word | jnp.where(qx == 2, XU, jnp.where(qx == 0, XD, 0))


def on(word, bits):
    return (word & bits) == bits


def ring_store(ref, lead, value):
    n = value.shape[0]
    ref[(*lead, slice(8, 8 + n), slice(None))] = value
    ref[(*lead, slice(0, 8), slice(None))] = value[n - 8 :]
    ref[(*lead, slice(8 + n, 16 + n), slice(None))] = value[:8]


def main_kernel(
    cx, cy, nbx, u, vf, mask, code, zh, y_lo, y_hi, xa, xb, sa, sb, out,
    cw, ht, hz, zf, ow, tmp_i, tmp_f, i1, zw, zi, h0, hm, hp, rc, av, dz,
):
    bx, by, bz = place()
    x_odd = bx % 2 == 1
    has_lo, has_hi = bx > 0, bx < nbx - 1
    n = NF * cx
    rows = cy + 8
    tiles = rows // 8
    tile_lane = lanes_of((8, 128))
    lane = lanes_of((rows, 128))
    first_lane, last_lane = lane == 0, lane == 127
    even = (lane & 1) == 0

    def lower(a, b):
        return jnp.where(x_odd, a, b)

    def upper(a, b):
        return jnp.where(x_odd, b, a)

    def x_raw(f, side):
        part = slice(f * cy, (f + 1) * cy)
        edge = EDGE if f >= C1 else 0.0
        if side == 0:
            return jnp.where(has_lo, lower(xa[part, :], xb[part, :]), edge)
        return jnp.where(has_hi, upper(xa[part, :], xb[part, :]), edge)

    ht[...] = jnp.zeros(ht.shape, jnp.float32)
    at = 2 * cy + 8
    for f in range(C2):
        for x in range(cx):
            ht[f, x + 2, 0:1, :] = y_hi[f * cx + x : f * cx + x + 1, :]
            ht[f, x + 2, 7:8, :] = y_lo[f * cx + x : f * cx + x + 1, :]
    for x in range(cx):
        ht[C1, x + 2, 1:2, :] = y_hi[C2 * cx + x : C2 * cx + x + 1, :]
        ht[C1, x + 2, 6:7, :] = y_lo[C2 * cx + x : C2 * cx + x + 1, :]
    for side, layer, second in ((0, 1, 0), (1, cx + 2, cx + 3)):
        present = has_lo if side == 0 else has_hi
        pick = lower if side == 0 else upper
        for y, row1, row2 in ((0, 7, 6), (1, 0, 1)):

            def rim(i, base=at + 10 * y, pick=pick, present=present, edge=0.0):
                return jnp.where(present, pick(sa[base + i : base + i + 1, :], sb[base + i : base + i + 1, :]), edge)

            for f in range(C1):
                ht[f, layer, row1 : row1 + 1, :] = rim(f)
            ht[C1, layer, row1 : row1 + 1, :] = rim(C1, edge=EDGE)
            ht[C1, layer, row2 : row2 + 1, :] = rim(C2, edge=EDGE)
            ht[C1, second, row1 : row1 + 1, :] = rim(NF, edge=EDGE)
            ht[C1, second, row2 : row2 + 1, :] = rim(NF + 1, edge=EDGE)

    def words(own, layer):
        both = jnp.concatenate([own, ht[C1, layer].astype(jnp.int32)], axis=0)
        ring_store(cw, (layer,), decode(both))

    def own_words(x, _):
        part = pl.ds(pl.multiple_of(x * cy, 8), cy)
        words(jnp.where(mask[part, :] == 1, code[part, :], 13), x + 2)
        return 0

    lax.fori_loop(0, cx, own_words, 0)
    words(x_raw(C2, 0).astype(jnp.int32), 0)
    words(x_raw(C1, 0).astype(jnp.int32), 1)
    words(x_raw(C1, 1).astype(jnp.int32), cx + 2)
    words(x_raw(C2, 1).astype(jnp.int32), cx + 3)

    zrow = 2 * cy
    for g in range(2):
        for i, row in enumerate((0, 1)):
            hz[0, g, row : row + 1, :] = y_hi[n + 2 * g + i : n + 2 * g + i + 1, :]
            hz[0, g, 7 - row : 8 - row, :] = y_lo[n + 2 * g + i : n + 2 * g + i + 1, :]
            for side, pick in ((1, lower), (2, upper)):
                hi, lo = zrow + 4 + 2 * g + i, zrow + 2 * g + i
                hz[side, g, row : row + 1, :] = pick(sa[hi : hi + 1, :], sb[hi : hi + 1, :])
                hz[side, g, 7 - row : 8 - row, :] = pick(sa[lo : lo + 1, :], sb[lo : lo + 1, :])
    below = (lane == 127) | (lane <= 2)
    above = (lane >= 2 * cx + 3) & (lane <= 2 * cx + 6)
    for f in range(NF):
        g, k = f // 4, f % 4
        part = slice(g * cy, (g + 1) * cy)
        edge = EDGE if f >= C1 else 0.0
        own = jnp.concatenate([zh[part, :], hz[0, g]], axis=0)
        lo = jnp.concatenate([lower(sa[part, :], sb[part, :]), hz[1, g]], axis=0)
        hi = jnp.concatenate([upper(sa[part, :], sb[part, :]), hz[2, g]], axis=0)
        base = 4 - 2 * cx * k
        lo = jnp.where(has_lo, roll(lo, base - 2 * cx), edge)
        hi = jnp.where(has_hi, roll(hi, base + 2 * cx), edge)
        zf[f] = jnp.where(below, lo, jnp.where(above, hi, roll(own, base)))

    def lane_pair(layer):
        return (lane == 2 * layer) | (lane == 2 * layer - 1) | ((lane == 127) & (layer == 0))

    def collect(layer, acc):
        return jnp.where(lane_pair(layer), roll(cw[layer, 8 : 8 + rows, :], 2 * layer), acc)

    inner = lax.fori_loop(0, cx + 4, collect, jnp.ones((rows, 128), jnp.int32))
    outer1 = decode(zf[C1].astype(jnp.int32))
    outer2 = decode(zf[C2].astype(jnp.int32))
    ring_store(ow, (), outer1)
    inward = jnp.where(even, ZU, ZD)
    outward = jnp.where(even, ZD, ZU)

    def spread_counts(planes):
        mid = up = down = jnp.zeros((rows, 128), jnp.int32)
        for word, bits in planes:
            v = 1 + ((word & YU) << 6) + ((word & YD) << 4)
            if bits is not None:
                v = jnp.where((word & bits) != 0, v, 0)
            mid = mid + v
            up = up + jnp.where((word & XU) != 0, v, 0)
            down = down + jnp.where((word & XD) != 0, v, 0)
        total = mid + roll(up, 2) + roll(down, -2)
        ring_store(tmp_i, (), total)
        before, after = tmp_i[7 : 7 + rows, :], tmp_i[9 : 9 + rows, :]
        return (total & 255) + ((before >> 8) & 255) + ((after >> 16) & 255)

    z_count = spread_counts(((outer1, None), (outer2, inward), (inner, outward)))
    i1[...] = spread_counts(((outer1, inward),))
    z_weight = zf[VF] / z_count.astype(jnp.float32)
    zw[0] = z_weight
    for f in range(NFIELD):
        zw[f + 1] = z_weight * zf[f]

    zi[...] = jnp.zeros(zi.shape, jnp.float32)

    def weigh(layer, field):
        mid, left, right = (cw[layer + d, 8 : 8 + rows, :] for d in (0, -1, 1))
        total = (mid & LOW) + jnp.where((left & XU) != 0, left & LOW, 0) + jnp.where((right & XD) != 0, right & LOW, 0)
        ring_store(tmp_i, (), total)
        before, after = tmp_i[7 : 7 + rows, :], tmp_i[9 : 9 + rows, :]
        total = (total & 0x333) + ((before >> 2) & 0x333) + ((after >> 12) & 0x333)
        back = 128 - 2 * layer
        extra = roll(i1[...], back)
        count = (total & 15) + jnp.where(first_lane, extra, (roll(total, 1) >> 4) & 15)
        count = count + jnp.where(last_lane, extra, (roll(total, -1) >> 8) & 15)
        inverse = 1.0 / count.astype(jnp.float32)
        rc[layer] = inverse[:cy]
        weight = field(VF) * inverse
        pair = lane_pair(layer)
        for f in range(NFIELD + 1):
            w = weight * field(f - 1) if f else weight
            halo = roll(zw[f], back)
            ring_store(h0, (f, layer), w)
            ring_store(hm, (f, layer), w + jnp.where(first_lane, halo, roll(w, 1)))
            ring_store(hp, (f, layer), w + jnp.where(last_lane, halo, roll(w, -1)))
            zi[f] = jnp.where(pair, roll(w, 2 * layer), zi[f])

    def own_field(x, f):
        base = (f * cx + x if f < NFIELD else x) * cy
        ref = u if f < NFIELD else vf
        return jnp.concatenate([ref[pl.ds(pl.multiple_of(base, 8), cy), :], ht[f, x + 2]], axis=0)

    def own_weigh(x, _):
        weigh(x + 2, functools.partial(own_field, x))
        return 0

    lax.fori_loop(0, cx, own_weigh, 0)
    weigh(1, lambda f: jnp.concatenate([x_raw(f, 0), ht[f, 1]], axis=0))
    weigh(cx + 2, lambda f: jnp.concatenate([x_raw(f, 1), ht[f, cx + 2]], axis=0))

    word = ow[8 : 8 + rows, :]
    sums = []
    for f in range(NFIELD + 1):
        ring_store(tmp_f, (), zw[f] + zi[f])
        mid, before, after = (tmp_f[s : s + rows, :] for s in (8, 7, 9))
        parts = []
        for d in (0, 1, -1):
            m, b, a = (roll(v, -2 * d) for v in (mid, before, after))
            parts.append(m + jnp.where((word & YU) != 0, a, jnp.where((word & YD) != 0, b, 0.0)))
        sums.append(parts[0] + jnp.where((word & XU) != 0, parts[1], jnp.where((word & XD) != 0, parts[2], 0.0)))
    inverse = 1.0 / sums[0]
    for f in range(NFIELD):
        v = jnp.where((word & inward) != 0, sums[f + 1] * inverse, 0.0)
        spread = []
        for bits in (0, YU, YD):
            w = jnp.where((word & bits) != 0, v, 0.0) if bits else v
            up, down = jnp.where((word & XU) != 0, w, 0.0), jnp.where((word & XD) != 0, w, 0.0)
            spread.append(w + roll(up, 2) + roll(down, -2))
        ring_store(tmp_f, (), spread[1])
        total = spread[0] + tmp_f[7 : 7 + rows, :]
        ring_store(tmp_f, (), spread[2])
        dz[f] = total + tmp_f[9 : 9 + rows, :]

    def average(layer, _):
        for t in range(tiles):
            at = 8 + 8 * t
            word = cw[layer, at : at + 8, :]
            zu, zd = (word & ZU) != 0, (word & ZD) != 0
            yu, yd = (word & YU) != 0, (word & YD) != 0
            xu, xd = (word & XU) != 0, (word & XD) != 0
            sums = []
            for f in range(NFIELD + 1):
                parts = []
                for d in (0, 1, -1):
                    line = []
                    for e in (0, 1, -1):
                        at_e = slice(at + e, at + e + 8)
                        v0, vm, vp = (r[f, layer + d, at_e, :] for r in (h0, hm, hp))
                        line.append(jnp.where(zu, vp, jnp.where(zd, vm, v0)))
                    parts.append(line[0] + jnp.where(yu, line[1], jnp.where(yd, line[2], 0.0)))
                sums.append(parts[0] + jnp.where(xu, parts[1], jnp.where(xd, parts[2], 0.0)))
            inverse = 1.0 / sums[0]
            for f in range(NFIELD):
                a = sums[f + 1] * inverse
                av[f, layer, at : at + 8, :] = a
                if t == 0:
                    av[f, layer, 8 + rows : 16 + rows, :] = a
                if t == tiles - 1:
                    av[f, layer, 0:8, :] = a
        return 0

    lax.fori_loop(1, cx + 3, average, 0)

    tile_first, tile_last = tile_lane == 0, tile_lane == 127

    def spread(x, _):
        layer = x + 2
        back = 128 - 2 * layer
        for t in range(tiles - 1):
            at = 8 + 8 * t
            base = [av[f, layer, at : at + 8, :] for f in range(NFIELD)]
            word = cw[layer, at : at + 8, :]
            up = [jnp.where((word & ZU) != 0, a, 0.0) for a in base]
            down = [jnp.where((word & ZD) != 0, a, 0.0) for a in base]
            for d in (0, 1, -1):
                for e in (0, 1, -1):
                    if d == 0 and e == 0:
                        continue
                    at_e = slice(at - e, at - e + 8)
                    word = cw[layer - d, at_e, :]
                    bits = (0, XU, XD)[d] | (0, YU, YD)[e]
                    here = on(word, bits)
                    here_up, here_down = on(word, bits | ZU), on(word, bits | ZD)
                    for f in range(NFIELD):
                        a = av[f, layer - d, at_e, :]
                        base[f] = base[f] + jnp.where(here, a, 0.0)
                        up[f] = up[f] + jnp.where(here_up, a, 0.0)
                        down[f] = down[f] + jnp.where(here_down, a, 0.0)
            inverse = rc[layer, 8 * t : 8 * t + 8, :]
            for f in range(NFIELD):
                halo = roll(dz[f, 8 * t : 8 * t + 8, :], back)
                total = base[f] + jnp.where(tile_first, halo, roll(up[f], 1))
                total = total + jnp.where(tile_last, halo, roll(down[f], -1))
                out[pl.ds(pl.multiple_of((f * cx + x) * cy + 8 * t, 8), 8), :] = total * inverse
        return 0

    lax.fori_loop(0, cx, spread, 0)


def call(kernel, ins, outs, scratch=(), name=None, grant=8, last=False):
    vmem = pl.BlockSpec(memory_space=pltpu.VMEM)
    return pl.pallas_call(
        kernel,
        in_specs=[vmem] * ins,
        out_specs=tuple([pl.BlockSpec() if last else vmem] * len(outs)),
        out_shape=tuple(
            jax.ShapeDtypeStruct(s, jnp.float32) if last else pltpu.VMEM(s, jnp.float32) for s in outs
        ),
        scratch_shapes=scratch,
        name=name,
        compiler_params=pltpu.CompilerParams(vmem_limit_bytes=grant << 20),
    )


def per_device(conserved, volume_fraction, cut_mask, merge_code):
    _, cx, cy, cz = cut_mask.shape
    devices = lax.axis_size(AXIS)
    nbx = devices // (NBY * NBZ)
    two_x = nbx > 2
    u = conserved.reshape(NFIELD * cx * cy, cz)
    vf, mask, code = (a.reshape(cx * cy, cz) for a in (volume_fraction, cut_mask, merge_code))

    def swap(value, stride, extent, odd):
        return lax.ppermute(value, AXIS, pairing(stride, extent, devices, odd))

    def x_swap(parts):
        got = [swap(p, NBY * NBZ, nbx, odd) for odd, p in enumerate(parts)]
        return got if two_x else got * 2

    n = NF * cx
    face, z_shape, y_shape, x_shape = (n, cz), (2 * cy, cz), (n + 8, cz), (NF * cy, cz)
    rim_shape = (2 * cy + 32, cz)
    copies = 2 if two_x else 1
    zp, ya, yb, *xs = call(
        functools.partial(pack_kernel, cx, cy, two_x), 4, [z_shape, face, face] + [x_shape] * copies, name="pack"
    )(u, vf, mask, code)
    xa, xb = x_swap(xs)
    zh, ya, yb = call(functools.partial(z_merge_kernel, cx, cy), 4, [z_shape, y_shape, y_shape], name="z_merge")(
        swap(zp, 1, NBZ, False), swap(zp, 1, NBZ, True), ya, yb
    )
    y_lo, y_hi, *rims = call(
        functools.partial(y_merge_kernel, cx, cy, two_x), 3, [y_shape, y_shape] + [rim_shape] * copies, name="y_merge"
    )(swap(ya, NBZ, NBY, False), swap(yb, NBZ, NBY, True), zh)
    sa, sb = x_swap(rims)

    rows, ring = cy + 8, cy + 24
    layers = cx + 4
    f32, i32 = jnp.float32, jnp.int32
    scratch = [
        pltpu.VMEM((layers, ring, cz), i32),
        pltpu.VMEM((C2, layers, 8, cz), f32),
        pltpu.VMEM((3, 2, 8, cz), f32),
        pltpu.VMEM((NF, rows, cz), f32),
        pltpu.VMEM((ring, cz), i32),
        pltpu.VMEM((ring, cz), i32),
        pltpu.VMEM((ring, cz), f32),
        pltpu.VMEM((rows, cz), i32),
        pltpu.VMEM((NFIELD + 1, rows, cz), f32),
        pltpu.VMEM((NFIELD + 1, rows, cz), f32),
        pltpu.VMEM((NFIELD + 1, layers, ring, cz), f32),
        pltpu.VMEM((NFIELD + 1, layers, ring, cz), f32),
        pltpu.VMEM((NFIELD + 1, layers, ring, cz), f32),
        pltpu.VMEM((layers, cy, cz), f32),
        pltpu.VMEM((NFIELD, layers, ring, cz), f32),
        pltpu.VMEM((NFIELD, rows, cz), f32),
    ]
    (out,) = call(functools.partial(main_kernel, cx, cy, nbx), 11, [(NFIELD * cx * cy, cz)], scratch, "redistribute", 28, True)(
        u, vf, mask, code, zh, y_lo, y_hi, xa, xb, sa, sb
    )
    return out.reshape(conserved.shape)


def solution(mesh):
    return jax.shard_map(
        per_device,
        mesh=mesh,
        in_specs=(
            P(AXIS, None, None, None, None),
            P(AXIS, None, None, None),
            P(AXIS, None, None, None),
            P(AXIS, None, None, None),
        ),
        out_specs=P(AXIS, None, None, None, None),
        check_vma=False,
    )
```

```python
import functools
import types

import jax
import jax.numpy as jnp
from jax import lax
from jax.experimental import pallas as pl
from jax.experimental.pallas import tpu as pltpu
from jax.sharding import PartitionSpec as P

NBY = 4
NBZ = 4
AXIS = "boxes"

NFIELD = 5
VF = 5
C1 = 6
C2 = 7
NF = 8
ZU, ZD, YU, YD, XU, XD = 16, 256, 4, 4096, 1 << 28, 1 << 29
LOW = (1 << 24) - 1
EDGE = 13.0


def pairing(stride, extent, devices, odd):
    pairs = []
    for i in range(devices):
        c = i // stride % extent
        partner = ((c + 1) ^ 1) - 1 if odd else c ^ 1
        pairs.append((i, i + (partner % extent - c) * stride))
    return pairs


def lanes_of(shape):
    return lax.broadcasted_iota(jnp.int32, shape, len(shape) - 1)


def roll(value, shift, axis=1):
    if isinstance(shift, int):
        shift %= value.shape[axis]
        if shift == 0:
            return value
    return pltpu.roll(value, shift, axis)


def place():
    me = lax.axis_index(AXIS)
    return me // (NBY * NBZ), me // NBZ % NBY, me % NBZ


def pack_kernel(cx, cy, u_in, vf_in, mask_in, code_in, zp, u, vf, c, mask, code, sems):
    copies = [
        pltpu.make_async_copy(mask_in, mask, sems.at[0]),
        pltpu.make_async_copy(code_in, code, sems.at[1]),
        pltpu.make_async_copy(vf_in, vf, sems.at[2]),
    ]
    for f in range(NFIELD):
        rows = pl.ds(f * cx * cy, cx * cy)
        copies.append(pltpu.make_async_copy(u_in.at[rows, :], u.at[rows, :], sems.at[3 + f]))
    for copy in copies:
        copy.start()
    lane = lanes_of((cy, 128))
    slot = ((lane + 1) & 127) >> 1
    low_lane = (lane & 1) == 0
    copies[0].wait()
    copies[1].wait()
    for x in range(cx):
        rows = pl.ds(x * cy, cy)
        c[rows, :] = jnp.where(mask[rows, :] == 1, code[rows, :], 13).astype(jnp.float32)
    for g in (1, 0):
        acc = jnp.zeros((cy, 128), jnp.float32)
        for k in (3, 2, 1, 0):
            f = 4 * g + k
            if f <= VF:
                copies[3 + f if f < VF else 2].wait()
            for x in range(cx):
                m = cx * k + x
                rows = pl.ds(x * cy, cy)
                if f < NFIELD:
                    part = roll(u[pl.ds((f * cx + x) * cy, cy), :], 2 * m)
                elif f < C2:
                    part = roll((vf if f == VF else c)[rows, :], 2 * m)
                else:
                    part = jnp.where(low_lane, roll(c[rows, :], 2 * m - 1), roll(c[rows, :], 2 * m + 1))
                acc = jnp.where(slot == m, part, acc)
        zp[g * cy : (g + 1) * cy, :] = acc


def faces_kernel(cx, cy, two_x, u, vf, c, y_a, y_b, *xs):
    bx, by, bz = place()

    def y_face(out, high):
        rim = jnp.where(high, cy - 1, 0)
        second = jnp.where(high, cy - 2, 1)

        def column(ref, base, row):
            return ref[pl.ds(base + row, cx, stride=cy), :]

        for f in range(NFIELD):
            out[f * cx : (f + 1) * cx, :] = column(u, f * cx * cy, rim)
        out[VF * cx : (VF + 1) * cx, :] = column(vf, 0, rim)
        out[C1 * cx : (C1 + 1) * cx, :] = column(c, 0, rim)
        out[C2 * cx : (C2 + 1) * cx, :] = column(c, 0, second)

    y_face(y_a, by % 2 == 0)
    y_face(y_b, by % 2 == 1)

    def x_face(out, high):
        rim = jnp.where(high, cx - 1, 0) * cy
        second = jnp.where(high, cx - 2, 1) * cy

        def rows(base, start):
            return pl.ds(pl.multiple_of(base + start, 8), cy)

        for f in range(NFIELD):
            out[f * cy : (f + 1) * cy, :] = u[rows(f * cx * cy, rim), :]
        out[VF * cy : (VF + 1) * cy, :] = vf[rows(0, rim), :]
        out[C1 * cy : (C1 + 1) * cy, :] = c[rows(0, rim), :]
        out[C2 * cy : (C2 + 1) * cy, :] = c[rows(0, second), :]

    x_face(xs[0], bx % 2 == 0)
    if two_x:
        x_face(xs[1], bx % 2 == 1)


def z_merge_kernel(cx, cy, r_a, r_b, ya_in, yb_in, zh, y_a, y_b):
    bx, by, bz = place()
    odd = bz % 2 == 1
    lane = lanes_of((cy, 128))
    low_lane = (lane & 1) == 0
    codes = (lane >= 63) & (lane <= 126)
    for g in range(2):
        rows = slice(g * cy, (g + 1) * cy)
        a, b = r_a[rows, :], r_b[rows, :]
        edge = jnp.where(codes, EDGE, 0.0) if g else jnp.zeros((cy, 128), jnp.float32)
        low = jnp.where(bz > 0, roll(jnp.where(odd, a, b), 1), edge)
        high = jnp.where(bz < NBZ - 1, roll(jnp.where(odd, b, a), -1), edge)
        zh[rows, :] = jnp.where(low_lane, low, high)
    n = NF * cx

    def finish(out, main, high):
        out[:n, :] = main[...]
        rim = jnp.where(high, cy - 1, 0)
        second = jnp.where(high, cy - 2, 1)
        for g in range(2):
            out[n + 2 * g : n + 2 * g + 1, :] = zh[pl.ds(g * cy + rim, 1), :]
            out[n + 2 * g + 1 : n + 2 * g + 2, :] = zh[pl.ds(g * cy + second, 1), :]
        out[n + 4 : n + 8, :] = jnp.zeros((4, 128), jnp.float32)

    finish(y_a, ya_in, by % 2 == 0)
    finish(y_b, yb_in, by % 2 == 1)


def z_edge_rows(cx):
    n = NF * cx
    row = lax.broadcasted_iota(jnp.int32, (n + 8, 128), 0)
    lane = lanes_of((n + 8, 128))
    codes = ((row >= C1 * cx) & (row < n)) | ((row >= n + 2) & (lane >= 63) & (lane <= 126))
    return jnp.where(codes, EDGE, 0.0)


def y_merge_kernel(cx, cy, two_x, r_a, r_b, zh, *refs):
    copies = 2 if two_x else 1
    mains, (y_lo, y_hi), xs = refs[:copies], refs[copies : copies + 2], refs[copies + 2 :]
    bx, by, bz = place()
    odd = by % 2 == 1
    edge = z_edge_rows(cx)
    a, b = r_a[...], r_b[...]
    y_lo[...] = jnp.where(by > 0, jnp.where(odd, a, b), edge)
    y_hi[...] = jnp.where(by < NBY - 1, jnp.where(odd, b, a), edge)
    n = NF * cx

    def x_rim(out, main, high):
        rim = jnp.where(high, cx - 1, 0)
        second = jnp.where(high, cx - 2, 1)
        at = NF * cy
        out[:at, :] = main[...]
        out[at : at + 2 * cy, :] = zh[...]
        at += 2 * cy
        for y in (y_lo, y_hi):
            out[at : at + 4, :] = y[n : n + 4, :]
            at += 4
        for y in (y_lo, y_hi):
            for f in range(NF):
                out[at : at + 1, :] = y[pl.ds(f * cx + rim, 1), :]
                at += 1
            for f in (C1, C2):
                out[at : at + 1, :] = y[pl.ds(f * cx + second, 1), :]
                at += 1
        out[at:, :] = jnp.zeros((out.shape[0] - at, 128), jnp.float32)

    x_rim(xs[0], mains[0], bx % 2 == 0)
    if two_x:
        x_rim(xs[1], mains[1], bx % 2 == 1)


def decode(code):
    qx = (code * 57) >> 9
    rest = code - 9 * qx
    qy = (rest * 11) >> 5
    qz = rest - 3 * qy
    word = 1 + jnp.where(qz == 2, ZU, 0) + jnp.where(qz == 0, ZD, 0)
    word = word * jnp.where(qy == 2, 1 + YU, jnp.where(qy == 0, 1 + YD, 1))
    return word | jnp.where(qx == 2, XU, jnp.where(qx == 0, XD, 0))


def on(word, bits):
    return (word & bits) == bits


def ring_store(ref, lead, value):
    n = value.shape[0]
    ref[(*lead, slice(8, 8 + n), slice(None))] = value
    ref[(*lead, slice(0, 8), slice(None))] = value[n - 8 :]
    ref[(*lead, slice(8 + n, 16 + n), slice(None))] = value[:8]


def y_rows(r, x):
    cx = r.cx
    for f in range(C2):
        r.ht[f, x + 2, 0:1, :] = r.y_hi[f * cx + x : f * cx + x + 1, :]
        r.ht[f, x + 2, 7:8, :] = r.y_lo[f * cx + x : f * cx + x + 1, :]
    r.ht[C1, x + 2, 1:2, :] = r.y_hi[C2 * cx + x : C2 * cx + x + 1, :]
    r.ht[C1, x + 2, 6:7, :] = r.y_lo[C2 * cx + x : C2 * cx + x + 1, :]


def set_words(r, own, layer):
    both = jnp.concatenate([own, r.ht[C1, layer]], axis=0)
    ring_store(r.cw, (layer,), decode(both.astype(jnp.int32)))


def z_pair(r, layer):
    return (r.lane == 2 * layer) | (r.lane == 2 * layer - 1) | ((r.lane == 127) & (layer == 0))


def collect(r, layer, acc):
    return jnp.where(z_pair(r, layer), roll(r.cw[layer, 8 : 8 + r.rows, :], 2 * layer), acc)


def z_halo(r, f, rows_of, shift):
    g, k = f // 4, f % 4
    return roll(rows_of(g), 4 - 2 * r.cx * k + shift)


def spread_counts(r, planes):
    mid = up = down = jnp.zeros((r.rows, 128), jnp.int32)
    for word, bits in planes:
        v = 1 + ((word & YU) << 6) + ((word & YD) << 4)
        if bits is not None:
            v = jnp.where((word & bits) != 0, v, 0)
        mid = mid + v
        up = up + jnp.where((word & XU) != 0, v, 0)
        down = down + jnp.where((word & XD) != 0, v, 0)
    total = mid + roll(up, 2) + roll(down, -2)
    ring_store(r.tmp_i, (0,), total)
    before, after = r.tmp_i[0, 7 : 7 + r.rows, :], r.tmp_i[0, 9 : 9 + r.rows, :]
    return (total & 255) + ((before >> 8) & 255) + ((after >> 16) & 255)


def z_counts(r, inner):
    outer1, outer2 = (decode(r.zf[f].astype(jnp.int32)) for f in (C1, C2))
    r.ow[...] = outer1
    z_count = spread_counts(r, ((outer1, None), (outer2, r.inward), (inner, r.outward)))
    r.i1[...] = spread_counts(r, ((outer1, r.inward),))
    z_weight = r.zf[VF] / z_count.astype(jnp.float32)
    r.zw[0] = z_weight
    for f in range(NFIELD):
        r.zw[f + 1] = z_weight * r.zf[f]


def weigh(r, layer, field, slot=0):
    rows = r.rows
    mid, left, right = (r.cw[layer + d, 8 : 8 + rows, :] for d in (0, -1, 1))
    total = (mid & LOW) + jnp.where((left & XU) != 0, left & LOW, 0) + jnp.where((right & XD) != 0, right & LOW, 0)
    ring_store(r.tmp_i, (slot,), total)
    before, after = r.tmp_i[slot, 7 : 7 + rows, :], r.tmp_i[slot, 9 : 9 + rows, :]
    total = (total & 0x333) + ((before >> 2) & 0x333) + ((after >> 12) & 0x333)
    back = 128 - 2 * layer
    extra = roll(r.i1[...], back)
    first_lane, last_lane = r.lane == 0, r.lane == 127
    count = (total & 15) + jnp.where(first_lane, extra, (roll(total, 1) >> 4) & 15)
    count = count + jnp.where(last_lane, extra, (roll(total, -1) >> 8) & 15)
    inverse = 1.0 / count.astype(jnp.float32)
    r.rc[layer] = inverse[: r.cy]
    weight = field(VF) * inverse
    pair = z_pair(r, layer)
    for f in range(NFIELD + 1):
        w = weight * field(f - 1) if f else weight
        halo = roll(r.zw[f], back)
        ring_store(r.h0, (f, layer), w)
        ring_store(r.hm, (f, layer), w + jnp.where(first_lane, halo, roll(w, 1)))
        ring_store(r.hp, (f, layer), w + jnp.where(last_lane, halo, roll(w, -1)))
        r.zi[f] = jnp.where(pair, roll(w, 2 * layer), r.zi[f])


def own_field(r, x, f):
    base = (f * r.cx + x if f < NFIELD else x) * r.cy
    ref = r.u if f < NFIELD else r.vf
    if not isinstance(base, int):
        base = pl.multiple_of(base, 8)
    return jnp.concatenate([ref[pl.ds(base, r.cy), :], r.ht[f, x + 2]], axis=0)


def z_averages(r):
    rows, word, tmp = r.rows, r.ow[...], r.tmp_f
    sums = []
    for f in range(NFIELD + 1):
        ring_store(tmp, (f,), r.zw[f] + r.zi[f])
        mid, before, after = (tmp[f, s : s + rows, :] for s in (8, 7, 9))
        parts = []
        for d in (0, 1, -1):
            m, b, a = (roll(v, -2 * d) for v in (mid, before, after))
            parts.append(m + jnp.where((word & YU) != 0, a, jnp.where((word & YD) != 0, b, 0.0)))
        sums.append(parts[0] + jnp.where((word & XU) != 0, parts[1], jnp.where((word & XD) != 0, parts[2], 0.0)))
    inverse = 1.0 / sums[0]
    for f in range(NFIELD):
        v = jnp.where((word & r.inward) != 0, sums[f + 1] * inverse, 0.0)
        spread = []
        for bits in (0, YU, YD):
            w = jnp.where((word & bits) != 0, v, 0.0) if bits else v
            up, down = jnp.where((word & XU) != 0, w, 0.0), jnp.where((word & XD) != 0, w, 0.0)
            spread.append(w + roll(up, 2) + roll(down, -2))
        ring_store(tmp, (6 + 2 * f,), spread[1])
        ring_store(tmp, (7 + 2 * f,), spread[2])
        r.dz[f] = spread[0] + tmp[6 + 2 * f, 7 : 7 + rows, :] + tmp[7 + 2 * f, 9 : 9 + rows, :]


def average(r, layer):
    rows = r.rows
    tiles = rows // 8
    for t in range(tiles):
        at = 8 + 8 * t
        word = r.cw[layer, at : at + 8, :]
        zu, zd = (word & ZU) != 0, (word & ZD) != 0
        yu, yd = (word & YU) != 0, (word & YD) != 0
        xu, xd = (word & XU) != 0, (word & XD) != 0
        sums = []
        for f in range(NFIELD + 1):
            parts = []
            for d in (0, 1, -1):
                line = []
                for e in (0, 1, -1):
                    at_e = slice(at + e, at + e + 8)
                    v0, vm, vp = (h[f, layer + d, at_e, :] for h in (r.h0, r.hm, r.hp))
                    line.append(jnp.where(zu, vp, jnp.where(zd, vm, v0)))
                parts.append(line[0] + jnp.where(yu, line[1], jnp.where(yd, line[2], 0.0)))
            sums.append(parts[0] + jnp.where(xu, parts[1], jnp.where(xd, parts[2], 0.0)))
        inverse = 1.0 / sums[0]
        for f in range(NFIELD):
            a = sums[f + 1] * inverse
            r.av[f, layer, at : at + 8, :] = a
            if t == 0:
                r.av[f, layer, 8 + rows : 16 + rows, :] = a
            if t == tiles - 1:
                r.av[f, layer, 0:8, :] = a


def redistribute(r, x, out):
    cx, cy = r.cx, r.cy
    layer = x + 2
    back = 128 - 2 * layer
    lane = lanes_of((8, 128))
    first_lane, last_lane = lane == 0, lane == 127
    for t in range(cy // 8):
        at = 8 + 8 * t
        base = [r.av[f, layer, at : at + 8, :] for f in range(NFIELD)]
        word = r.cw[layer, at : at + 8, :]
        up = [jnp.where((word & ZU) != 0, a, 0.0) for a in base]
        down = [jnp.where((word & ZD) != 0, a, 0.0) for a in base]
        for d in (0, 1, -1):
            for e in (0, 1, -1):
                if d == 0 and e == 0:
                    continue
                at_e = slice(at - e, at - e + 8)
                word = r.cw[layer - d, at_e, :]
                bits = (0, XU, XD)[d] | (0, YU, YD)[e]
                here = on(word, bits)
                here_up, here_down = on(word, bits | ZU), on(word, bits | ZD)
                for f in range(NFIELD):
                    a = r.av[f, layer - d, at_e, :]
                    base[f] = base[f] + jnp.where(here, a, 0.0)
                    up[f] = up[f] + jnp.where(here_up, a, 0.0)
                    down[f] = down[f] + jnp.where(here_down, a, 0.0)
        inverse = r.rc[layer, 8 * t : 8 * t + 8, :]
        for f in range(NFIELD):
            halo = roll(r.dz[f, 8 * t : 8 * t + 8, :], back)
            total = base[f] + jnp.where(first_lane, halo, roll(up[f], 1))
            total = total + jnp.where(last_lane, halo, roll(down[f], -1))
            out[pl.ds(pl.multiple_of((f * cx + x) * cy + 8 * t, 8), 8), :] = total * inverse


def common(r):
    r.rows = r.cy + 8
    r.lane = lanes_of((r.rows, 128))
    even = (r.lane & 1) == 0
    r.inward = jnp.where(even, ZU, ZD)
    r.outward = jnp.where(even, ZD, ZU)
    n = NF * r.cx
    for g in range(2):
        for i, row in enumerate((0, 1)):
            r.hz[0, g, row : row + 1, :] = r.y_hi[n + 2 * g + i : n + 2 * g + i + 1, :]
            r.hz[0, g, 7 - row : 8 - row, :] = r.y_lo[n + 2 * g + i : n + 2 * g + i + 1, :]

    def own_z(g):
        return jnp.concatenate([r.zh[g * r.cy : (g + 1) * r.cy, :], r.hz[0, g]], axis=0)

    return own_z


KEPT = ("cw", "inner", "zi", "h0", "hm", "hp", "rc", "av")
SCRATCH = ("ht", "hz", "zf", "ow", "tmp_i", "tmp_f", "i1", "zw", "dz")


def inner_kernel(cx, cy, *refs):
    names = ("u", "vf", "c", "zh", "y_lo", "y_hi", *KEPT, "res", *SCRATCH)
    r = types.SimpleNamespace(cx=cx, cy=cy, **dict(zip(names, refs)))
    own_z = common(r)
    r.ht[...] = jnp.zeros(r.ht.shape, jnp.float32)
    for x in range(cx):
        y_rows(r, x)

    def words(x, acc):
        set_words(r, r.c[pl.ds(pl.multiple_of(x * cy, 8), cy), :], x + 2)
        return collect(r, x + 2, acc)

    inner = lax.fori_loop(0, cx, words, jnp.ones((r.rows, 128), jnp.int32), unroll=4)
    r.inner[...] = inner
    for f in range(NF):
        r.zf[f] = z_halo(r, f, own_z, 0)
    z_counts(r, inner)
    r.zi[...] = jnp.zeros(r.zi.shape, jnp.float32)

    def weigh_two(i, _):
        for j in range(2):
            x = 1 + 2 * i + j
            weigh(r, x + 2, functools.partial(own_field, r, x), j)
        return 0

    lax.fori_loop(0, (cx - 2) // 2, weigh_two, 0)
    z_averages(r)

    def average_one(layer, _):
        average(r, layer)
        return 0

    lax.fori_loop(4, cx, average_one, 0)

    def spread_one(x, _):
        redistribute(r, x, r.res)
        return 0

    lax.fori_loop(3, cx - 3, spread_one, 0)


def outer_kernel(cx, cy, nbx, *refs):
    kept_in = len(KEPT)
    names = ("u", "vf", "c", "zh", "y_lo", "y_hi", "res", "xa", "xb")
    ins = refs[: len(names)]
    rest = refs[len(names) + kept_in :]
    r = types.SimpleNamespace(cx=cx, cy=cy, **dict(zip(names, ins)))
    r.__dict__.update(zip(("out", *KEPT, *SCRATCH, "rim", "sems"), rest))
    size = cx * cy

    def send(src, first, last, base):
        copies = []
        for f in range(NFIELD):
            rows = pl.ds(f * size + first * cy, (last - first) * cy)
            copies.append(pltpu.make_async_copy(src.at[rows, :], r.out.at[rows, :], r.sems.at[base + f]))
        for copy in copies:
            copy.start()
        return copies

    copies = send(r.res, 3, cx - 3, 0)
    own_z = common(r)
    bx, by, bz = place()
    x_odd = bx % 2 == 1
    has_lo, has_hi = bx > 0, bx < nbx - 1

    def x_part(side, first, count):
        a, b = r.xa[first : first + count, :], r.xb[first : first + count, :]
        return jnp.where(x_odd, a, b) if side == 0 else jnp.where(x_odd, b, a)

    def x_raw(f, side):
        edge = EDGE if f >= C1 else 0.0
        return jnp.where(has_hi if side else has_lo, x_part(side, f * cy, cy), edge)

    zrow = NF * cy
    edges = zrow + 2 * cy
    for x in (0, cx - 1):
        y_rows(r, x)
    for side, layer, second in ((0, 1, 0), (1, cx + 2, cx + 3)):
        present = has_hi if side else has_lo
        for y, row1, row2 in ((0, 7, 6), (1, 0, 1)):
            base = edges + 8 + 10 * y

            def rim(i, edge, base=base, side=side, present=present):
                return jnp.where(present, x_part(side, base + i, 1), edge)

            for f in range(C1):
                r.ht[f, layer, row1 : row1 + 1, :] = rim(f, 0.0)
            r.ht[C1, layer, row1 : row1 + 1, :] = rim(C1, EDGE)
            r.ht[C1, layer, row2 : row2 + 1, :] = rim(C2, EDGE)
            r.ht[C1, second, row1 : row1 + 1, :] = rim(NF, EDGE)
            r.ht[C1, second, row2 : row2 + 1, :] = rim(NF + 1, EDGE)
    set_words(r, x_raw(C2, 0), 0)
    set_words(r, x_raw(C1, 0), 1)
    set_words(r, x_raw(C1, 1), cx + 2)
    set_words(r, x_raw(C2, 1), cx + 3)

    for side in (0, 1):
        for g in range(2):
            for i, row in enumerate((0, 1)):
                lo, hi = edges + 2 * g + i, edges + 4 + 2 * g + i
                r.hz[1 + side, g, row : row + 1, :] = x_part(side, hi, 1)
                r.hz[1 + side, g, 7 - row : 8 - row, :] = x_part(side, lo, 1)

    def x_z(side):
        return lambda g: jnp.concatenate([x_part(side, zrow + g * cy, cy), r.hz[1 + side, g]], axis=0)

    below = (r.lane == 127) | (r.lane <= 2)
    above = (r.lane >= 2 * cx + 3) & (r.lane <= 2 * cx + 6)
    for f in range(NF):
        edge = EDGE if f >= C1 else 0.0
        lo = jnp.where(has_lo, z_halo(r, f, x_z(0), -2 * cx), edge)
        hi = jnp.where(has_hi, z_halo(r, f, x_z(1), 2 * cx), edge)
        r.zf[f] = jnp.where(below, lo, jnp.where(above, hi, z_halo(r, f, own_z, 0)))
    inner = r.inner[...]
    for layer in (0, 1, cx + 2, cx + 3):
        inner = collect(r, layer, inner)
    z_counts(r, inner)
    weigh(r, 1, lambda f: jnp.concatenate([x_raw(f, 0), r.ht[f, 1]], axis=0), 0)
    weigh(r, 2, functools.partial(own_field, r, 0), 1)
    weigh(r, cx + 1, functools.partial(own_field, r, cx - 1), 2)
    weigh(r, cx + 2, lambda f: jnp.concatenate([x_raw(f, 1), r.ht[f, cx + 2]], axis=0), 3)
    z_averages(r)

    def average_one(i, _):
        average(r, 1 + i + jnp.where(i >= 3, cx - 4, 0))
        return 0

    lax.fori_loop(0, 6, average_one, 0)

    def spread_one(x, _):
        redistribute(r, x, r.rim)
        return 0

    lax.fori_loop(0, 3, spread_one, 0)
    copies += send(r.rim, 0, 3, NFIELD)
    lax.fori_loop(cx - 3, cx, spread_one, 0)
    copies += send(r.rim, cx - 3, cx, 2 * NFIELD)
    for copy in copies:
        copy.wait()


def call(kernel, ins, outs, scratch=(), name=None, grant=8, flops=0, **kwargs):
    return pl.pallas_call(
        kernel,
        in_specs=ins,
        out_specs=tuple(pl.BlockSpec(memory_space=o.memory_space) for o in outs),
        out_shape=tuple(outs),
        scratch_shapes=scratch,
        name=name,
        cost_estimate=pl.CostEstimate(flops=flops, transcendentals=0, bytes_accessed=0),
        compiler_params=pltpu.CompilerParams(vmem_limit_bytes=grant << 20),
        **kwargs,
    )


def per_device(conserved, volume_fraction, cut_mask, merge_code):
    _, cx, cy, cz = cut_mask.shape
    devices = lax.axis_size(AXIS)
    nbx = devices // (NBY * NBZ)
    two_x = nbx > 2
    cells = cx * cy
    u = conserved.reshape(NFIELD * cells, cz)
    vf, mask, code = (a.reshape(cells, cz) for a in (volume_fraction, cut_mask, merge_code))
    f32, i32 = jnp.float32, jnp.int32
    on_chip, far = pl.BlockSpec(memory_space=pltpu.VMEM), pl.BlockSpec(memory_space=pltpu.HBM)

    def vmem(*shape, dtype=f32):
        return pltpu.VMEM((*shape, cz), dtype)

    def swap(value, stride, extent, odd):
        return lax.ppermute(value, AXIS, pairing(stride, extent, devices, odd))

    n = NF * cx
    copies = 2 if two_x else 1
    zp, u, vf, c = call(
        functools.partial(pack_kernel, cx, cy),
        [far] * 4,
        [vmem(2 * cy), vmem(NFIELD * cells), vmem(cells), vmem(cells)],
        [vmem(cells, dtype=i32), vmem(cells, dtype=i32), pltpu.SemaphoreType.DMA((3 + NFIELD,))],
        "pack",
    )(*(pltpu.with_memory_space_constraint(a, pltpu.HBM) for a in (u, vf, mask, code)))
    za, zb = swap(zp, 1, NBZ, False), swap(zp, 1, NBZ, True)
    ya, yb, *xs = call(
        functools.partial(faces_kernel, cx, cy, two_x),
        [on_chip] * 3,
        [vmem(n), vmem(n)] + [vmem(NF * cy)] * copies,
        name="faces",
        flops=1 << 20,
    )(u, vf, c)
    zh, ya, yb = call(
        functools.partial(z_merge_kernel, cx, cy), [on_chip] * 4, [vmem(2 * cy), vmem(n + 8), vmem(n + 8)], name="z_merge"
    )(za, zb, ya, yb)
    ya, yb = swap(ya, NBZ, NBY, False), swap(yb, NBZ, NBY, True)
    y_lo, y_hi, *xs = call(
        functools.partial(y_merge_kernel, cx, cy, two_x),
        [on_chip] * (3 + copies),
        [vmem(n + 8), vmem(n + 8)] + [vmem(NF * cy + 2 * cy + 32)] * copies,
        name="y_merge",
    )(ya, yb, zh, *xs)
    xs = [swap(x, NBY * NBZ, nbx, odd) for odd, x in enumerate(xs)]
    xa, xb = xs if two_x else xs * 2

    rows, ring, layers = cy + 8, cy + 24, cx + 4
    kept = [
        vmem(layers, ring, dtype=i32),
        vmem(rows, dtype=i32),
        vmem(NFIELD + 1, rows),
        vmem(NFIELD + 1, layers, ring),
        vmem(NFIELD + 1, layers, ring),
        vmem(NFIELD + 1, layers, ring),
        vmem(layers, cy),
        vmem(NFIELD, layers, ring),
    ]
    scratch = [
        vmem(C2, layers, 8),
        vmem(3, 2, 8),
        vmem(NF, rows),
        vmem(rows, dtype=i32),
        vmem(4, ring, dtype=i32),
        vmem(6 + 2 * NFIELD, ring),
        vmem(rows, dtype=i32),
        vmem(NFIELD + 1, rows),
        vmem(NFIELD, rows),
    ]
    *state, res = call(
        functools.partial(inner_kernel, cx, cy),
        [on_chip] * 6,
        kept + [vmem(NFIELD * cells)],
        scratch,
        "inner",
        flops=1 << 26,
    )(u, vf, c, zh, y_lo, y_hi)
    first = 9
    out, *_ = call(
        functools.partial(outer_kernel, cx, cy, nbx),
        [on_chip] * (first + len(kept)),
        [pltpu.HBM((NFIELD * cells, cz), f32)] + kept,
        scratch + [vmem(NFIELD * cells), pltpu.SemaphoreType.DMA((3 * NFIELD,))],
        "outer",
        flops=1 << 25,
        input_output_aliases={first + i: 1 + i for i in range(len(kept))},
    )(u, vf, c, zh, y_lo, y_hi, res, xa, xb, *state)
    return out.reshape(conserved.shape)


def solution(mesh):
    return jax.shard_map(
        per_device,
        mesh=mesh,
        in_specs=(
            P(AXIS, None, None, None, None),
            P(AXIS, None, None, None),
            P(AXIS, None, None, None),
            P(AXIS, None, None, None),
        ),
        out_specs=P(AXIS, None, None, None, None),
        check_vma=False,
    )
```

```python
import functools
import types

import jax
import jax.numpy as jnp
from jax import lax
from jax.experimental import pallas as pl
from jax.experimental.pallas import tpu as pltpu
from jax.sharding import PartitionSpec as P

NBY = 4
NBZ = 4
AXIS = "boxes"

NFIELD = 5
VF = 5
C1 = 6
C2 = 7
NF = 8
ZU, ZD, YU, YD, XU, XD = 16, 256, 4, 4096, 1 << 28, 1 << 29
LOW = (1 << 24) - 1
EDGE = 13.0


def pairing(stride, extent, devices, odd):
    pairs = []
    for i in range(devices):
        c = i // stride % extent
        partner = ((c + 1) ^ 1) - 1 if odd else c ^ 1
        pairs.append((i, i + (partner % extent - c) * stride))
    return pairs


def lanes_of(shape):
    return lax.broadcasted_iota(jnp.int32, shape, len(shape) - 1)


def roll(value, shift, axis=1):
    if isinstance(shift, int):
        shift %= value.shape[axis]
        if shift == 0:
            return value
    return pltpu.roll(value, shift, axis)


def place():
    me = lax.axis_index(AXIS)
    return me // (NBY * NBZ), me // NBZ % NBY, me % NBZ


def pack_kernel(cx, cy, u_in, vf_in, mask_in, code_in, zp, u, vf, c, mask, code, sems):
    copies = [
        pltpu.make_async_copy(mask_in, mask, sems.at[0]),
        pltpu.make_async_copy(code_in, code, sems.at[1]),
        pltpu.make_async_copy(vf_in, vf, sems.at[2]),
    ]
    for f in range(NFIELD):
        rows = pl.ds(f * cx * cy, cx * cy)
        copies.append(pltpu.make_async_copy(u_in.at[rows, :], u.at[rows, :], sems.at[3 + f]))
    for copy in copies:
        copy.start()
    lane = lanes_of((cy, 128))
    slot = ((lane + 1) & 127) >> 1
    low_lane = (lane & 1) == 0
    copies[0].wait()
    copies[1].wait()
    for x in range(cx):
        rows = pl.ds(x * cy, cy)
        c[rows, :] = jnp.where(mask[rows, :] == 1, code[rows, :], 13).astype(jnp.float32)
    for g in (1, 0):
        acc = jnp.zeros((cy, 128), jnp.float32)
        for k in (3, 2, 1, 0):
            f = 4 * g + k
            if f <= VF:
                copies[3 + f if f < VF else 2].wait()
            for x in range(cx):
                m = cx * k + x
                rows = pl.ds(x * cy, cy)
                if f < NFIELD:
                    part = roll(u[pl.ds((f * cx + x) * cy, cy), :], 2 * m)
                elif f < C2:
                    part = roll((vf if f == VF else c)[rows, :], 2 * m)
                else:
                    part = jnp.where(low_lane, roll(c[rows, :], 2 * m - 1), roll(c[rows, :], 2 * m + 1))
                acc = jnp.where(slot == m, part, acc)
        zp[g * cy : (g + 1) * cy, :] = acc


def faces_kernel(cx, cy, two_x, u, vf, c, y_a, y_b, *xs):
    bx, by, bz = place()

    def y_face(out, high):
        rim = jnp.where(high, cy - 1, 0)
        second = jnp.where(high, cy - 2, 1)

        def column(ref, base, row):
            return ref[pl.ds(base + row, cx, stride=cy), :]

        for f in range(NFIELD):
            out[f * cx : (f + 1) * cx, :] = column(u, f * cx * cy, rim)
        out[VF * cx : (VF + 1) * cx, :] = column(vf, 0, rim)
        out[C1 * cx : (C1 + 1) * cx, :] = column(c, 0, rim)
        out[C2 * cx : (C2 + 1) * cx, :] = column(c, 0, second)

    y_face(y_a, by % 2 == 0)
    y_face(y_b, by % 2 == 1)

    def x_face(out, high):
        rim = jnp.where(high, cx - 1, 0) * cy
        second = jnp.where(high, cx - 2, 1) * cy

        def rows(base, start):
            return pl.ds(pl.multiple_of(base + start, 8), cy)

        for f in range(NFIELD):
            out[f * cy : (f + 1) * cy, :] = u[rows(f * cx * cy, rim), :]
        out[VF * cy : (VF + 1) * cy, :] = vf[rows(0, rim), :]
        out[C1 * cy : (C1 + 1) * cy, :] = c[rows(0, rim), :]
        out[C2 * cy : (C2 + 1) * cy, :] = c[rows(0, second), :]

    x_face(xs[0], bx % 2 == 0)
    if two_x:
        x_face(xs[1], bx % 2 == 1)


def z_merge_kernel(cx, cy, r_a, r_b, ya_in, yb_in, zh, y_a, y_b):
    bx, by, bz = place()
    odd = bz % 2 == 1
    lane = lanes_of((cy, 128))
    low_lane = (lane & 1) == 0
    codes = (lane >= 63) & (lane <= 126)
    for g in range(2):
        rows = slice(g * cy, (g + 1) * cy)
        a, b = r_a[rows, :], r_b[rows, :]
        edge = jnp.where(codes, EDGE, 0.0) if g else jnp.zeros((cy, 128), jnp.float32)
        low = jnp.where(bz > 0, roll(jnp.where(odd, a, b), 1), edge)
        high = jnp.where(bz < NBZ - 1, roll(jnp.where(odd, b, a), -1), edge)
        zh[rows, :] = jnp.where(low_lane, low, high)
    n = NF * cx

    def finish(out, main, high):
        out[:n, :] = main[...]
        rim = jnp.where(high, cy - 1, 0)
        second = jnp.where(high, cy - 2, 1)
        for g in range(2):
            out[n + 2 * g : n + 2 * g + 1, :] = zh[pl.ds(g * cy + rim, 1), :]
            out[n + 2 * g + 1 : n + 2 * g + 2, :] = zh[pl.ds(g * cy + second, 1), :]
        out[n + 4 : n + 8, :] = jnp.zeros((4, 128), jnp.float32)

    finish(y_a, ya_in, by % 2 == 0)
    finish(y_b, yb_in, by % 2 == 1)


def z_edge_rows(cx):
    n = NF * cx
    row = lax.broadcasted_iota(jnp.int32, (n + 8, 128), 0)
    lane = lanes_of((n + 8, 128))
    codes = ((row >= C1 * cx) & (row < n)) | ((row >= n + 2) & (lane >= 63) & (lane <= 126))
    return jnp.where(codes, EDGE, 0.0)


def y_merge_kernel(cx, cy, two_x, r_a, r_b, zh, *refs):
    copies = 2 if two_x else 1
    mains, (y_lo, y_hi), xs = refs[:copies], refs[copies : copies + 2], refs[copies + 2 :]
    bx, by, bz = place()
    odd = by % 2 == 1
    edge = z_edge_rows(cx)
    a, b = r_a[...], r_b[...]
    y_lo[...] = jnp.where(by > 0, jnp.where(odd, a, b), edge)
    y_hi[...] = jnp.where(by < NBY - 1, jnp.where(odd, b, a), edge)
    n = NF * cx

    def x_rim(out, main, high):
        rim = jnp.where(high, cx - 1, 0)
        second = jnp.where(high, cx - 2, 1)
        at = NF * cy
        out[:at, :] = main[...]
        lane = lanes_of((8, 128))
        spot = (lane - jnp.where(high, 2 * cx - 5, 2 * cx - 1)) & (2 * cx - 1)
        tile = jnp.zeros((8, 128), jnp.float32)
        for t in range(cy // 8):
            for g in range(2):
                start = 8 * t + 4 * g
                part = roll(zh[g * cy + 8 * t : g * cy + 8 * t + 8, :], start)
                tile = jnp.where((spot >= start) & (spot < start + 4), part, tile)
        out[at : at + 8, :] = tile
        at += 8
        for y in (y_lo, y_hi):
            out[at : at + 4, :] = y[n : n + 4, :]
            at += 4
        for y in (y_lo, y_hi):
            for f in range(NF):
                out[at : at + 1, :] = y[pl.ds(f * cx + rim, 1), :]
                at += 1
            for f in (C1, C2):
                out[at : at + 1, :] = y[pl.ds(f * cx + second, 1), :]
                at += 1
        out[at:, :] = jnp.zeros((out.shape[0] - at, 128), jnp.float32)

    x_rim(xs[0], mains[0], bx % 2 == 0)
    if two_x:
        x_rim(xs[1], mains[1], bx % 2 == 1)


def decode(code):
    qx = (code * 57) >> 9
    rest = code - 9 * qx
    qy = (rest * 11) >> 5
    qz = rest - 3 * qy
    word = 1 + jnp.where(qz == 2, ZU, 0) + jnp.where(qz == 0, ZD, 0)
    word = word * jnp.where(qy == 2, 1 + YU, jnp.where(qy == 0, 1 + YD, 1))
    return word | jnp.where(qx == 2, XU, jnp.where(qx == 0, XD, 0))


def on(word, bits):
    return (word & bits) == bits


def ring_store(ref, lead, value):
    n = value.shape[0]
    ref[(*lead, slice(8, 8 + n), slice(None))] = value
    ref[(*lead, slice(0, 8), slice(None))] = value[n - 8 :]


def ring_load(ref, lead, step):
    n = ref.shape[-2] - 16
    if step <= 0:
        return ref[(*lead, slice(8 + step, 8 + step + n), slice(None))]
    own = ref[(*lead, slice(8 + step, n + step), slice(None))]
    return jnp.concatenate([own, ref[(*lead, slice(step, 8 + step), slice(None))]], axis=0)


def y_rows(r, x):
    cx = r.cx
    for f in range(C2):
        r.ht[f, x + 2, 0:1, :] = r.y_hi[f * cx + x : f * cx + x + 1, :]
        r.ht[f, x + 2, 7:8, :] = r.y_lo[f * cx + x : f * cx + x + 1, :]
    r.ht[C1, x + 2, 1:2, :] = r.y_hi[C2 * cx + x : C2 * cx + x + 1, :]
    r.ht[C1, x + 2, 6:7, :] = r.y_lo[C2 * cx + x : C2 * cx + x + 1, :]


def set_words(r, own, layer):
    both = jnp.concatenate([own, r.ht[C1, layer]], axis=0)
    ring_store(r.cw, (layer,), decode(both.astype(jnp.int32)))


def z_pair(r, layer):
    return (r.lane == 2 * layer) | (r.lane == 2 * layer - 1) | ((r.lane == 127) & (layer == 0))


def collect(r, layer, acc):
    return jnp.where(z_pair(r, layer), roll(r.cw[layer, 8 : 8 + r.rows, :], 2 * layer), acc)


def z_halo(r, f, own):
    g, k = f // 4, f % 4
    return roll(own(g), 4 - 2 * r.cx * k)


def spread_counts(r, planes):
    mid = up = down = jnp.zeros((r.rows, 128), jnp.int32)
    for word, bits in planes:
        v = 1 + ((word & YU) << 6) + ((word & YD) << 4)
        if bits is not None:
            v = jnp.where((word & bits) != 0, v, 0)
        mid = mid + v
        up = up + jnp.where((word & XU) != 0, v, 0)
        down = down + jnp.where((word & XD) != 0, v, 0)
    total = mid + roll(up, 2) + roll(down, -2)
    ring_store(r.tmp_i, (0,), total)
    before, after = ring_load(r.tmp_i, (0,), -1), ring_load(r.tmp_i, (0,), 1)
    return (total & 255) + ((before >> 8) & 255) + ((after >> 16) & 255)


def z_counts(r, inner):
    outer1, outer2 = (decode(r.zf[f].astype(jnp.int32)) for f in (C1, C2))
    r.ow[...] = outer1
    z_count = spread_counts(r, ((outer1, None), (outer2, r.inward), (inner, r.outward)))
    r.i1[...] = spread_counts(r, ((outer1, r.inward),))
    z_weight = r.zf[VF] / z_count.astype(jnp.float32)
    r.zw[0] = z_weight
    for f in range(NFIELD):
        r.zw[f + 1] = z_weight * r.zf[f]


def weigh(r, group):
    rows = r.rows
    first_lane, last_lane = r.lane == 0, r.lane == 127
    totals = []
    for slot, (layer, _) in enumerate(group):
        mid, left, right = (r.cw[layer + d, 8 : 8 + rows, :] for d in (0, -1, 1))
        total = (mid & LOW) + jnp.where((left & XU) != 0, left & LOW, 0)
        ring_store(r.tmp_i, (slot,), total + jnp.where((right & XD) != 0, right & LOW, 0))
    for slot, (layer, _) in enumerate(group):
        total, before, after = (ring_load(r.tmp_i, (slot,), step) for step in (0, -1, 1))
        total = (total & 0x333) + ((before >> 2) & 0x333) + ((after >> 12) & 0x333)
        totals.append((total, roll(total, 1), roll(total, -1), roll(r.i1[...], -2 * layer)))
    for slot, (layer, field) in enumerate(group):
        total, below, above, extra = totals[slot]
        count = (total & 15) + jnp.where(first_lane, extra, (below >> 4) & 15)
        count = count + jnp.where(last_lane, extra, (above >> 8) & 15)
        inverse = 1.0 / count.astype(jnp.float32)
        r.rc[layer] = inverse[: r.cy]
        ring_store(r.h0, (0, layer), field(VF) * inverse)
    for slot, (layer, field) in enumerate(group):
        weight = ring_load(r.h0, (0, layer), 0)
        pair = z_pair(r, layer)
        for f in range(NFIELD + 1):
            w = weight
            if f:
                w = weight * field(f - 1)
                ring_store(r.h0, (f, layer), w)
            halo = roll(r.zw[f], -2 * layer)
            ring_store(r.hm, (f, layer), w + jnp.where(first_lane, halo, roll(w, 1)))
            ring_store(r.hp, (f, layer), w + jnp.where(last_lane, halo, roll(w, -1)))
            r.zi[f] = jnp.where(pair, roll(w, 2 * layer), r.zi[f])


def own_field(r, x, f):
    base = (f * r.cx + x if f < NFIELD else x) * r.cy
    ref = r.u if f < NFIELD else r.vf
    if not isinstance(base, int):
        base = pl.multiple_of(base, 8)
    return jnp.concatenate([ref[pl.ds(base, r.cy), :], r.ht[f, x + 2]], axis=0)


def z_averages(r):
    word, tmp = r.ow[...], r.tmp_f
    sums = []
    for f in range(NFIELD + 1):
        ring_store(tmp, (f,), r.zw[f] + r.zi[f])
        mid, before, after = (ring_load(tmp, (f,), step) for step in (0, -1, 1))
        parts = []
        for d in (0, 1, -1):
            m, b, a = (roll(v, -2 * d) for v in (mid, before, after))
            parts.append(m + jnp.where((word & YU) != 0, a, jnp.where((word & YD) != 0, b, 0.0)))
        sums.append(parts[0] + jnp.where((word & XU) != 0, parts[1], jnp.where((word & XD) != 0, parts[2], 0.0)))
    inverse = 1.0 / sums[0]
    for f in range(NFIELD):
        v = jnp.where((word & r.inward) != 0, sums[f + 1] * inverse, 0.0)
        spread = []
        for bits in (0, YU, YD):
            w = jnp.where((word & bits) != 0, v, 0.0) if bits else v
            up, down = jnp.where((word & XU) != 0, w, 0.0), jnp.where((word & XD) != 0, w, 0.0)
            spread.append(w + roll(up, 2) + roll(down, -2))
        ring_store(tmp, (6 + 2 * f,), spread[1])
        ring_store(tmp, (7 + 2 * f,), spread[2])
        r.dz[f] = spread[0] + ring_load(tmp, (6 + 2 * f,), -1) + ring_load(tmp, (7 + 2 * f,), 1)


def average(r, layer):
    rows = r.rows
    tiles = rows // 8
    for t in range(tiles):
        at = 8 + 8 * t
        word = r.cw[layer, at : at + 8, :]
        zu, zd = (word & ZU) != 0, (word & ZD) != 0
        yu, yd = (word & YU) != 0, (word & YD) != 0
        xu, xd = (word & XU) != 0, (word & XD) != 0
        sums = []
        for f in range(NFIELD + 1):
            parts = []
            for d in (0, 1, -1):
                line = []
                for e in (0, 1, -1):
                    base = 0 if t == tiles - 1 and e == 1 else at
                    at_e = slice(base + e, base + e + 8)
                    v0, vm, vp = (h[f, layer + d, at_e, :] for h in (r.h0, r.hm, r.hp))
                    line.append(jnp.where(zu, vp, jnp.where(zd, vm, v0)))
                parts.append(line[0] + jnp.where(yu, line[1], jnp.where(yd, line[2], 0.0)))
            sums.append(parts[0] + jnp.where(xu, parts[1], jnp.where(xd, parts[2], 0.0)))
        inverse = 1.0 / sums[0]
        for f in range(NFIELD):
            a = sums[f + 1] * inverse
            r.av[f, layer, at : at + 8, :] = a
            if t == tiles - 1:
                r.av[f, layer, 0:8, :] = a


def redistribute(r, x, out):
    cx, cy = r.cx, r.cy
    layer = x + 2
    back = 128 - 2 * layer
    lane = lanes_of((8, 128))
    first_lane, last_lane = lane == 0, lane == 127
    for t in range(cy // 8):
        at = 8 + 8 * t
        base = [r.av[f, layer, at : at + 8, :] for f in range(NFIELD)]
        word = r.cw[layer, at : at + 8, :]
        up = [jnp.where((word & ZU) != 0, a, 0.0) for a in base]
        down = [jnp.where((word & ZD) != 0, a, 0.0) for a in base]
        for d in (0, 1, -1):
            for e in (0, 1, -1):
                if d == 0 and e == 0:
                    continue
                at_e = slice(at - e, at - e + 8)
                word = r.cw[layer - d, at_e, :]
                bits = (0, XU, XD)[d] | (0, YU, YD)[e]
                here = on(word, bits)
                here_up, here_down = on(word, bits | ZU), on(word, bits | ZD)
                for f in range(NFIELD):
                    a = r.av[f, layer - d, at_e, :]
                    base[f] = base[f] + jnp.where(here, a, 0.0)
                    up[f] = up[f] + jnp.where(here_up, a, 0.0)
                    down[f] = down[f] + jnp.where(here_down, a, 0.0)
        inverse = r.rc[layer, 8 * t : 8 * t + 8, :]
        for f in range(NFIELD):
            halo = roll(r.dz[f, 8 * t : 8 * t + 8, :], back)
            total = base[f] + jnp.where(first_lane, halo, roll(up[f], 1))
            total = total + jnp.where(last_lane, halo, roll(down[f], -1))
            out[pl.ds(pl.multiple_of((f * cx + x) * cy + 8 * t, 8), 8), :] = total * inverse


def common(r):
    r.rows = r.cy + 8
    r.lane = lanes_of((r.rows, 128))
    even = (r.lane & 1) == 0
    r.inward = jnp.where(even, ZU, ZD)
    r.outward = jnp.where(even, ZD, ZU)
    n = NF * r.cx
    for g in range(2):
        for i, row in enumerate((0, 1)):
            r.hz[0, g, row : row + 1, :] = r.y_hi[n + 2 * g + i : n + 2 * g + i + 1, :]
            r.hz[0, g, 7 - row : 8 - row, :] = r.y_lo[n + 2 * g + i : n + 2 * g + i + 1, :]

    def own_z(g):
        return jnp.concatenate([r.zh[g * r.cy : (g + 1) * r.cy, :], r.hz[0, g]], axis=0)

    return own_z


KEPT = ("cw", "inner", "zi", "h0", "hm", "hp", "rc", "av")
SCRATCH = ("ht", "hz", "zf", "ow", "tmp_i", "tmp_f", "i1", "zw", "dz")


def inner_kernel(cx, cy, *refs):
    names = ("u", "vf", "c", "zh", "y_lo", "y_hi", *KEPT, "res", *SCRATCH)
    r = types.SimpleNamespace(cx=cx, cy=cy, **dict(zip(names, refs)))
    own_z = common(r)
    r.ht[...] = jnp.zeros(r.ht.shape, jnp.float32)
    for x in range(cx):
        y_rows(r, x)

    def words(x, acc):
        set_words(r, r.c[pl.ds(pl.multiple_of(x * cy, 8), cy), :], x + 2)
        return collect(r, x + 2, acc)

    inner = lax.fori_loop(0, cx, words, jnp.ones((r.rows, 128), jnp.int32), unroll=4)
    r.inner[...] = inner
    for f in range(NF):
        r.zf[f] = z_halo(r, f, own_z)
    z_counts(r, inner)
    r.zi[...] = jnp.zeros(r.zi.shape, jnp.float32)

    weigh(r, [(x + 2, functools.partial(own_field, r, x)) for x in range(1, cx - 1)])
    z_averages(r)

    def average_one(layer, _):
        average(r, layer)
        return 0

    lax.fori_loop(4, cx, average_one, 0)

    def spread_one(x, _):
        redistribute(r, x, r.res)
        return 0

    lax.fori_loop(3, cx - 3, spread_one, 0)


def outer_kernel(cx, cy, nbx, *refs):
    kept_in = len(KEPT)
    names = ("u", "vf", "c", "zh", "y_lo", "y_hi", "res", "xa", "xb")
    ins = refs[: len(names)]
    rest = refs[len(names) + kept_in :]
    r = types.SimpleNamespace(cx=cx, cy=cy, **dict(zip(names, ins)))
    r.__dict__.update(zip(("out", *KEPT, *SCRATCH, "rim", "sems"), rest))
    size = cx * cy

    def send(src, first, last, base):
        copies = []
        for f in range(NFIELD):
            rows = pl.ds(f * size + first * cy, (last - first) * cy)
            copies.append(pltpu.make_async_copy(src.at[rows, :], r.out.at[rows, :], r.sems.at[base + f]))
        for copy in copies:
            copy.start()
        return copies

    copies = send(r.res, 3, cx - 3, 0)
    own_z = common(r)
    bx, by, bz = place()
    x_odd = bx % 2 == 1
    has_lo, has_hi = bx > 0, bx < nbx - 1

    def x_part(side, first, count):
        a, b = r.xa[first : first + count, :], r.xb[first : first + count, :]
        return jnp.where(x_odd, a, b) if side == 0 else jnp.where(x_odd, b, a)

    def x_raw(f, side):
        edge = EDGE if f >= C1 else 0.0
        return jnp.where(has_hi if side else has_lo, x_part(side, f * cy, cy), edge)

    zrow = NF * cy
    edges = zrow + 8
    for x in (0, cx - 1):
        y_rows(r, x)
    for side, layer, second in ((0, 1, 0), (1, cx + 2, cx + 3)):
        present = has_hi if side else has_lo
        for y, row1, row2 in ((0, 7, 6), (1, 0, 1)):
            base = edges + 8 + 10 * y

            def rim(i, edge, base=base, side=side, present=present):
                return jnp.where(present, x_part(side, base + i, 1), edge)

            for f in range(C1):
                r.ht[f, layer, row1 : row1 + 1, :] = rim(f, 0.0)
            r.ht[C1, layer, row1 : row1 + 1, :] = rim(C1, EDGE)
            r.ht[C1, layer, row2 : row2 + 1, :] = rim(C2, EDGE)
            r.ht[C1, second, row1 : row1 + 1, :] = rim(NF, EDGE)
            r.ht[C1, second, row2 : row2 + 1, :] = rim(NF + 1, EDGE)
    set_words(r, x_raw(C2, 0), 0)
    set_words(r, x_raw(C1, 0), 1)
    set_words(r, x_raw(C1, 1), cx + 2)
    set_words(r, x_raw(C2, 1), cx + 3)

    for side in (0, 1):
        for g in range(2):
            for i, row in enumerate((0, 1)):
                lo, hi = edges + 2 * g + i, edges + 4 + 2 * g + i
                r.hz[1 + side, g, row : row + 1, :] = x_part(side, hi, 1)
                r.hz[1 + side, g, 7 - row : 8 - row, :] = x_part(side, lo, 1)

    def x_z(side, f):
        g, k = f // 4, f % 4
        shift = 4 - 2 * cx * k + (2 * cx if side else -2 * cx)
        tile = x_part(side, zrow, 8)
        tiles = [roll(tile, shift - 8 * t - 4 * g) for t in range(cy // 8)]
        return jnp.concatenate([*tiles, roll(r.hz[1 + side, g], shift)], axis=0)

    below = (r.lane == 127) | (r.lane <= 2)
    above = (r.lane >= 2 * cx + 3) & (r.lane <= 2 * cx + 6)
    for f in range(NF):
        edge = EDGE if f >= C1 else 0.0
        lo, hi = jnp.where(has_lo, x_z(0, f), edge), jnp.where(has_hi, x_z(1, f), edge)
        r.zf[f] = jnp.where(below, lo, jnp.where(above, hi, z_halo(r, f, own_z)))
    inner = r.inner[...]
    for layer in (0, 1, cx + 2, cx + 3):
        inner = collect(r, layer, inner)
    z_counts(r, inner)
    weigh(
        r,
        [
            (1, lambda f: jnp.concatenate([x_raw(f, 0), r.ht[f, 1]], axis=0)),
            (2, functools.partial(own_field, r, 0)),
            (cx + 1, functools.partial(own_field, r, cx - 1)),
            (cx + 2, lambda f: jnp.concatenate([x_raw(f, 1), r.ht[f, cx + 2]], axis=0)),
        ],
    )
    z_averages(r)

    def average_one(i, _):
        average(r, 1 + i + jnp.where(i >= 3, cx - 4, 0))
        return 0

    lax.fori_loop(0, 6, average_one, 0)

    def spread_one(x, _):
        redistribute(r, x, r.rim)
        return 0

    lax.fori_loop(0, 3, spread_one, 0)
    copies += send(r.rim, 0, 3, NFIELD)
    lax.fori_loop(cx - 3, cx, spread_one, 0)
    copies += send(r.rim, cx - 3, cx, 2 * NFIELD)
    for copy in copies:
        copy.wait()


def call(kernel, ins, outs, scratch=(), name=None, grant=8, flops=0, **kwargs):
    return pl.pallas_call(
        kernel,
        in_specs=ins,
        out_specs=tuple(pl.BlockSpec(memory_space=o.memory_space) for o in outs),
        out_shape=tuple(outs),
        scratch_shapes=scratch,
        name=name,
        cost_estimate=pl.CostEstimate(flops=flops, transcendentals=0, bytes_accessed=0),
        compiler_params=pltpu.CompilerParams(vmem_limit_bytes=grant << 20),
        **kwargs,
    )


def per_device(conserved, volume_fraction, cut_mask, merge_code):
    _, cx, cy, cz = cut_mask.shape
    devices = lax.axis_size(AXIS)
    nbx = devices // (NBY * NBZ)
    two_x = nbx > 2
    cells = cx * cy
    u = conserved.reshape(NFIELD * cells, cz)
    vf, mask, code = (a.reshape(cells, cz) for a in (volume_fraction, cut_mask, merge_code))
    f32, i32 = jnp.float32, jnp.int32
    on_chip, far = pl.BlockSpec(memory_space=pltpu.VMEM), pl.BlockSpec(memory_space=pltpu.HBM)

    def vmem(*shape, dtype=f32):
        return pltpu.VMEM((*shape, cz), dtype)

    def swap(value, stride, extent, odd):
        return lax.ppermute(value, AXIS, pairing(stride, extent, devices, odd))

    n = NF * cx
    copies = 2 if two_x else 1
    zp, u, vf, c = call(
        functools.partial(pack_kernel, cx, cy),
        [far] * 4,
        [vmem(2 * cy), vmem(NFIELD * cells), vmem(cells), vmem(cells)],
        [vmem(cells, dtype=i32), vmem(cells, dtype=i32), pltpu.SemaphoreType.DMA((3 + NFIELD,))],
        "pack",
    )(*(pltpu.with_memory_space_constraint(a, pltpu.HBM) for a in (u, vf, mask, code)))
    za, zb = swap(zp, 1, NBZ, False), swap(zp, 1, NBZ, True)
    ya, yb, *xs = call(
        functools.partial(faces_kernel, cx, cy, two_x),
        [on_chip] * 3,
        [vmem(n), vmem(n)] + [vmem(NF * cy)] * copies,
        name="faces",
        flops=1 << 20,
    )(u, vf, c)
    zh, ya, yb = call(
        functools.partial(z_merge_kernel, cx, cy), [on_chip] * 4, [vmem(2 * cy), vmem(n + 8), vmem(n + 8)], name="z_merge"
    )(za, zb, ya, yb)
    yb = swap(yb, NBZ, NBY, True)
    ya = swap(ya, NBZ, NBY, False)
    y_lo, y_hi, *xs = call(
        functools.partial(y_merge_kernel, cx, cy, two_x),
        [on_chip] * (3 + copies),
        [vmem(n + 8), vmem(n + 8)] + [vmem(NF * cy + 40)] * copies,
        name="y_merge",
    )(ya, yb, zh, *xs)
    xs = [swap(x, NBY * NBZ, nbx, odd) for odd, x in enumerate(xs)]
    xa, xb = xs if two_x else xs * 2

    rows, ring, layers = cy + 8, cy + 24, cx + 4
    kept = [
        vmem(layers, ring, dtype=i32),
        vmem(rows, dtype=i32),
        vmem(NFIELD + 1, rows),
        vmem(NFIELD + 1, layers, ring),
        vmem(NFIELD + 1, layers, ring),
        vmem(NFIELD + 1, layers, ring),
        vmem(layers, cy),
        vmem(NFIELD, layers, ring),
    ]
    scratch = [
        vmem(C2, layers, 8),
        vmem(3, 2, 8),
        vmem(NF, rows),
        vmem(rows, dtype=i32),
        vmem(cx, ring, dtype=i32),
        vmem(6 + 2 * NFIELD, ring),
        vmem(rows, dtype=i32),
        vmem(NFIELD + 1, rows),
        vmem(NFIELD, rows),
    ]
    *state, res = call(
        functools.partial(inner_kernel, cx, cy),
        [on_chip] * 6,
        kept + [vmem(NFIELD * cells)],
        scratch,
        "inner",
        flops=1 << 26,
    )(u, vf, c, zh, y_lo, y_hi)
    first = 9
    out, *_ = call(
        functools.partial(outer_kernel, cx, cy, nbx),
        [on_chip] * (first + len(kept)),
        [pltpu.HBM((NFIELD * cells, cz), f32)] + kept,
        scratch + [vmem(NFIELD * cells), pltpu.SemaphoreType.DMA((3 * NFIELD,))],
        "outer",
        flops=1 << 25,
        input_output_aliases={first + i: 1 + i for i in range(len(kept))},
    )(u, vf, c, zh, y_lo, y_hi, res, xa, xb, *state)
    return out.reshape(conserved.shape)


def solution(mesh):
    return jax.shard_map(
        per_device,
        mesh=mesh,
        in_specs=(
            P(AXIS, None, None, None, None),
            P(AXIS, None, None, None),
            P(AXIS, None, None, None),
            P(AXIS, None, None, None),
        ),
        out_specs=P(AXIS, None, None, None, None),
        check_vma=False,
    )
```

```python
import functools
import types

import jax
import jax.numpy as jnp
from jax import lax
from jax.experimental import pallas as pl
from jax.experimental.pallas import tpu as pltpu
from jax.sharding import PartitionSpec as P

NBY = 4
NBZ = 4
AXIS = "boxes"

NFIELD = 5
VF = 5
C1 = 6
C2 = 7
NF = 8
ZU, ZD, YU, YD, XU, XD = 16, 256, 4, 4096, 1 << 28, 1 << 29
LOW = (1 << 24) - 1
EDGE = 13.0


def pairing(stride, extent, devices, odd):
    pairs = []
    for i in range(devices):
        c = i // stride % extent
        partner = ((c + 1) ^ 1) - 1 if odd else c ^ 1
        pairs.append((i, i + (partner % extent - c) * stride))
    return pairs


def lanes_of(shape):
    return lax.broadcasted_iota(jnp.int32, shape, len(shape) - 1)


def roll(value, shift, axis=1):
    if isinstance(shift, int):
        shift %= value.shape[axis]
        if shift == 0:
            return value
    else:
        shift &= value.shape[axis] - 1
    return pltpu.roll(value, shift, axis)


def place():
    me = lax.axis_index(AXIS)
    return me // (NBY * NBZ), me // NBZ % NBY, me % NBZ


def pack_kernel(cx, cy, u_in, vf_in, mask_in, code_in, zp, u, vf, c, mask, code, sems):
    copies = [
        pltpu.make_async_copy(mask_in, mask, sems.at[0]),
        pltpu.make_async_copy(code_in, code, sems.at[1]),
        pltpu.make_async_copy(vf_in, vf, sems.at[2]),
    ]
    for f in range(NFIELD):
        rows = pl.ds(f * cx * cy, cx * cy)
        copies.append(pltpu.make_async_copy(u_in.at[rows, :], u.at[rows, :], sems.at[3 + f]))
    for copy in copies:
        copy.start()
    lane = lanes_of((cy, 128))
    slot = ((lane + 1) & 127) >> 1
    low_lane = (lane & 1) == 0
    copies[0].wait()
    copies[1].wait()
    for x in range(cx):
        rows = pl.ds(x * cy, cy)
        c[rows, :] = jnp.where(mask[rows, :] == 1, code[rows, :], 13).astype(jnp.float32)
    for g in (1, 0):
        acc = jnp.zeros((cy, 128), jnp.float32)
        for k in (3, 2, 1, 0):
            f = 4 * g + k
            if f <= VF:
                copies[3 + f if f < VF else 2].wait()
            for x in range(cx):
                m = cx * k + x
                rows = pl.ds(x * cy, cy)
                if f < NFIELD:
                    part = roll(u[pl.ds((f * cx + x) * cy, cy), :], 2 * m)
                elif f < C2:
                    part = roll((vf if f == VF else c)[rows, :], 2 * m)
                else:
                    part = jnp.where(low_lane, roll(c[rows, :], 2 * m - 1), roll(c[rows, :], 2 * m + 1))
                acc = jnp.where(slot == m, part, acc)
        zp[g * cy : (g + 1) * cy, :] = acc


def faces_kernel(cx, cy, two_x, u, vf, c, y_a, y_b, *xs):
    bx, by, bz = place()

    def y_face(out, high):
        rim = jnp.where(high, cy - 1, 0)
        second = jnp.where(high, cy - 2, 1)

        def column(ref, base, row):
            return ref[pl.ds(base + row, cx, stride=cy), :]

        for f in range(NFIELD):
            out[f * cx : (f + 1) * cx, :] = column(u, f * cx * cy, rim)
        out[VF * cx : (VF + 1) * cx, :] = column(vf, 0, rim)
        out[C1 * cx : (C1 + 1) * cx, :] = column(c, 0, rim)
        out[C2 * cx : (C2 + 1) * cx, :] = column(c, 0, second)

    y_face(y_a, by % 2 == 0)
    y_face(y_b, by % 2 == 1)

    def x_face(out, high):
        rim = jnp.where(high, cx - 1, 0) * cy
        second = jnp.where(high, cx - 2, 1) * cy

        def rows(base, start):
            return pl.ds(pl.multiple_of(base + start, 8), cy)

        for f in range(NFIELD):
            out[f * cy : (f + 1) * cy, :] = u[rows(f * cx * cy, rim), :]
        out[VF * cy : (VF + 1) * cy, :] = vf[rows(0, rim), :]
        out[C1 * cy : (C1 + 1) * cy, :] = c[rows(0, rim), :]
        out[C2 * cy : (C2 + 1) * cy, :] = c[rows(0, second), :]

    x_face(xs[0], bx % 2 == 0)
    if two_x:
        x_face(xs[1], bx % 2 == 1)


def z_merge_kernel(cx, cy, r_a, r_b, ya_in, yb_in, zh, y_a, y_b):
    bx, by, bz = place()
    odd = bz % 2 == 1
    lane = lanes_of((cy, 128))
    low_lane = (lane & 1) == 0
    codes = (lane >= 63) & (lane <= 126)
    for g in range(2):
        rows = slice(g * cy, (g + 1) * cy)
        a, b = r_a[rows, :], r_b[rows, :]
        edge = jnp.where(codes, EDGE, 0.0) if g else jnp.zeros((cy, 128), jnp.float32)
        low = jnp.where(bz > 0, roll(jnp.where(odd, a, b), 1), edge)
        high = jnp.where(bz < NBZ - 1, roll(jnp.where(odd, b, a), -1), edge)
        zh[rows, :] = jnp.where(low_lane, low, high)
    n = NF * cx

    def finish(out, main, high):
        out[:n, :] = main[...]
        rim = jnp.where(high, cy - 1, 0)
        second = jnp.where(high, cy - 2, 1)
        for g in range(2):
            out[n + 2 * g : n + 2 * g + 1, :] = zh[pl.ds(g * cy + rim, 1), :]
            out[n + 2 * g + 1 : n + 2 * g + 2, :] = zh[pl.ds(g * cy + second, 1), :]
        out[n + 4 : n + 8, :] = jnp.zeros((4, 128), jnp.float32)

    finish(y_a, ya_in, by % 2 == 0)
    finish(y_b, yb_in, by % 2 == 1)


def z_edge_rows(cx):
    n = NF * cx
    row = lax.broadcasted_iota(jnp.int32, (n + 8, 128), 0)
    lane = lanes_of((n + 8, 128))
    codes = ((row >= C1 * cx) & (row < n)) | ((row >= n + 2) & (lane >= 63) & (lane <= 126))
    return jnp.where(codes, EDGE, 0.0)


def y_merge_kernel(cx, cy, two_x, r_a, r_b, zh, *refs):
    copies = 2 if two_x else 1
    mains, (y_lo, y_hi), xs = refs[:copies], refs[copies : copies + 2], refs[copies + 2 :]
    bx, by, bz = place()
    odd = by % 2 == 1
    edge = z_edge_rows(cx)
    a, b = r_a[...], r_b[...]
    y_lo[...] = jnp.where(by > 0, jnp.where(odd, a, b), edge)
    y_hi[...] = jnp.where(by < NBY - 1, jnp.where(odd, b, a), edge)
    n = NF * cx

    def x_rim(out, main, high):
        rim = jnp.where(high, cx - 1, 0)
        second = jnp.where(high, cx - 2, 1)
        at = NF * cy
        out[:at, :] = main[...]
        lane = lanes_of((8, 128))
        spot = (lane - jnp.where(high, 2 * cx - 5, 2 * cx - 1)) & (2 * cx - 1)
        tile = jnp.zeros((8, 128), jnp.float32)
        for t in range(cy // 8):
            for g in range(2):
                start = 8 * t + 4 * g
                part = roll(zh[g * cy + 8 * t : g * cy + 8 * t + 8, :], start)
                tile = jnp.where((spot >= start) & (spot < start + 4), part, tile)
        out[at : at + 8, :] = tile
        at += 8
        for y in (y_lo, y_hi):
            out[at : at + 4, :] = y[n : n + 4, :]
            at += 4
        for y in (y_lo, y_hi):
            for f in range(NF):
                out[at : at + 1, :] = y[pl.ds(f * cx + rim, 1), :]
                at += 1
            for f in (C1, C2):
                out[at : at + 1, :] = y[pl.ds(f * cx + second, 1), :]
                at += 1
        out[at:, :] = jnp.zeros((out.shape[0] - at, 128), jnp.float32)

    x_rim(xs[0], mains[0], bx % 2 == 0)
    if two_x:
        x_rim(xs[1], mains[1], bx % 2 == 1)


def decode(code):
    qx = (code * 57) >> 9
    rest = code - 9 * qx
    qy = (rest * 11) >> 5
    qz = rest - 3 * qy
    word = 1 + jnp.where(qz == 2, ZU, 0) + jnp.where(qz == 0, ZD, 0)
    word = word * jnp.where(qy == 2, 1 + YU, jnp.where(qy == 0, 1 + YD, 1))
    return word | jnp.where(qx == 2, XU, jnp.where(qx == 0, XD, 0))


def on(word, bits):
    return (word & bits) == bits


def ring_store(ref, lead, value):
    n = value.shape[0]
    ref[(*lead, slice(8, 8 + n), slice(None))] = value
    ref[(*lead, slice(0, 8), slice(None))] = value[n - 8 :]


def ring_load(ref, lead, step):
    n = ref.shape[-2] - 16
    if step <= 0:
        return ref[(*lead, slice(8 + step, 8 + step + n), slice(None))]
    own = ref[(*lead, slice(8 + step, n + step), slice(None))]
    return jnp.concatenate([own, ref[(*lead, slice(step, 8 + step), slice(None))]], axis=0)


def y_rows(r, x):
    cx = r.cx
    for f in range(C2):
        r.ht[f, x + 2, 0:1, :] = r.y_hi[pl.ds(f * cx + x, 1), :]
        r.ht[f, x + 2, 7:8, :] = r.y_lo[pl.ds(f * cx + x, 1), :]
    r.ht[C1, x + 2, 1:2, :] = r.y_hi[pl.ds(C2 * cx + x, 1), :]
    r.ht[C1, x + 2, 6:7, :] = r.y_lo[pl.ds(C2 * cx + x, 1), :]


def set_words(r, own, layer):
    both = jnp.concatenate([own, r.ht[C1, layer]], axis=0)
    ring_store(r.cw, (layer,), decode(both.astype(jnp.int32)))


def z_pair(r, layer):
    return (r.lane == 2 * layer) | (r.lane == 2 * layer - 1) | ((r.lane == 127) & (layer == 0))


def collect(r, layer, acc):
    return jnp.where(z_pair(r, layer), roll(r.cw[layer, 8 : 8 + r.rows, :], 2 * layer), acc)


def z_halo(r, f, own):
    g, k = f // 4, f % 4
    return roll(own(g), 4 - 2 * r.cx * k)


def spread_counts(r, planes):
    mid = up = down = jnp.zeros((r.rows, 128), jnp.int32)
    for word, bits in planes:
        v = 1 + ((word & YU) << 6) + ((word & YD) << 4)
        if bits is not None:
            v = jnp.where((word & bits) != 0, v, 0)
        mid = mid + v
        up = up + jnp.where((word & XU) != 0, v, 0)
        down = down + jnp.where((word & XD) != 0, v, 0)
    total = mid + roll(up, 2) + roll(down, -2)
    ring_store(r.tmp_i, (0,), total)
    before, after = ring_load(r.tmp_i, (0,), -1), ring_load(r.tmp_i, (0,), 1)
    return (total & 255) + ((before >> 8) & 255) + ((after >> 16) & 255)


def z_counts(r, inner):
    outer1, outer2 = (decode(r.zf[f].astype(jnp.int32)) for f in (C1, C2))
    r.ow[...] = outer1
    z_count = spread_counts(r, ((outer1, None), (outer2, r.inward), (inner, r.outward)))
    r.i1[...] = spread_counts(r, ((outer1, r.inward),))
    z_weight = r.zf[VF] / z_count.astype(jnp.float32)
    r.zw[0] = z_weight
    for f in range(NFIELD):
        r.zw[f + 1] = z_weight * r.zf[f]


def weigh(r, group):
    rows = r.rows
    first_lane, last_lane = r.lane == 0, r.lane == 127
    totals = []
    for slot, (layer, _) in enumerate(group):
        mid, left, right = (r.cw[layer + d, 8 : 8 + rows, :] for d in (0, -1, 1))
        total = (mid & LOW) + jnp.where((left & XU) != 0, left & LOW, 0)
        ring_store(r.tmp_i, (slot,), total + jnp.where((right & XD) != 0, right & LOW, 0))
    for slot, (layer, _) in enumerate(group):
        total, before, after = (ring_load(r.tmp_i, (slot,), step) for step in (0, -1, 1))
        total = (total & 0x333) + ((before >> 2) & 0x333) + ((after >> 12) & 0x333)
        totals.append((total, roll(total, 1), roll(total, -1), roll(r.i1[...], -2 * layer)))
    for slot, (layer, field) in enumerate(group):
        total, below, above, extra = totals[slot]
        count = (total & 15) + jnp.where(first_lane, extra, (below >> 4) & 15)
        count = count + jnp.where(last_lane, extra, (above >> 8) & 15)
        inverse = 1.0 / count.astype(jnp.float32)
        r.rc[layer] = inverse[: r.cy]
        ring_store(r.h0, (0, layer), field(VF) * inverse)
    for slot, (layer, field) in enumerate(group):
        weight = ring_load(r.h0, (0, layer), 0)
        pair = z_pair(r, layer)
        for f in range(NFIELD + 1):
            w = weight
            if f:
                w = weight * field(f - 1)
                ring_store(r.h0, (f, layer), w)
            halo = roll(r.zw[f], -2 * layer)
            ring_store(r.hm, (f, layer), w + jnp.where(first_lane, halo, roll(w, 1)))
            ring_store(r.hp, (f, layer), w + jnp.where(last_lane, halo, roll(w, -1)))
            r.zi[f] = jnp.where(pair, roll(w, 2 * layer), r.zi[f])


def own_field(r, x, f):
    base = (f * r.cx + x if f < NFIELD else x) * r.cy
    ref = r.u if f < NFIELD else r.vf
    if not isinstance(base, int):
        base = pl.multiple_of(base, 8)
    return jnp.concatenate([ref[pl.ds(base, r.cy), :], r.ht[f, x + 2]], axis=0)


def z_averages(r):
    word, tmp = r.ow[...], r.tmp_f

    def pick(up, down, values):
        mid, plus, minus = values
        return mid + jnp.where((word & up) != 0, plus, jnp.where((word & down) != 0, minus, 0.0))

    sums = []
    for f in range(NFIELD + 1):
        both = r.zw[f] + r.zi[f]
        for i, value in enumerate((both, roll(both, -2), roll(both, 2))):
            ring_store(tmp, (3 * f + i,), value)
        lines = [pick(YU, YD, [ring_load(tmp, (3 * f + i,), step) for step in (0, 1, -1)]) for i in range(3)]
        sums.append(pick(XU, XD, lines))
    inverse = 1.0 / sums[0]
    first = 3 * NFIELD + 3
    for f in range(NFIELD):
        v = jnp.where((word & r.inward) != 0, sums[f + 1] * inverse, 0.0)
        totals = []
        for i, bits in enumerate((0, XU, XD)):
            w = jnp.where((word & bits) != 0, v, 0.0) if bits else v
            slot = first + 6 * f + 2 * i
            ring_store(tmp, (slot,), jnp.where((word & YU) != 0, w, 0.0))
            ring_store(tmp, (slot + 1,), jnp.where((word & YD) != 0, w, 0.0))
            totals.append(w + ring_load(tmp, (slot,), -1) + ring_load(tmp, (slot + 1,), 1))
        r.dz[f] = totals[0] + roll(totals[1], 2) + roll(totals[2], -2)


def average(r, layer):
    rows = r.rows
    tiles = rows // 8
    for t in range(tiles):
        at = 8 + 8 * t
        word = r.cw[layer, at : at + 8, :]
        zu, zd = (word & ZU) != 0, (word & ZD) != 0
        yu, yd = (word & YU) != 0, (word & YD) != 0
        xu, xd = (word & XU) != 0, (word & XD) != 0
        sums = []
        for f in range(NFIELD + 1):
            parts = []
            for d in (0, 1, -1):
                line = []
                for e in (0, 1, -1):
                    base = 0 if t == tiles - 1 and e == 1 else at
                    at_e = slice(base + e, base + e + 8)
                    v0, vm, vp = (h[f, layer + d, at_e, :] for h in (r.h0, r.hm, r.hp))
                    line.append(jnp.where(zu, vp, jnp.where(zd, vm, v0)))
                parts.append(line[0] + jnp.where(yu, line[1], jnp.where(yd, line[2], 0.0)))
            sums.append(parts[0] + jnp.where(xu, parts[1], jnp.where(xd, parts[2], 0.0)))
        inverse = 1.0 / sums[0]
        for f in range(NFIELD):
            a = sums[f + 1] * inverse
            r.av[f, layer, at : at + 8, :] = a
            if t == tiles - 1:
                r.av[f, layer, 0:8, :] = a


def redistribute(r, x, out):
    cx, cy = r.cx, r.cy
    layer = x + 2
    back = -2 * layer
    lane = lanes_of((8, 128))
    first_lane, last_lane = lane == 0, lane == 127
    for t in range(cy // 8):
        at = 8 + 8 * t
        base = [r.av[f, layer, at : at + 8, :] for f in range(NFIELD)]
        word = r.cw[layer, at : at + 8, :]
        up = [jnp.where((word & ZU) != 0, a, 0.0) for a in base]
        down = [jnp.where((word & ZD) != 0, a, 0.0) for a in base]
        for d in (0, 1, -1):
            for e in (0, 1, -1):
                if d == 0 and e == 0:
                    continue
                at_e = slice(at - e, at - e + 8)
                word = r.cw[layer - d, at_e, :]
                bits = (0, XU, XD)[d] | (0, YU, YD)[e]
                here = on(word, bits)
                here_up, here_down = on(word, bits | ZU), on(word, bits | ZD)
                for f in range(NFIELD):
                    a = r.av[f, layer - d, at_e, :]
                    base[f] = base[f] + jnp.where(here, a, 0.0)
                    up[f] = up[f] + jnp.where(here_up, a, 0.0)
                    down[f] = down[f] + jnp.where(here_down, a, 0.0)
        inverse = r.rc[layer, 8 * t : 8 * t + 8, :]
        for f in range(NFIELD):
            halo = roll(r.dz[f, 8 * t : 8 * t + 8, :], back)
            total = base[f] + jnp.where(first_lane, halo, roll(up[f], 1))
            total = total + jnp.where(last_lane, halo, roll(down[f], -1))
            out[pl.ds(pl.multiple_of((f * cx + x) * cy + 8 * t, 8), 8), :] = total * inverse


def common(r):
    r.rows = r.cy + 8
    r.lane = lanes_of((r.rows, 128))
    even = (r.lane & 1) == 0
    r.inward = jnp.where(even, ZU, ZD)
    r.outward = jnp.where(even, ZD, ZU)
    n = NF * r.cx
    for g in range(2):
        for i, row in enumerate((0, 1)):
            r.hz[0, g, row : row + 1, :] = r.y_hi[n + 2 * g + i : n + 2 * g + i + 1, :]
            r.hz[0, g, 7 - row : 8 - row, :] = r.y_lo[n + 2 * g + i : n + 2 * g + i + 1, :]

    def own_z(g):
        return jnp.concatenate([r.zh[g * r.cy : (g + 1) * r.cy, :], r.hz[0, g]], axis=0)

    return own_z


KEPT = ("cw", "inner", "zi", "zf", "h0", "hm", "hp", "rc", "av")
SCRATCH = ("ht", "hz", "ow", "tmp_i", "tmp_f", "i1", "zw", "dz")


def plan(cx, nbx, bx):
    if nbx == 2:
        high = bx == 0

        def at(j):
            return jnp.where(high, j + 1, cx + 2 - j)

        return types.SimpleNamespace(
            at=at,
            inner_weigh=[at(j) for j in range(1, cx)],
            inner_average=(1, cx - 2),
            inner_spread=(1, cx - 3),
            outer_weigh=[at(cx)],
            outer_average=[(cx - 1, 3)],
            outer_spread=[(cx - 2, 3)],
            inner_rows=(jnp.where(high, 0, 3), cx - 3),
            outer_rows=[(jnp.where(high, cx - 3, 0), 3)],
        )
    return types.SimpleNamespace(
        at=lambda j: j + 1,
        inner_weigh=range(3, cx + 1),
        inner_average=(3, cx - 4),
        inner_spread=(4, cx - 6),
        outer_weigh=[2, cx + 1],
        outer_average=[(0, 3), (cx - 1, 3)],
        outer_spread=[(1, 3), (cx - 2, 3)],
        inner_rows=(3, cx - 6),
        outer_rows=[(0, 3), (cx - 3, 3)],
    )


def x_lanes(r, high):
    below = (r.lane == 127) | (r.lane <= 2)
    above = (r.lane >= 2 * r.cx + 3) & (r.lane <= 2 * r.cx + 6)
    if isinstance(high, bool):
        return above if high else below
    return (above & high) | (below & jnp.logical_not(high))


def each(span, step):
    def body(j, _):
        step(j)
        return 0

    lax.fori_loop(span[0], span[0] + span[1], body, 0)


def inner_kernel(cx, cy, nbx, *refs):
    names = ("u", "vf", "c", "zh", "y_lo", "y_hi", *KEPT, "res", *SCRATCH)
    r = types.SimpleNamespace(cx=cx, cy=cy, **dict(zip(names, refs)))
    own_z = common(r)
    bx, by, bz = place()
    todo = plan(cx, nbx, bx)
    r.ht[...] = jnp.zeros(r.ht.shape, jnp.float32)
    for x in range(cx):
        y_rows(r, x)

    def words(x, acc):
        set_words(r, r.c[pl.ds(pl.multiple_of(x * cy, 8), cy), :], x + 2)
        return collect(r, x + 2, acc)

    inner = lax.fori_loop(0, cx, words, jnp.ones((r.rows, 128), jnp.int32), unroll=4)
    r.inner[...] = inner
    outside = x_lanes(r, bx > 0) if nbx == 2 else None
    for f in range(NF):
        value = z_halo(r, f, own_z)
        if nbx == 2:
            value = jnp.where(outside, EDGE if f >= C1 else 0.0, value)
        r.zf[f] = value
    if nbx == 2:
        edge = todo.at(0)
        ring_store(r.cw, (edge,), jnp.ones((r.rows, 128), jnp.int32))
        for f in range(NFIELD + 1):
            for h in (r.h0, r.hm, r.hp):
                ring_store(h, (f, edge), jnp.zeros((r.rows, 128), jnp.float32))
    z_counts(r, inner)
    r.zi[...] = jnp.zeros(r.zi.shape, jnp.float32)
    weigh(r, [(layer, functools.partial(own_field, r, layer - 2)) for layer in todo.inner_weigh])
    z_averages(r)
    each(todo.inner_average, lambda j: average(r, todo.at(j)))
    each(todo.inner_spread, lambda j: redistribute(r, todo.at(j) - 2, r.res))


def outer_kernel(cx, cy, nbx, *refs):
    kept_in = len(KEPT)
    names = ("u", "vf", "c", "zh", "y_lo", "y_hi", "res", "xa", "xb")
    ins = refs[: len(names)]
    rest = refs[len(names) + kept_in :]
    r = types.SimpleNamespace(cx=cx, cy=cy, **dict(zip(names, ins)))
    r.__dict__.update(zip(("out", *KEPT, *SCRATCH, "rim", "sems"), rest))
    size = cx * cy
    bx, by, bz = place()
    todo = plan(cx, nbx, bx)

    def send(src, rows, base):
        copies = []
        for f in range(NFIELD):
            part = pl.ds(pl.multiple_of(f * size + rows[0] * cy, 8), rows[1] * cy)
            copies.append(pltpu.make_async_copy(src.at[part, :], r.out.at[part, :], r.sems.at[base + f]))
        for copy in copies:
            copy.start()
        return copies

    copies = send(r.res, todo.inner_rows, 0)
    common(r)
    x_odd = bx % 2 == 1

    if nbx == 2:
        sides = [(bx == 0, True, lambda first, count: r.xa[first : first + count, :])]
    else:

        def message(high):
            def rows(first, count):
                a, b = r.xa[first : first + count, :], r.xb[first : first + count, :]
                return jnp.where(x_odd, b, a) if high else jnp.where(x_odd, a, b)

            return rows

        sides = [(False, bx > 0, message(False)), (True, bx < nbx - 1, message(True))]

    def choose(high, a, b):
        return (a if high else b) if isinstance(high, bool) else jnp.where(high, a, b)

    def present_or(present, value, edge):
        return value if present is True else jnp.where(present, value, edge)

    zrow = NF * cy
    edges = zrow + 8
    halo = []
    for high, present, part in sides:
        layer, second, own = (choose(high, a, b) for a, b in ((cx + 2, 1), (cx + 3, 0), (cx - 1, 0)))
        y_rows(r, own)

        def raw(f, present=present, part=part):
            return present_or(present, part(f * cy, cy), EDGE if f >= C1 else 0.0)

        for y, row1, row2 in ((0, 7, 6), (1, 0, 1)):
            base = edges + 8 + 10 * y

            def rim(i, edge, base=base, present=present, part=part):
                return present_or(present, part(base + i, 1), edge)

            for f in range(C1):
                r.ht[f, layer, row1 : row1 + 1, :] = rim(f, 0.0)
            r.ht[C1, layer, row1 : row1 + 1, :] = rim(C1, EDGE)
            r.ht[C1, layer, row2 : row2 + 1, :] = rim(C2, EDGE)
            r.ht[C1, second, row1 : row1 + 1, :] = rim(NF, EDGE)
            r.ht[C1, second, row2 : row2 + 1, :] = rim(NF + 1, EDGE)
        set_words(r, raw(C1), layer)
        set_words(r, raw(C2), second)
        halo.append((layer, lambda f, raw=raw, layer=layer: jnp.concatenate([raw(f), r.ht[f, layer]], axis=0)))

        for g in range(2):
            for i, row in enumerate((0, 1)):
                lo, hi = edges + 2 * g + i, edges + 4 + 2 * g + i
                r.hz[1, g, row : row + 1, :] = part(hi, 1)
                r.hz[1, g, 7 - row : 8 - row, :] = part(lo, 1)
        lanes = x_lanes(r, high)
        for f in range(NF):
            g, k = f // 4, f % 4
            shift = 4 - 2 * cx * k + choose(high, 2 * cx, -2 * cx)
            tile = part(zrow, 8)
            tiles = [roll(tile, shift - 8 * t - 4 * g) for t in range(cy // 8)]
            value = jnp.concatenate([*tiles, roll(r.hz[1, g], shift)], axis=0)
            r.zf[f] = jnp.where(lanes, present_or(present, value, EDGE if f >= C1 else 0.0), r.zf[f])
    inner = r.inner[...]
    for high, _, _ in sides:
        for a, b in ((cx + 2, 1), (cx + 3, 0)):
            inner = collect(r, choose(high, a, b), inner)
    z_counts(r, inner)
    weigh(r, [(layer, functools.partial(own_field, r, layer - 2)) for layer in todo.outer_weigh] + halo)
    z_averages(r)
    for span in todo.outer_average:
        each(span, lambda j: average(r, todo.at(j)))
    for i, (span, rows) in enumerate(zip(todo.outer_spread, todo.outer_rows)):
        each(span, lambda j: redistribute(r, todo.at(j) - 2, r.rim))
        copies += send(r.rim, rows, (1 + i) * NFIELD)
    for copy in copies:
        copy.wait()


def call(kernel, ins, outs, scratch=(), name=None, grant=8, flops=0, **kwargs):
    return pl.pallas_call(
        kernel,
        in_specs=ins,
        out_specs=tuple(pl.BlockSpec(memory_space=o.memory_space) for o in outs),
        out_shape=tuple(outs),
        scratch_shapes=scratch,
        name=name,
        cost_estimate=pl.CostEstimate(flops=flops, transcendentals=0, bytes_accessed=0),
        compiler_params=pltpu.CompilerParams(vmem_limit_bytes=grant << 20),
        **kwargs,
    )


def per_device(conserved, volume_fraction, cut_mask, merge_code):
    _, cx, cy, cz = cut_mask.shape
    devices = lax.axis_size(AXIS)
    nbx = devices // (NBY * NBZ)
    two_x = nbx > 2
    cells = cx * cy
    u = conserved.reshape(NFIELD * cells, cz)
    vf, mask, code = (a.reshape(cells, cz) for a in (volume_fraction, cut_mask, merge_code))
    f32, i32 = jnp.float32, jnp.int32
    on_chip, far = pl.BlockSpec(memory_space=pltpu.VMEM), pl.BlockSpec(memory_space=pltpu.HBM)

    def vmem(*shape, dtype=f32):
        return pltpu.VMEM((*shape, cz), dtype)

    def swap(value, stride, extent, odd):
        return lax.ppermute(value, AXIS, pairing(stride, extent, devices, odd))

    n = NF * cx
    copies = 2 if two_x else 1
    zp, u, vf, c = call(
        functools.partial(pack_kernel, cx, cy),
        [far] * 4,
        [vmem(2 * cy), vmem(NFIELD * cells), vmem(cells), vmem(cells)],
        [vmem(cells, dtype=i32), vmem(cells, dtype=i32), pltpu.SemaphoreType.DMA((3 + NFIELD,))],
        "pack",
    )(*(pltpu.with_memory_space_constraint(a, pltpu.HBM) for a in (u, vf, mask, code)))
    za, zb = swap(zp, 1, NBZ, False), swap(zp, 1, NBZ, True)
    ya, yb, *xs = call(
        functools.partial(faces_kernel, cx, cy, two_x),
        [on_chip] * 3,
        [vmem(n), vmem(n)] + [vmem(NF * cy)] * copies,
        name="faces",
        flops=1 << 20,
    )(u, vf, c)
    zh, ya, yb = call(
        functools.partial(z_merge_kernel, cx, cy), [on_chip] * 4, [vmem(2 * cy), vmem(n + 8), vmem(n + 8)], name="z_merge"
    )(za, zb, ya, yb)
    yb = swap(yb, NBZ, NBY, True)
    ya = swap(ya, NBZ, NBY, False)
    y_lo, y_hi, *xs = call(
        functools.partial(y_merge_kernel, cx, cy, two_x),
        [on_chip] * (3 + copies),
        [vmem(n + 8), vmem(n + 8)] + [vmem(NF * cy + 40)] * copies,
        name="y_merge",
    )(ya, yb, zh, *xs)
    xs = [swap(x, NBY * NBZ, nbx, odd) for odd, x in enumerate(xs)]
    xa, xb = xs if two_x else xs * 2

    rows, ring, layers = cy + 8, cy + 24, cx + 4
    kept = [
        vmem(layers, ring, dtype=i32),
        vmem(rows, dtype=i32),
        vmem(NFIELD + 1, rows),
        vmem(NF, rows),
        vmem(NFIELD + 1, layers, ring),
        vmem(NFIELD + 1, layers, ring),
        vmem(NFIELD + 1, layers, ring),
        vmem(layers, cy),
        vmem(NFIELD, layers, ring),
    ]
    scratch = [
        vmem(C2, layers, 8),
        vmem(2, 2, 8),
        vmem(rows, dtype=i32),
        vmem(cx, ring, dtype=i32),
        vmem(9 * NFIELD + 3, ring),
        vmem(rows, dtype=i32),
        vmem(NFIELD + 1, rows),
        vmem(NFIELD, rows),
    ]
    *state, res = call(
        functools.partial(inner_kernel, cx, cy, nbx),
        [on_chip] * 6,
        kept + [vmem(NFIELD * cells)],
        scratch,
        "inner",
        flops=1 << 26,
    )(u, vf, c, zh, y_lo, y_hi)
    first = 9
    out, *_ = call(
        functools.partial(outer_kernel, cx, cy, nbx),
        [on_chip] * (first + len(kept)),
        [pltpu.HBM((NFIELD * cells, cz), f32)] + kept,
        scratch + [vmem(NFIELD * cells), pltpu.SemaphoreType.DMA((3 * NFIELD,))],
        "outer",
        flops=1 << 25,
        input_output_aliases={first + i: 1 + i for i in range(len(kept))},
    )(u, vf, c, zh, y_lo, y_hi, res, xa, xb, *state)
    return out.reshape(conserved.shape)


def solution(mesh):
    return jax.shard_map(
        per_device,
        mesh=mesh,
        in_specs=(
            P(AXIS, None, None, None, None),
            P(AXIS, None, None, None),
            P(AXIS, None, None, None),
            P(AXIS, None, None, None),
        ),
        out_specs=P(AXIS, None, None, None, None),
        check_vma=False,
    )
```

```python
import functools
import types

import jax
import jax.numpy as jnp
from jax import lax
from jax.experimental import pallas as pl
from jax.experimental.pallas import tpu as pltpu
from jax.sharding import PartitionSpec as P

NBY = 4
NBZ = 4
AXIS = "boxes"

NFIELD = 5
VF = 5
C1 = 6
C2 = 7
NF = 8
ZU, ZD, YU, YD, XU, XD = 16, 256, 4, 4096, 1 << 28, 1 << 29
LOW = (1 << 24) - 1
EDGE = 13.0


def pairing(stride, extent, devices, odd):
    pairs = []
    for i in range(devices):
        c = i // stride % extent
        partner = ((c + 1) ^ 1) - 1 if odd else c ^ 1
        pairs.append((i, i + (partner % extent - c) * stride))
    return pairs


def lanes_of(shape):
    return lax.broadcasted_iota(jnp.int32, shape, len(shape) - 1)


def roll(value, shift, axis=1):
    if isinstance(shift, int):
        shift %= value.shape[axis]
        if shift == 0:
            return value
    else:
        shift &= value.shape[axis] - 1
    return pltpu.roll(value, shift, axis)


def place():
    me = lax.axis_index(AXIS)
    return me // (NBY * NBZ), me // NBZ % NBY, me % NBZ


def decode(code):
    qx = (code * 57) >> 9
    rest = code - 9 * qx
    qy = (rest * 11) >> 5
    qz = rest - 3 * qy
    word = 1 + jnp.where(qz == 2, ZU, 0) + jnp.where(qz == 0, ZD, 0)
    word = word * jnp.where(qy == 2, 1 + YU, jnp.where(qy == 0, 1 + YD, 1))
    return word | jnp.where(qx == 2, XU, jnp.where(qx == 0, XD, 0))


def on(word, bits):
    return (word & bits) == bits


def ring_store(ref, lead, value):
    n = value.shape[0]
    ref[(*lead, slice(8, 8 + n), slice(None))] = value
    ref[(*lead, slice(0, 8), slice(None))] = value[n - 8 :]


def ring_load(ref, lead, step):
    n = ref.shape[-2] - 16
    if step <= 0:
        return ref[(*lead, slice(8 + step, 8 + step + n), slice(None))]
    own = ref[(*lead, slice(8 + step, n + step), slice(None))]
    return jnp.concatenate([own, ref[(*lead, slice(step, 8 + step), slice(None))]], axis=0)


def pack_kernel(cx, cy, u_in, vf_in, mask_in, code_in, zp, u, vf, c, mask, code, sems):
    copies = [
        pltpu.make_async_copy(mask_in, mask, sems.at[0]),
        pltpu.make_async_copy(code_in, code, sems.at[1]),
        pltpu.make_async_copy(vf_in, vf, sems.at[2]),
    ]
    for f in range(NFIELD):
        rows = pl.ds(f * cx * cy, cx * cy)
        copies.append(pltpu.make_async_copy(u_in.at[rows, :], u.at[rows, :], sems.at[3 + f]))
    for copy in copies:
        copy.start()
    lane = lanes_of((cy, 128))
    slot = ((lane + 1) & 127) >> 1
    low_lane = (lane & 1) == 0
    copies[0].wait()
    copies[1].wait()
    for x in range(cx):
        rows = pl.ds(x * cy, cy)
        c[rows, :] = jnp.where(mask[rows, :] == 1, code[rows, :], 13).astype(jnp.float32)
    for g in (1, 0):
        acc = jnp.zeros((cy, 128), jnp.float32)
        for k in (3, 2, 1, 0):
            f = 4 * g + k
            if f <= VF:
                copies[3 + f if f < VF else 2].wait()
            for x in range(cx):
                m = cx * k + x
                rows = pl.ds(x * cy, cy)
                if f < NFIELD:
                    part = roll(u[pl.ds((f * cx + x) * cy, cy), :], 2 * m)
                elif f < C2:
                    part = roll((vf if f == VF else c)[rows, :], 2 * m)
                else:
                    part = jnp.where(low_lane, roll(c[rows, :], 2 * m - 1), roll(c[rows, :], 2 * m + 1))
                acc = jnp.where(slot == m, part, acc)
        zp[g * cy : (g + 1) * cy, :] = acc


def faces_kernel(cx, cy, two_x, u, vf, c, cw, y_a, y_b, *xs):
    bx, by, bz = place()
    for x in range(cx):
        cw[x + 2, 8 : 8 + cy, :] = decode(c[x * cy : (x + 1) * cy, :].astype(jnp.int32))

    def y_face(out, high):
        rim = jnp.where(high, cy - 1, 0)
        second = jnp.where(high, cy - 2, 1)

        def column(ref, base, row):
            return ref[pl.ds(base + row, cx, stride=cy), :]

        for f in range(NFIELD):
            out[f * cx : (f + 1) * cx, :] = column(u, f * cx * cy, rim)
        out[VF * cx : (VF + 1) * cx, :] = column(vf, 0, rim)
        out[C1 * cx : (C1 + 1) * cx, :] = column(c, 0, rim)
        out[C2 * cx : (C2 + 1) * cx, :] = column(c, 0, second)

    y_face(y_a, by % 2 == 0)
    y_face(y_b, by % 2 == 1)

    def x_face(out, high):
        rim = jnp.where(high, cx - 1, 0) * cy
        second = jnp.where(high, cx - 2, 1) * cy

        def rows(base, start):
            return pl.ds(pl.multiple_of(base + start, 8), cy)

        for f in range(NFIELD):
            out[f * cy : (f + 1) * cy, :] = u[rows(f * cx * cy, rim), :]
        out[VF * cy : (VF + 1) * cy, :] = vf[rows(0, rim), :]
        out[C1 * cy : (C1 + 1) * cy, :] = c[rows(0, rim), :]
        out[C2 * cy : (C2 + 1) * cy, :] = c[rows(0, second), :]

    x_face(xs[0], bx % 2 == 0)
    if two_x:
        x_face(xs[1], bx % 2 == 1)


def z_merge_kernel(cx, cy, r_a, r_b, zp, ya_in, yb_in, zh, y_a, y_b):
    bx, by, bz = place()
    odd = bz % 2 == 1
    lane = lanes_of((cy, 128))
    low_lane = (lane & 1) == 0
    codes = (lane >= 63) & (lane <= 126)
    for g in range(2):
        rows = slice(g * cy, (g + 1) * cy)
        a, b = r_a[rows, :], r_b[rows, :]
        edge = jnp.where(codes, EDGE, 0.0) if g else jnp.zeros((cy, 128), jnp.float32)
        low = jnp.where(bz > 0, roll(jnp.where(odd, a, b), 1), edge)
        high = jnp.where(bz < NBZ - 1, roll(jnp.where(odd, b, a), -1), edge)
        zh[rows, :] = jnp.where(low_lane, low, high)
    zh[2 * cy :, :] = zp[...]
    n = NF * cx

    def finish(out, main, high):
        out[:n, :] = main[...]
        rim = jnp.where(high, cy - 1, 0)
        second = jnp.where(high, cy - 2, 1)
        for g in range(4):
            out[n + 2 * g : n + 2 * g + 1, :] = zh[pl.ds(g * cy + rim, 1), :]
            out[n + 2 * g + 1 : n + 2 * g + 2, :] = zh[pl.ds(g * cy + second, 1), :]

    finish(y_a, ya_in, by % 2 == 0)
    finish(y_b, yb_in, by % 2 == 1)


def z_edge_rows(cx):
    n = NF * cx
    row = lax.broadcasted_iota(jnp.int32, (n + 8, 128), 0)
    lane = lanes_of((n + 8, 128))
    codes = ((row >= C1 * cx) & (row < n)) | ((row >= n) & ((row & 2) != 0) & (lane >= 63) & (lane <= 126))
    return jnp.where(codes, EDGE, 0.0)


def y_merge_kernel(cx, cy, two_x, r_a, r_b, zh, *refs):
    copies = 2 if two_x else 1
    mains, (y_lo, y_hi), xs = refs[:copies], refs[copies : copies + 2], refs[copies + 2 :]
    bx, by, bz = place()
    odd = by % 2 == 1
    edge = z_edge_rows(cx)
    a, b = r_a[...], r_b[...]
    y_lo[...] = jnp.where(by > 0, jnp.where(odd, a, b), edge)
    y_hi[...] = jnp.where(by < NBY - 1, jnp.where(odd, b, a), edge)
    n = NF * cx

    def x_rim(out, main, high):
        rim = jnp.where(high, cx - 1, 0)
        second = jnp.where(high, cx - 2, 1)
        at = NF * cy
        out[:at, :] = main[...]
        lane = lanes_of((8, 128))
        spot = (lane - jnp.where(high, 2 * cx - 5, 2 * cx - 1)) & (2 * cx - 1)
        for half in range(2):
            tile = jnp.zeros((8, 128), jnp.float32)
            for t in range(cy // 8):
                for g in range(2):
                    start, row = 8 * t + 4 * g, (2 * half + g) * cy + 8 * t
                    tile = jnp.where((spot >= start) & (spot < start + 4), roll(zh[row : row + 8, :], start), tile)
            out[at : at + 8, :] = tile
            at += 8
        for y in (y_lo, y_hi):
            out[at : at + 8, :] = y[n : n + 8, :]
            at += 8
        for y in (y_lo, y_hi):
            for f in range(NF):
                out[at : at + 1, :] = y[pl.ds(f * cx + rim, 1), :]
                at += 1
            for f in (C1, C2):
                out[at : at + 1, :] = y[pl.ds(f * cx + second, 1), :]
                at += 1
        out[at:, :] = jnp.zeros((out.shape[0] - at, 128), jnp.float32)

    x_rim(xs[0], mains[0], bx % 2 == 0)
    if two_x:
        x_rim(xs[1], mains[1], bx % 2 == 1)


def y_rows(r, x):
    cx = r.cx
    for f in range(C2):
        r.ht[f, x + 2, 0:1, :] = r.y_hi[pl.ds(f * cx + x, 1), :]
        r.ht[f, x + 2, 7:8, :] = r.y_lo[pl.ds(f * cx + x, 1), :]
    r.ht[C1, x + 2, 1:2, :] = r.y_hi[pl.ds(C2 * cx + x, 1), :]
    r.ht[C1, x + 2, 6:7, :] = r.y_lo[pl.ds(C2 * cx + x, 1), :]


def set_words(r, own, layer):
    both = jnp.concatenate([own, r.ht[C1, layer]], axis=0)
    ring_store(r.cw, (layer,), decode(both.astype(jnp.int32)))


def set_halo_words(r, layer):
    words = decode(r.ht[C1, layer].astype(jnp.int32))
    r.cw[layer, 0:8, :] = words
    r.cw[layer, 8 + r.cy : 16 + r.cy, :] = words


def z_halo(r, f, own):
    g, k = f // 4, f % 4
    return roll(own(g), 4 - 2 * r.cx * k)


def spread_counts(r, planes, slot):
    mid = up = down = jnp.zeros((r.rows, 128), jnp.int32)
    for word, bits in planes:
        v = 1 + ((word & YU) << 6) + ((word & YD) << 4)
        if bits is not None:
            v = jnp.where((word & bits) != 0, v, 0)
        mid = mid + v
        up = up + jnp.where((word & XU) != 0, v, 0)
        down = down + jnp.where((word & XD) != 0, v, 0)
    total = mid + roll(up, 2) + roll(down, -2)
    ring_store(r.tmp_i, (slot,), total)
    before, after = ring_load(r.tmp_i, (slot,), -1), ring_load(r.tmp_i, (slot,), 1)
    return (total & 255) + ((before >> 8) & 255) + ((after >> 16) & 255)


def z_counts(r):
    outer1, outer2, inner1, inner2 = (decode(r.zf[f].astype(jnp.int32)) for f in (C1, C2, NF + C1, NF + C2))
    r.ow[...], r.iw[...] = outer1, inner1
    planes = ((outer1, None), (outer2, r.inward), (inner1, r.outward)), ((inner1, None), (outer1, r.inward), (inner2, r.outward))
    for first, out, plane in zip((0, NF), (r.zw, r.zi), planes):
        inverse = 1.0 / spread_counts(r, plane, first // NF).astype(jnp.float32)
        weight = r.zf[first + VF] * inverse
        out[0] = weight
        for f in range(NFIELD):
            out[f + 1] = weight * r.zf[first + f]
    r.ci[...] = inverse


def weigh(r, group):
    rows = r.rows
    edge_lane = (r.lane == 0) | (r.lane == 127)
    totals = []
    for slot, (layer, _) in enumerate(group, 2):
        mid, left, right = (r.cw[layer + d, 8 : 8 + rows, :] for d in (0, -1, 1))
        total = (mid & LOW) + jnp.where((left & XU) != 0, left & LOW, 0)
        ring_store(r.tmp_i, (slot,), total + jnp.where((right & XD) != 0, right & LOW, 0))
    for slot, (layer, _) in enumerate(group, 2):
        total, before, after = (ring_load(r.tmp_i, (slot,), step) for step in (0, -1, 1))
        total = (total & 0x333) + ((before >> 2) & 0x333) + ((after >> 12) & 0x333)
        totals.append((total, roll(total, 1), roll(total, -1), roll(r.ci[...], -2 * layer)))
    for (layer, field), (total, below, above, edge) in zip(group, totals):
        count = (total & 15) + ((below >> 4) & 15) + ((above >> 8) & 15)
        inverse = jnp.where(edge_lane, edge, 1.0 / count.astype(jnp.float32))
        r.rc[layer] = inverse[: r.cy]
        ring_store(r.h0, (0, layer), field(VF) * inverse)
    for layer, field in group:
        weight = ring_load(r.h0, (0, layer), 0)
        for f in range(NFIELD + 1):
            w = weight
            if f:
                w = weight * field(f - 1)
                ring_store(r.h0, (f, layer), w)
            ring_store(r.hm, (f, layer), w + roll(w, 1))
            ring_store(r.hp, (f, layer), w + roll(w, -1))


def own_field(r, x, f):
    base = (f * r.cx + x if f < NFIELD else x) * r.cy
    ref = r.u if f < NFIELD else r.vf
    if not isinstance(base, int):
        base = pl.multiple_of(base, 8)
    return jnp.concatenate([ref[pl.ds(base, r.cy), :], r.ht[f, x + 2]], axis=0)


def z_averages(r):
    tmp = r.tmp_f

    def pick(word, up, down, values):
        mid, plus, minus = values
        return mid + jnp.where((word & up) != 0, plus, jnp.where((word & down) != 0, minus, 0.0))

    sums, inner_sums = [], []
    for f in range(NFIELD + 1):
        both = r.zw[f] + r.zi[f]
        for i, value in enumerate((both, roll(both, -2), roll(both, 2))):
            ring_store(tmp, (3 * f + i,), value)
        around = [[ring_load(tmp, (3 * f + i,), step) for step in (0, 1, -1)] for i in range(3)]
        for word, out in ((r.ow[...], sums), (r.iw[...], inner_sums)):
            out.append(pick(word, XU, XD, [pick(word, YU, YD, line) for line in around]))
    inverse = 1.0 / inner_sums[0]
    for f in range(NFIELD):
        r.ai[f] = inner_sums[f + 1] * inverse
    word = r.ow[...]
    inverse = 1.0 / sums[0]
    first = 3 * NFIELD + 3
    for f in range(NFIELD):
        v = jnp.where((word & r.inward) != 0, sums[f + 1] * inverse, 0.0)
        totals = []
        for i, bits in enumerate((0, XU, XD)):
            w = jnp.where((word & bits) != 0, v, 0.0) if bits else v
            slot = first + 6 * f + 2 * i
            ring_store(tmp, (slot,), jnp.where((word & YU) != 0, w, 0.0))
            ring_store(tmp, (slot + 1,), jnp.where((word & YD) != 0, w, 0.0))
            totals.append(w + ring_load(tmp, (slot,), -1) + ring_load(tmp, (slot + 1,), 1))
        r.dz[f] = totals[0] + roll(totals[1], 2) + roll(totals[2], -2)


def average(r, layer):
    rows = r.rows
    tiles = rows // 8
    lane = lanes_of((8, 128))
    for t in range(tiles):
        at = 8 + 8 * t
        word = r.cw[layer, at : at + 8, :]
        zu, zd = (word & ZU) != 0, (word & ZD) != 0
        yu, yd = (word & YU) != 0, (word & YD) != 0
        xu, xd = (word & XU) != 0, (word & XD) != 0
        sums = []
        for f in range(NFIELD + 1):
            parts = []
            for d in (0, 1, -1):
                line = []
                for e in (0, 1, -1):
                    base = 0 if t == tiles - 1 and e == 1 else at
                    at_e = slice(base + e, base + e + 8)
                    v0, vm, vp = (h[f, layer + d, at_e, :] for h in (r.h0, r.hm, r.hp))
                    line.append(jnp.where(zu, vp, jnp.where(zd, vm, v0)))
                parts.append(line[0] + jnp.where(yu, line[1], jnp.where(yd, line[2], 0.0)))
            sums.append(parts[0] + jnp.where(xu, parts[1], jnp.where(xd, parts[2], 0.0)))
        inverse = 1.0 / sums[0]
        leaves = ((lane == 0) & zd) | ((lane == 127) & zu)
        for f in range(NFIELD):
            column = roll(r.ai[f, 8 * t : 8 * t + 8, :], -2 * layer)
            a = jnp.where(leaves, column, sums[f + 1] * inverse)
            r.av[f, layer, at : at + 8, :] = a
            if t == tiles - 1:
                r.av[f, layer, 0:8, :] = a


def redistribute(r, x, out):
    cx, cy = r.cx, r.cy
    layer = x + 2
    back = -2 * layer
    lane = lanes_of((8, 128))
    first_lane, last_lane = lane == 0, lane == 127
    for t in range(cy // 8):
        at = 8 + 8 * t
        base = [r.av[f, layer, at : at + 8, :] for f in range(NFIELD)]
        word = r.cw[layer, at : at + 8, :]
        up = [jnp.where((word & ZU) != 0, a, 0.0) for a in base]
        down = [jnp.where((word & ZD) != 0, a, 0.0) for a in base]
        for d in (0, 1, -1):
            for e in (0, 1, -1):
                if d == 0 and e == 0:
                    continue
                at_e = slice(at - e, at - e + 8)
                word = r.cw[layer - d, at_e, :]
                bits = (0, XU, XD)[d] | (0, YU, YD)[e]
                here = on(word, bits)
                here_up, here_down = on(word, bits | ZU), on(word, bits | ZD)
                for f in range(NFIELD):
                    a = r.av[f, layer - d, at_e, :]
                    base[f] = base[f] + jnp.where(here, a, 0.0)
                    up[f] = up[f] + jnp.where(here_up, a, 0.0)
                    down[f] = down[f] + jnp.where(here_down, a, 0.0)
        inverse = r.rc[layer, 8 * t : 8 * t + 8, :]
        for f in range(NFIELD):
            halo = roll(r.dz[f, 8 * t : 8 * t + 8, :], back)
            total = base[f] + jnp.where(first_lane, halo, roll(up[f], 1))
            total = total + jnp.where(last_lane, halo, roll(down[f], -1))
            out[pl.ds(pl.multiple_of((f * cx + x) * cy + 8 * t, 8), 8), :] = total * inverse


def common(r):
    r.rows = r.cy + 8
    r.lane = lanes_of((r.rows, 128))
    even = (r.lane & 1) == 0
    r.inward = jnp.where(even, ZU, ZD)
    r.outward = jnp.where(even, ZD, ZU)
    n = NF * r.cx
    for g in range(4):
        for i, row in enumerate((0, 1)):
            r.hz[0, g, row : row + 1, :] = r.y_hi[n + 2 * g + i : n + 2 * g + i + 1, :]
            r.hz[0, g, 7 - row : 8 - row, :] = r.y_lo[n + 2 * g + i : n + 2 * g + i + 1, :]

    def own_z(g):
        return jnp.concatenate([r.zh[g * r.cy : (g + 1) * r.cy, :], r.hz[0, g]], axis=0)

    return own_z


KEPT = ("cw", "zf", "h0", "hm", "hp", "rc", "av")
SCRATCH = ("ht", "hz", "ow", "iw", "tmp_i", "tmp_f", "ci", "zw", "zi", "ai", "dz")


def plan(cx, nbx, bx):
    if nbx == 2:
        high = bx == 0

        def at(j):
            return jnp.where(high, j + 1, cx + 2 - j)

        return types.SimpleNamespace(
            at=at,
            inner_weigh=[at(j) for j in range(1, cx)],
            inner_average=(1, cx - 2),
            inner_spread=(1, cx - 3),
            outer_weigh=[at(cx)],
            outer_average=[(cx - 1, 3)],
            outer_spread=[(cx - 2, 3)],
            inner_rows=(jnp.where(high, 0, 3), cx - 3),
            outer_rows=[(jnp.where(high, cx - 3, 0), 3)],
        )
    return types.SimpleNamespace(
        at=lambda j: j + 1,
        inner_weigh=range(3, cx + 1),
        inner_average=(3, cx - 4),
        inner_spread=(4, cx - 6),
        outer_weigh=[2, cx + 1],
        outer_average=[(0, 3), (cx - 1, 3)],
        outer_spread=[(1, 3), (cx - 2, 3)],
        inner_rows=(3, cx - 6),
        outer_rows=[(0, 3), (cx - 3, 3)],
    )


def x_lanes(r, high):
    below = (r.lane == 127) | (r.lane <= 2)
    above = (r.lane >= 2 * r.cx + 3) & (r.lane <= 2 * r.cx + 6)
    if isinstance(high, bool):
        return above if high else below
    return (above & high) | (below & jnp.logical_not(high))


def each(span, step):
    def body(j, _):
        step(j)
        return 0

    lax.fori_loop(span[0], span[0] + span[1], body, 0)


def inner_kernel(cx, cy, nbx, *refs):
    names = ("u", "vf", "zh", "y_lo", "y_hi", "cw_in", *KEPT, "res", *SCRATCH)
    r = types.SimpleNamespace(cx=cx, cy=cy, **dict(zip(names, refs)))
    own_z = common(r)
    bx, by, bz = place()
    todo = plan(cx, nbx, bx)
    r.ht[...] = jnp.zeros(r.ht.shape, jnp.float32)
    for x in range(cx):
        y_rows(r, x)

    for x in range(cx):
        set_halo_words(r, x + 2)
    outside = x_lanes(r, bx > 0) if nbx == 2 else None
    for f in range(2 * NF):
        value = z_halo(r, f, own_z)
        if nbx == 2:
            value = jnp.where(outside, EDGE if f % NF >= C1 else 0.0, value)
        r.zf[f] = value
    if nbx == 2:
        edge = todo.at(0)
        ring_store(r.cw, (edge,), jnp.ones((r.rows, 128), jnp.int32))
        for f in range(NFIELD + 1):
            for h in (r.h0, r.hm, r.hp):
                ring_store(h, (f, edge), jnp.zeros((r.rows, 128), jnp.float32))
    z_counts(r)
    weigh(r, [(layer, functools.partial(own_field, r, layer - 2)) for layer in todo.inner_weigh])
    z_averages(r)
    each(todo.inner_average, lambda j: average(r, todo.at(j)))
    each(todo.inner_spread, lambda j: redistribute(r, todo.at(j) - 2, r.res))


def outer_kernel(cx, cy, nbx, *refs):
    kept_in = len(KEPT)
    names = ("u", "vf", "zh", "y_lo", "y_hi", "res", "xa", "xb")
    ins = refs[: len(names)]
    rest = refs[len(names) + kept_in :]
    r = types.SimpleNamespace(cx=cx, cy=cy, **dict(zip(names, ins)))
    r.__dict__.update(zip(("out", *KEPT, *SCRATCH, "rim", "sems"), rest))
    size = cx * cy
    bx, by, bz = place()
    todo = plan(cx, nbx, bx)

    def send(src, rows, base):
        copies = []
        for f in range(NFIELD):
            part = pl.ds(pl.multiple_of(f * size + rows[0] * cy, 8), rows[1] * cy)
            copies.append(pltpu.make_async_copy(src.at[part, :], r.out.at[part, :], r.sems.at[base + f]))
        for copy in copies:
            copy.start()
        return copies

    copies = send(r.res, todo.inner_rows, 0)
    common(r)
    x_odd = bx % 2 == 1

    if nbx == 2:
        sides = [(bx == 0, True, lambda first, count: r.xa[first : first + count, :])]
    else:

        def message(high):
            def rows(first, count):
                a, b = r.xa[first : first + count, :], r.xb[first : first + count, :]
                return jnp.where(x_odd, b, a) if high else jnp.where(x_odd, a, b)

            return rows

        sides = [(False, bx > 0, message(False)), (True, bx < nbx - 1, message(True))]

    def choose(high, a, b):
        return (a if high else b) if isinstance(high, bool) else jnp.where(high, a, b)

    def present_or(present, value, edge):
        return value if present is True else jnp.where(present, value, edge)

    zrow = NF * cy
    edges = zrow + 16
    halo = []
    for high, present, part in sides:
        layer, second, own = (choose(high, a, b) for a, b in ((cx + 2, 1), (cx + 3, 0), (cx - 1, 0)))
        y_rows(r, own)

        def raw(f, present=present, part=part):
            return present_or(present, part(f * cy, cy), EDGE if f >= C1 else 0.0)

        for y, row1, row2 in ((0, 7, 6), (1, 0, 1)):
            base = edges + 16 + 10 * y

            def rim(i, edge, base=base, present=present, part=part):
                return present_or(present, part(base + i, 1), edge)

            for f in range(C1):
                r.ht[f, layer, row1 : row1 + 1, :] = rim(f, 0.0)
            r.ht[C1, layer, row1 : row1 + 1, :] = rim(C1, EDGE)
            r.ht[C1, layer, row2 : row2 + 1, :] = rim(C2, EDGE)
            r.ht[C1, second, row1 : row1 + 1, :] = rim(NF, EDGE)
            r.ht[C1, second, row2 : row2 + 1, :] = rim(NF + 1, EDGE)
        set_words(r, raw(C1), layer)
        set_words(r, raw(C2), second)
        halo.append((layer, lambda f, raw=raw, layer=layer: jnp.concatenate([raw(f), r.ht[f, layer]], axis=0)))

        for g in range(4):
            for i, row in enumerate((0, 1)):
                lo, hi = edges + 2 * g + i, edges + 8 + 2 * g + i
                r.hz[1, g, row : row + 1, :] = part(hi, 1)
                r.hz[1, g, 7 - row : 8 - row, :] = part(lo, 1)
        lanes = x_lanes(r, high)
        for f in range(2 * NF):
            g, k = f // 4, f % 4
            shift = 4 - 2 * cx * k + choose(high, 2 * cx, -2 * cx)
            tile = part(zrow + 8 * (g // 2), 8)
            tiles = [roll(tile, shift - 8 * t - 4 * (g % 2)) for t in range(cy // 8)]
            value = jnp.concatenate([*tiles, roll(r.hz[1, g], shift)], axis=0)
            r.zf[f] = jnp.where(lanes, present_or(present, value, EDGE if f % NF >= C1 else 0.0), r.zf[f])
    z_counts(r)
    weigh(r, [(layer, functools.partial(own_field, r, layer - 2)) for layer in todo.outer_weigh] + halo)
    z_averages(r)
    for span in todo.outer_average:
        each(span, lambda j: average(r, todo.at(j)))
    for i, (span, rows) in enumerate(zip(todo.outer_spread, todo.outer_rows)):
        each(span, lambda j: redistribute(r, todo.at(j) - 2, r.rim))
        copies += send(r.rim, rows, (1 + i) * NFIELD)
    for copy in copies:
        copy.wait()


def call(kernel, ins, outs, scratch=(), name=None, grant=8, flops=0, **kwargs):
    return pl.pallas_call(
        kernel,
        in_specs=ins,
        out_specs=tuple(pl.BlockSpec(memory_space=o.memory_space) for o in outs),
        out_shape=tuple(outs),
        scratch_shapes=scratch,
        name=name,
        cost_estimate=pl.CostEstimate(flops=flops, transcendentals=0, bytes_accessed=0),
        compiler_params=pltpu.CompilerParams(vmem_limit_bytes=grant << 20),
        **kwargs,
    )


def per_device(conserved, volume_fraction, cut_mask, merge_code):
    _, cx, cy, cz = cut_mask.shape
    devices = lax.axis_size(AXIS)
    nbx = devices // (NBY * NBZ)
    two_x = nbx > 2
    cells = cx * cy
    u = conserved.reshape(NFIELD * cells, cz)
    vf, mask, code = (a.reshape(cells, cz) for a in (volume_fraction, cut_mask, merge_code))
    f32, i32 = jnp.float32, jnp.int32
    on_chip, far = pl.BlockSpec(memory_space=pltpu.VMEM), pl.BlockSpec(memory_space=pltpu.HBM)

    def vmem(*shape, dtype=f32):
        return pltpu.VMEM((*shape, cz), dtype)

    def swap(value, stride, extent, odd):
        return lax.ppermute(value, AXIS, pairing(stride, extent, devices, odd))

    n = NF * cx
    copies = 2 if two_x else 1
    zp, u, vf, c = call(
        functools.partial(pack_kernel, cx, cy),
        [far] * 4,
        [vmem(2 * cy), vmem(NFIELD * cells), vmem(cells), vmem(cells)],
        [vmem(cells, dtype=i32), vmem(cells, dtype=i32), pltpu.SemaphoreType.DMA((3 + NFIELD,))],
        "pack",
    )(*(pltpu.with_memory_space_constraint(a, pltpu.HBM) for a in (u, vf, mask, code)))
    za, zb = swap(zp, 1, NBZ, False), swap(zp, 1, NBZ, True)
    rows, ring, layers = cy + 8, cy + 24, cx + 4
    cw, ya, yb, *xs = call(
        functools.partial(faces_kernel, cx, cy, two_x),
        [on_chip] * 3,
        [vmem(layers, ring, dtype=i32), vmem(n), vmem(n)] + [vmem(NF * cy)] * copies,
        name="faces",
        flops=1 << 20,
    )(u, vf, c)
    zh, ya, yb = call(
        functools.partial(z_merge_kernel, cx, cy), [on_chip] * 5, [vmem(4 * cy), vmem(n + 8), vmem(n + 8)], name="z_merge"
    )(za, zb, zp, ya, yb)
    yb = swap(yb, NBZ, NBY, True)
    ya = swap(ya, NBZ, NBY, False)
    y_lo, y_hi, *xs = call(
        functools.partial(y_merge_kernel, cx, cy, two_x),
        [on_chip] * (3 + copies),
        [vmem(n + 8), vmem(n + 8)] + [vmem(NF * cy + 56)] * copies,
        name="y_merge",
    )(ya, yb, zh, *xs)
    xs = [swap(x, NBY * NBZ, nbx, odd) for odd, x in enumerate(xs)]
    xa, xb = xs if two_x else xs * 2

    kept = [
        vmem(layers, ring, dtype=i32),
        vmem(2 * NF, rows),
        vmem(NFIELD + 1, layers, ring),
        vmem(NFIELD + 1, layers, ring),
        vmem(NFIELD + 1, layers, ring),
        vmem(layers, cy),
        vmem(NFIELD, layers, ring),
    ]
    scratch = [
        vmem(C2, layers, 8),
        vmem(2, 4, 8),
        vmem(rows, dtype=i32),
        vmem(rows, dtype=i32),
        vmem(layers, ring, dtype=i32),
        vmem(9 * NFIELD + 3, ring),
        vmem(rows),
        vmem(NFIELD + 1, rows),
        vmem(NFIELD + 1, rows),
        vmem(NFIELD, rows),
        vmem(NFIELD, rows),
    ]
    *state, res = call(
        functools.partial(inner_kernel, cx, cy, nbx),
        [on_chip] * 6,
        kept + [vmem(NFIELD * cells)],
        scratch,
        "inner",
        flops=1 << 26,
        input_output_aliases={5: 0},
    )(u, vf, zh, y_lo, y_hi, cw)
    first = 8
    out, *_ = call(
        functools.partial(outer_kernel, cx, cy, nbx),
        [on_chip] * (first + len(kept)),
        [pltpu.HBM((NFIELD * cells, cz), f32)] + kept,
        scratch + [vmem(NFIELD * cells), pltpu.SemaphoreType.DMA((3 * NFIELD,))],
        "outer",
        flops=1 << 25,
        input_output_aliases={first + i: 1 + i for i in range(len(kept))},
    )(u, vf, zh, y_lo, y_hi, res, xa, xb, *state)
    return out.reshape(conserved.shape)


def solution(mesh):
    return jax.shard_map(
        per_device,
        mesh=mesh,
        in_specs=(
            P(AXIS, None, None, None, None),
            P(AXIS, None, None, None),
            P(AXIS, None, None, None),
            P(AXIS, None, None, None),
        ),
        out_specs=P(AXIS, None, None, None, None),
        check_vma=False,
    )
```

```python
import functools
import types

import jax
import jax.numpy as jnp
from jax import lax
from jax.experimental import pallas as pl
from jax.experimental.pallas import tpu as pltpu
from jax.sharding import PartitionSpec as P

NBY = 4
NBZ = 4
AXIS = "boxes"

NFIELD = 5
VF = 5
C1 = 6
C2 = 7
NF = 8
ZU, ZD, YU, YD, XU, XD = 16, 256, 4, 4096, 1 << 28, 1 << 29
LOW = (1 << 24) - 1
EDGE = 13.0


def pairing(stride, extent, devices, odd):
    pairs = []
    for i in range(devices):
        c = i // stride % extent
        partner = ((c + 1) ^ 1) - 1 if odd else c ^ 1
        pairs.append((i, i + (partner % extent - c) * stride))
    return pairs


def lanes_of(shape):
    return lax.broadcasted_iota(jnp.int32, shape, len(shape) - 1)


def roll(value, shift, axis=1):
    if isinstance(shift, int):
        shift %= value.shape[axis]
        if shift == 0:
            return value
    else:
        shift &= value.shape[axis] - 1
    return pltpu.roll(value, shift, axis)


def place():
    me = lax.axis_index(AXIS)
    return me // (NBY * NBZ), me // NBZ % NBY, me % NBZ


def decode(code):
    qx = (code * 57) >> 9
    rest = code - 9 * qx
    qy = (rest * 11) >> 5
    qz = rest - 3 * qy
    word = 1 + jnp.where(qz == 2, ZU, 0) + jnp.where(qz == 0, ZD, 0)
    word = word * jnp.where(qy == 2, 1 + YU, jnp.where(qy == 0, 1 + YD, 1))
    return word | jnp.where(qx == 2, XU, jnp.where(qx == 0, XD, 0))


def on(word, bits):
    return (word & bits) == bits


ALL, OWN, RIM = "all", "own", "rim"


def ring_store(ref, lead, value, part=ALL):
    def put(first, rows):
        ref[(*lead, slice(first, first + rows.shape[0]), slice(None))] = rows

    if part == RIM:
        put(8, value[16:])
        put(ref.shape[-2] - 24, value[:16])
        put(0, value[8:16])
    else:
        put(8, value)
        if part == ALL:
            put(0, value[-8:])


def ring_load(ref, lead, step, part=ALL):
    n = ref.shape[-2] - 16

    def get(first, last):
        return ref[(*lead, slice(first + step, last + step), slice(None))]

    if part == OWN:
        return get(8, n)
    if part == RIM:
        spans = [(n - 8, n), (0, 16)] if step > 0 else [(n - 8, n + 8), (8, 16)]
    else:
        spans = [(8, n), (0, 8)] if step > 0 else [(8, n + 8)]
    return jnp.concatenate([get(*span) for span in spans], axis=0)


def cut(value, part):
    if part == ALL:
        return value
    n = value.shape[0] - 8
    return value[:n] if part == OWN else jnp.concatenate([value[n - 8 :], value[:8]], axis=0)


def pack_kernel(cx, cy, u_in, vf_in, mask_in, code_in, zp, u, vf, c, mask, code, sems):
    copies = [
        pltpu.make_async_copy(mask_in, mask, sems.at[0]),
        pltpu.make_async_copy(code_in, code, sems.at[1]),
        pltpu.make_async_copy(vf_in, vf, sems.at[2]),
    ]
    for f in range(NFIELD):
        rows = pl.ds(f * cx * cy, cx * cy)
        copies.append(pltpu.make_async_copy(u_in.at[rows, :], u.at[rows, :], sems.at[3 + f]))
    for copy in copies:
        copy.start()
    lane = lanes_of((cy, 128))
    slot = ((lane + 1) & 127) >> 1
    low_lane = (lane & 1) == 0
    copies[0].wait()
    copies[1].wait()
    for x in range(cx):
        rows = pl.ds(x * cy, cy)
        c[rows, :] = jnp.where(mask[rows, :] == 1, code[rows, :], 13).astype(jnp.float32)
    for g in (1, 0):
        acc = jnp.zeros((cy, 128), jnp.float32)
        for k in (3, 2, 1, 0):
            f = 4 * g + k
            if f <= VF:
                copies[3 + f if f < VF else 2].wait()
            for x in range(cx):
                m = cx * k + x
                rows = pl.ds(x * cy, cy)
                if f < NFIELD:
                    part = roll(u[pl.ds((f * cx + x) * cy, cy), :], 2 * m)
                elif f < C2:
                    part = roll((vf if f == VF else c)[rows, :], 2 * m)
                else:
                    part = jnp.where(low_lane, roll(c[rows, :], 2 * m - 1), roll(c[rows, :], 2 * m + 1))
                acc = jnp.where(slot == m, part, acc)
        zp[g * cy : (g + 1) * cy, :] = acc


def faces_kernel(cx, cy, two_x, u, vf, c, cw, y_a, y_b, *xs):
    bx, by, bz = place()
    for x in range(cx):
        cw[x + 2, 8 : 8 + cy, :] = decode(c[x * cy : (x + 1) * cy, :].astype(jnp.int32))

    def y_face(out, high):
        rim = jnp.where(high, cy - 1, 0)
        second = jnp.where(high, cy - 2, 1)

        def column(ref, base, row):
            return ref[pl.ds(base + row, cx, stride=cy), :]

        for f in range(NFIELD):
            out[f * cx : (f + 1) * cx, :] = column(u, f * cx * cy, rim)
        out[VF * cx : (VF + 1) * cx, :] = column(vf, 0, rim)
        out[C1 * cx : (C1 + 1) * cx, :] = column(c, 0, rim)
        out[C2 * cx : (C2 + 1) * cx, :] = column(c, 0, second)

    y_face(y_a, by % 2 == 0)
    y_face(y_b, by % 2 == 1)

    def x_face(out, high):
        rim = jnp.where(high, cx - 1, 0) * cy
        second = jnp.where(high, cx - 2, 1) * cy

        def rows(base, start):
            return pl.ds(pl.multiple_of(base + start, 8), cy)

        for f in range(NFIELD):
            out[f * cy : (f + 1) * cy, :] = u[rows(f * cx * cy, rim), :]
        out[VF * cy : (VF + 1) * cy, :] = vf[rows(0, rim), :]
        out[C1 * cy : (C1 + 1) * cy, :] = c[rows(0, rim), :]
        out[C2 * cy : (C2 + 1) * cy, :] = c[rows(0, second), :]

    x_face(xs[0], bx % 2 == 0)
    if two_x:
        x_face(xs[1], bx % 2 == 1)


def z_merge_kernel(cx, cy, r_a, r_b, zp, ya_in, yb_in, zh, y_a, y_b):
    bx, by, bz = place()
    odd = bz % 2 == 1
    lane = lanes_of((cy, 128))
    low_lane = (lane & 1) == 0
    codes = (lane >= 63) & (lane <= 126)
    for g in range(2):
        rows = slice(g * cy, (g + 1) * cy)
        a, b = r_a[rows, :], r_b[rows, :]
        edge = jnp.where(codes, EDGE, 0.0) if g else jnp.zeros((cy, 128), jnp.float32)
        low = jnp.where(bz > 0, roll(jnp.where(odd, a, b), 1), edge)
        high = jnp.where(bz < NBZ - 1, roll(jnp.where(odd, b, a), -1), edge)
        zh[rows, :] = jnp.where(low_lane, low, high)
    zh[2 * cy :, :] = zp[...]
    n = NF * cx

    def finish(out, main, high):
        out[:n, :] = main[...]
        rim = jnp.where(high, cy - 1, 0)
        second = jnp.where(high, cy - 2, 1)
        for g in range(4):
            out[n + 2 * g : n + 2 * g + 1, :] = zh[pl.ds(g * cy + rim, 1), :]
            out[n + 2 * g + 1 : n + 2 * g + 2, :] = zh[pl.ds(g * cy + second, 1), :]

    finish(y_a, ya_in, by % 2 == 0)
    finish(y_b, yb_in, by % 2 == 1)


def z_edge_rows(cx):
    n = NF * cx
    row = lax.broadcasted_iota(jnp.int32, (n + 8, 128), 0)
    lane = lanes_of((n + 8, 128))
    codes = ((row >= C1 * cx) & (row < n)) | ((row >= n) & ((row & 2) != 0) & (lane >= 63) & (lane <= 126))
    return jnp.where(codes, EDGE, 0.0)


def y_merge_kernel(cx, cy, two_x, ended, r_a, r_b, zh, *refs):
    copies = 2 if two_x else 1
    mains, (y_lo, y_hi), xs = refs[:copies], refs[copies : copies + 2], refs[copies + 2 :]
    bx, by, bz = place()
    odd = by % 2 == 1
    edge = z_edge_rows(cx)
    a, b = r_a[...], r_b[...]
    y_lo[...] = jnp.where(by > 0, jnp.where(odd, a, b), edge)
    y_hi[...] = jnp.where(by < NBY - 1, jnp.where(odd, b, a), edge)
    n = NF * cx

    def x_rim(out, main, high):
        rim = jnp.where(high, cx - 1, 0)
        second = jnp.where(high, cx - 2, 1)
        at = NF * cy
        out[:at, :] = main[...]
        lane = lanes_of((8, 128))
        spot = (lane - jnp.where(high, 2 * cx - 5, 2 * cx - 1)) & (2 * cx - 1)
        for half in range(2):
            tile = jnp.zeros((8, 128), jnp.float32)
            for t in range(cy // 8):
                for g in range(2):
                    start, row = 8 * t + 4 * g, (2 * half + g) * cy + 8 * t
                    tile = jnp.where((spot >= start) & (spot < start + 4), roll(zh[row : row + 8, :], start), tile)
            out[at : at + 8, :] = tile
            at += 8
        for y in (y_lo, y_hi):
            out[at : at + 8, :] = y[n : n + 8, :]
            at += 8
        for y in (y_lo, y_hi):
            for f in range(NF):
                out[at : at + 1, :] = y[pl.ds(f * cx + rim, 1), :]
                at += 1
            for f in (C1, C2):
                out[at : at + 1, :] = y[pl.ds(f * cx + second, 1), :]
                at += 1
        out[at:, :] = jnp.zeros((out.shape[0] - at, 128), jnp.float32)

    x_rim(xs[0], mains[0], bx % 2 == 0)
    if two_x:
        x_rim(xs[1], mains[1], bx % 2 == 1)


def y_rows(r, x):
    cx = r.cx
    for f in range(C2):
        r.ht[f, x + 2, 0:1, :] = r.y_hi[pl.ds(f * cx + x, 1), :]
        r.ht[f, x + 2, 7:8, :] = r.y_lo[pl.ds(f * cx + x, 1), :]
    r.ht[C1, x + 2, 1:2, :] = r.y_hi[pl.ds(C2 * cx + x, 1), :]
    r.ht[C1, x + 2, 6:7, :] = r.y_lo[pl.ds(C2 * cx + x, 1), :]


def set_words(r, own, layer):
    both = jnp.concatenate([own, r.ht[C1, layer]], axis=0)
    ring_store(r.cw, (layer,), decode(both.astype(jnp.int32)))


def set_halo_words(r, layer):
    words = decode(r.ht[C1, layer].astype(jnp.int32))
    r.cw[layer, 0:8, :] = words
    r.cw[layer, 8 + r.cy : 16 + r.cy, :] = words


def z_halo(r, f, own):
    g, k = f // 4, f % 4
    return roll(own(g), 4 - 2 * r.cx * k)


def spread_counts(r, planes, slot):
    mid = up = down = jnp.zeros(r.lane.shape, jnp.int32)
    for word, bits in planes:
        v = 1 + ((word & YU) << 6) + ((word & YD) << 4)
        if bits is not None:
            v = jnp.where((word & bits) != 0, v, 0)
        mid = mid + v
        up = up + jnp.where((word & XU) != 0, v, 0)
        down = down + jnp.where((word & XD) != 0, v, 0)
    total = mid + roll(up, 2) + roll(down, -2)
    ring_store(r.tmp_i, (slot,), total, r.part)
    before, after = (ring_load(r.tmp_i, (slot,), step, r.part) for step in (-1, 1))
    return (total & 255) + ((before >> 8) & 255) + ((after >> 16) & 255)


def z_counts(r):
    rows = slice(0, r.lane.shape[0])
    outer1, outer2, inner1, inner2 = (decode(r.zf[f, rows].astype(jnp.int32)) for f in (C1, C2, NF + C1, NF + C2))
    r.ow[rows], r.iw[rows] = outer1, inner1
    planes = ((outer1, None), (outer2, r.inward), (inner1, r.outward)), ((inner1, None), (outer1, r.inward), (inner2, r.outward))
    for first, out, plane in zip((0, NF), (r.zw, r.zi), planes):
        inverse = 1.0 / spread_counts(r, plane, first // NF).astype(jnp.float32)
        weight = r.zf[first + VF, rows] * inverse
        out[0, rows] = weight
        for f in range(NFIELD):
            out[f + 1, rows] = weight * r.zf[first + f, rows]
    r.ci[rows] = inverse


def sum_x(mid, left, right):
    total = (mid & LOW) + jnp.where((left & XU) != 0, left & LOW, 0)
    return total + jnp.where((right & XD) != 0, right & LOW, 0)


def weigh(r, group, part):
    n = r.cy
    lane = lanes_of(({ALL: n + 8, OWN: n, RIM: 24}[part], 128))
    edge_lane = (lane == 0) | (lane == 127)
    totals = []
    for layer, _ in group:
        if part == RIM:
            total = sum_x(*(r.cw[layer + d, 8 + n : 16 + n, :] for d in (0, -1, 1)))
            r.xt[layer, 8 + n : 16 + n, :] = total
            r.xt[layer, 0:8, :] = total
        else:
            ring_store(r.xt, (layer,), sum_x(*(ring_load(r.cw, (layer + d,), 0, part) for d in (0, -1, 1))), part)
    for layer, _ in group:
        total, before, after = (ring_load(r.xt, (layer,), step, part) for step in (0, -1, 1))
        total = (total & 0x333) + ((before >> 2) & 0x333) + ((after >> 12) & 0x333)
        totals.append((total, roll(total, 1), roll(total, -1), roll(cut(r.ci[...], part), -2 * layer)))
    for (layer, field), (total, below, above, edge) in zip(group, totals):
        count = (total & 15) + ((below >> 4) & 15) + ((above >> 8) & 15)
        inverse = jnp.where(edge_lane, edge, 1.0 / count.astype(jnp.float32))
        if part == RIM:
            r.rc[layer, n - 8 :], r.rc[layer, 0:8] = inverse[:8], inverse[16:]
        else:
            r.rc[layer] = inverse[:n]
        ring_store(r.h0, (0, layer), field(VF, part) * inverse, part)
    for layer, field in group:
        weight = ring_load(r.h0, (0, layer), 0, part)
        for f in range(NFIELD + 1):
            w = weight
            if f:
                w = weight * field(f - 1, part)
                ring_store(r.h0, (f, layer), w, part)
            ring_store(r.hm, (f, layer), w + roll(w, 1), part)
            ring_store(r.hp, (f, layer), w + roll(w, -1), part)


def own_field(r, x, f, part):
    base = (f * r.cx + x if f < NFIELD else x) * r.cy
    ref = r.u if f < NFIELD else r.vf

    def rows(first, count):
        start = base + first
        return ref[pl.ds(start if isinstance(start, int) else pl.multiple_of(start, 8), count), :]

    if part == OWN:
        return rows(0, r.cy)
    if part == RIM:
        return jnp.concatenate([rows(r.cy - 8, 8), r.ht[f, x + 2], rows(0, 8)], axis=0)
    return jnp.concatenate([rows(0, r.cy), r.ht[f, x + 2]], axis=0)


def z_averages(r, deposit=True):
    tmp = r.tmp_f

    def pick(word, up, down, values):
        mid, plus, minus = values
        return mid + jnp.where((word & up) != 0, plus, jnp.where((word & down) != 0, minus, 0.0))

    rows = slice(0, r.lane.shape[0])
    sums, inner_sums = [], []
    for f in range(NFIELD + 1):
        both = r.zw[f, rows] + r.zi[f, rows]
        for i, value in enumerate((both, roll(both, -2), roll(both, 2))):
            ring_store(tmp, (3 * f + i,), value, r.part)
        around = [[ring_load(tmp, (3 * f + i,), step, r.part) for step in (0, 1, -1)] for i in range(3)]
        for word, out in ((r.ow[rows], sums), (r.iw[rows], inner_sums))[1 - deposit :]:
            out.append(pick(word, XU, XD, [pick(word, YU, YD, line) for line in around]))
    inverse = 1.0 / inner_sums[0]
    for f in range(NFIELD):
        r.ai[f, rows] = inner_sums[f + 1] * inverse
    if not deposit:
        return
    word = r.ow[...]
    inverse = 1.0 / sums[0]
    first = 3 * NFIELD + 3
    for f in range(NFIELD):
        v = jnp.where((word & r.inward) != 0, sums[f + 1] * inverse, 0.0)
        totals = []
        for i, bits in enumerate((0, XU, XD)):
            w = jnp.where((word & bits) != 0, v, 0.0) if bits else v
            slot = first + 6 * f + 2 * i
            ring_store(tmp, (slot,), jnp.where((word & YU) != 0, w, 0.0))
            ring_store(tmp, (slot + 1,), jnp.where((word & YD) != 0, w, 0.0))
            totals.append(w + ring_load(tmp, (slot,), -1) + ring_load(tmp, (slot + 1,), 1))
        r.dz[f] = totals[0] + roll(totals[1], 2) + roll(totals[2], -2)


def average(r, layer, rows_of=None):
    rows = r.cy + 8
    tiles = rows // 8
    lane = lanes_of((8, 128))
    for t in range(tiles) if rows_of is None else rows_of:
        at = 8 + 8 * t
        word = r.cw[layer, at : at + 8, :]
        zu, zd = (word & ZU) != 0, (word & ZD) != 0
        yu, yd = (word & YU) != 0, (word & YD) != 0
        xu, xd = (word & XU) != 0, (word & XD) != 0
        sums = []
        for f in range(NFIELD + 1):
            parts = []
            for d in (0, 1, -1):
                line = []
                for e in (0, 1, -1):
                    base = 0 if t == tiles - 1 and e == 1 else at
                    at_e = slice(base + e, base + e + 8)
                    v0, vm, vp = (h[f, layer + d, at_e, :] for h in (r.h0, r.hm, r.hp))
                    line.append(jnp.where(zu, vp, jnp.where(zd, vm, v0)))
                parts.append(line[0] + jnp.where(yu, line[1], jnp.where(yd, line[2], 0.0)))
            sums.append(parts[0] + jnp.where(xu, parts[1], jnp.where(xd, parts[2], 0.0)))
        inverse = 1.0 / sums[0]
        leaves = ((lane == 0) & zd) | ((lane == 127) & zu)
        for f in range(NFIELD):
            column = roll(r.ai[f, 8 * t : 8 * t + 8, :], -2 * layer)
            a = jnp.where(leaves, column, sums[f + 1] * inverse)
            r.av[f, layer, at : at + 8, :] = a
            if t == tiles - 1:
                r.av[f, layer, 0:8, :] = a


def redistribute(r, x, out):
    cx, cy = r.cx, r.cy
    layer = x + 2
    back = -2 * layer
    lane = lanes_of((8, 128))
    first_lane, last_lane = lane == 0, lane == 127
    for t in range(cy // 8):
        at = 8 + 8 * t
        base = [r.av[f, layer, at : at + 8, :] for f in range(NFIELD)]
        word = r.cw[layer, at : at + 8, :]
        up = [jnp.where((word & ZU) != 0, a, 0.0) for a in base]
        down = [jnp.where((word & ZD) != 0, a, 0.0) for a in base]
        for d in (0, 1, -1):
            for e in (0, 1, -1):
                if d == 0 and e == 0:
                    continue
                at_e = slice(at - e, at - e + 8)
                word = r.cw[layer - d, at_e, :]
                bits = (0, XU, XD)[d] | (0, YU, YD)[e]
                here = on(word, bits)
                here_up, here_down = on(word, bits | ZU), on(word, bits | ZD)
                for f in range(NFIELD):
                    a = r.av[f, layer - d, at_e, :]
                    base[f] = base[f] + jnp.where(here, a, 0.0)
                    up[f] = up[f] + jnp.where(here_up, a, 0.0)
                    down[f] = down[f] + jnp.where(here_down, a, 0.0)
        inverse = r.rc[layer, 8 * t : 8 * t + 8, :]
        for f in range(NFIELD):
            halo = roll(r.dz[f, 8 * t : 8 * t + 8, :], back)
            total = base[f] + jnp.where(first_lane, halo, roll(up[f], 1))
            total = total + jnp.where(last_lane, halo, roll(down[f], -1))
            out[pl.ds(pl.multiple_of((f * cx + x) * cy + 8 * t, 8), 8), :] = total * inverse


def common(r, part):
    r.part = part
    r.lane = lanes_of((r.cy + (8 if part == ALL else 0), 128))
    even = (r.lane & 1) == 0
    r.inward = jnp.where(even, ZU, ZD)
    r.outward = jnp.where(even, ZD, ZU)


def z_fields(r, rows, own):
    for f in range(2 * NF):
        value = z_halo(r, f, own)
        if r.outside is not None:
            value = jnp.where(r.outside[: value.shape[0]], EDGE if f % NF >= C1 else 0.0, value)
        r.zf[f, rows] = value


KEPT = ("cw", "zf", "xt", "h0", "hm", "hp", "rc", "av")
SCRATCH = ("ht", "hz", "ow", "iw", "tmp_i", "tmp_f", "ci", "zw", "zi", "ai", "dz")


def plan(cx, nbx, bx):
    if nbx == 2:
        high = bx == 0

        def at(j):
            return jnp.where(high, j + 1, cx + 2 - j)

        return types.SimpleNamespace(
            at=at,
            inner_weigh=[at(j) for j in range(1, cx)],
            inner_average=(1, cx - 2),
            inner_spread=(1, cx - 3),
            outer_weigh=[at(cx)],
            outer_average=[(cx - 1, 3)],
            outer_spread=[(cx - 2, 3)],
            inner_rows=(jnp.where(high, 0, 3), cx - 3),
            outer_rows=[(jnp.where(high, cx - 3, 0), 3)],
        )
    return types.SimpleNamespace(
        at=lambda j: j + 1,
        inner_weigh=range(3, cx + 1),
        inner_average=(3, cx - 4),
        inner_spread=(4, cx - 6),
        outer_weigh=[2, cx + 1],
        outer_average=[(0, 3), (cx - 1, 3)],
        outer_spread=[(1, 3), (cx - 2, 3)],
        inner_rows=(3, cx - 6),
        outer_rows=[(0, 3), (cx - 3, 3)],
    )


def x_lanes(r, high):
    below = (r.lane == 127) | (r.lane <= 2)
    above = (r.lane >= 2 * r.cx + 3) & (r.lane <= 2 * r.cx + 6)
    if isinstance(high, bool):
        return above if high else below
    return (above & high) | (below & jnp.logical_not(high))


def each(span, step):
    def body(j, _):
        step(j)
        return 0

    lax.fori_loop(span[0], span[0] + span[1], body, 0)


def set_outside(r, nbx, bx):
    r.outside = x_lanes(r, bx > 0) if nbx == 2 else None


def early_kernel(cx, cy, nbx, *refs):
    names = ("u", "vf", "zh", "cw_in", *KEPT, "ended", *SCRATCH)
    r = types.SimpleNamespace(cx=cx, cy=cy, **dict(zip(names, refs)))
    common(r, OWN)
    bx, by, bz = place()
    todo = plan(cx, nbx, bx)
    set_outside(r, nbx, bx)
    z_fields(r, slice(0, cy), lambda g: r.zh[g * cy : (g + 1) * cy, :])
    if nbx == 2:
        edge = todo.at(0)
        ring_store(r.cw, (edge,), jnp.ones((cy + 8, 128), jnp.int32))
        for f in range(NFIELD + 1):
            for h in (r.h0, r.hm, r.hp):
                ring_store(h, (f, edge), jnp.zeros((cy + 8, 128), jnp.float32))
    z_counts(r)
    weigh(r, [(layer, functools.partial(own_field, r, layer - 2)) for layer in todo.inner_weigh], OWN)
    z_averages(r, deposit=False)
    each(todo.inner_average, lambda j: average(r, todo.at(j), range(1, cy // 8 - 1)))
    r.ended[...] = r.ci[0:8]


def inner_kernel(cx, cy, nbx, *refs):
    kept_in = len(KEPT)
    names = ("u", "vf", "y_lo", "y_hi")
    rest = refs[len(names) + kept_in :]
    r = types.SimpleNamespace(cx=cx, cy=cy, **dict(zip(names, refs)))
    r.__dict__.update(zip((*KEPT, "res", *SCRATCH), rest))
    common(r, ALL)
    bx, by, bz = place()
    todo = plan(cx, nbx, bx)
    set_outside(r, nbx, bx)
    r.ht[...] = jnp.zeros(r.ht.shape, jnp.float32)
    for x in range(cx):
        y_rows(r, x)
        set_halo_words(r, x + 2)
    n = NF * cx
    for g in range(4):
        for i, row in enumerate((0, 1)):
            r.hz[g, row : row + 1, :] = r.y_hi[n + 2 * g + i : n + 2 * g + i + 1, :]
            r.hz[g, 7 - row : 8 - row, :] = r.y_lo[n + 2 * g + i : n + 2 * g + i + 1, :]
    z_fields(r, slice(cy, cy + 8), lambda g: r.hz[g])
    z_counts(r)
    weigh(r, [(layer, functools.partial(own_field, r, layer - 2)) for layer in todo.inner_weigh], RIM)
    z_averages(r)
    each(todo.inner_average, lambda j: average(r, todo.at(j), (0, cy // 8 - 1, cy // 8)))
    each(todo.inner_spread, lambda j: redistribute(r, todo.at(j) - 2, r.res))


def outer_kernel(cx, cy, nbx, *refs):
    kept_in = len(KEPT)
    names = ("u", "vf", "y_lo", "y_hi", "res", "xa", "xb")
    ins = refs[: len(names)]
    rest = refs[len(names) + kept_in :]
    r = types.SimpleNamespace(cx=cx, cy=cy, **dict(zip(names, ins)))
    r.__dict__.update(zip(("out", *KEPT, *SCRATCH, "rim", "sems"), rest))
    size = cx * cy
    bx, by, bz = place()
    todo = plan(cx, nbx, bx)

    def send(src, rows, base):
        copies = []
        for f in range(NFIELD):
            part = pl.ds(pl.multiple_of(f * size + rows[0] * cy, 8), rows[1] * cy)
            copies.append(pltpu.make_async_copy(src.at[part, :], r.out.at[part, :], r.sems.at[base + f]))
        for copy in copies:
            copy.start()
        return copies

    copies = send(r.res, todo.inner_rows, 0)
    common(r, ALL)
    x_odd = bx % 2 == 1

    if nbx == 2:
        sides = [(bx == 0, True, lambda first, count: r.xa[first : first + count, :])]
    else:

        def message(high):
            def rows(first, count):
                a, b = r.xa[first : first + count, :], r.xb[first : first + count, :]
                return jnp.where(x_odd, b, a) if high else jnp.where(x_odd, a, b)

            return rows

        sides = [(False, bx > 0, message(False)), (True, bx < nbx - 1, message(True))]

    def choose(high, a, b):
        return (a if high else b) if isinstance(high, bool) else jnp.where(high, a, b)

    def present_or(present, value, edge):
        return value if present is True else jnp.where(present, value, edge)

    zrow = NF * cy
    edges = zrow + 16
    halo = []
    for high, present, part in sides:
        layer, second, own = (choose(high, a, b) for a, b in ((cx + 2, 1), (cx + 3, 0), (cx - 1, 0)))
        y_rows(r, own)

        def raw(f, present=present, part=part):
            return present_or(present, part(f * cy, cy), EDGE if f >= C1 else 0.0)

        for y, row1, row2 in ((0, 7, 6), (1, 0, 1)):
            base = edges + 16 + 10 * y

            def rim(i, edge, base=base, present=present, part=part):
                return present_or(present, part(base + i, 1), edge)

            for f in range(C1):
                r.ht[f, layer, row1 : row1 + 1, :] = rim(f, 0.0)
            r.ht[C1, layer, row1 : row1 + 1, :] = rim(C1, EDGE)
            r.ht[C1, layer, row2 : row2 + 1, :] = rim(C2, EDGE)
            r.ht[C1, second, row1 : row1 + 1, :] = rim(NF, EDGE)
            r.ht[C1, second, row2 : row2 + 1, :] = rim(NF + 1, EDGE)
        set_words(r, raw(C1), layer)
        set_words(r, raw(C2), second)
        halo.append((layer, lambda f, part, raw=raw, layer=layer: jnp.concatenate([raw(f), r.ht[f, layer]], axis=0)))

        for g in range(4):
            for i, row in enumerate((0, 1)):
                lo, hi = edges + 2 * g + i, edges + 8 + 2 * g + i
                r.hz[g, row : row + 1, :] = part(hi, 1)
                r.hz[g, 7 - row : 8 - row, :] = part(lo, 1)
        lanes = x_lanes(r, high)
        for f in range(2 * NF):
            g, k = f // 4, f % 4
            shift = 4 - 2 * cx * k + choose(high, 2 * cx, -2 * cx)
            tile = part(zrow + 8 * (g // 2), 8)
            tiles = [roll(tile, shift - 8 * t - 4 * (g % 2)) for t in range(cy // 8)]
            value = jnp.concatenate([*tiles, roll(r.hz[g], shift)], axis=0)
            r.zf[f] = jnp.where(lanes, present_or(present, value, EDGE if f % NF >= C1 else 0.0), r.zf[f])
    z_counts(r)
    weigh(r, [(layer, functools.partial(own_field, r, layer - 2)) for layer in todo.outer_weigh] + halo, ALL)
    z_averages(r)
    for span in todo.outer_average:
        each(span, lambda j: average(r, todo.at(j)))
    for i, (span, rows) in enumerate(zip(todo.outer_spread, todo.outer_rows)):
        each(span, lambda j: redistribute(r, todo.at(j) - 2, r.rim))
        copies += send(r.rim, rows, (1 + i) * NFIELD)
    for copy in copies:
        copy.wait()


def call(kernel, ins, outs, scratch=(), name=None, grant=8, flops=0, **kwargs):
    return pl.pallas_call(
        kernel,
        in_specs=ins,
        out_specs=tuple(pl.BlockSpec(memory_space=o.memory_space) for o in outs),
        out_shape=tuple(outs),
        scratch_shapes=scratch,
        name=name,
        cost_estimate=pl.CostEstimate(flops=flops, transcendentals=0, bytes_accessed=0),
        compiler_params=pltpu.CompilerParams(vmem_limit_bytes=grant << 20),
        **kwargs,
    )


def per_device(conserved, volume_fraction, cut_mask, merge_code):
    _, cx, cy, cz = cut_mask.shape
    devices = lax.axis_size(AXIS)
    nbx = devices // (NBY * NBZ)
    two_x = nbx > 2
    cells = cx * cy
    u = conserved.reshape(NFIELD * cells, cz)
    vf, mask, code = (a.reshape(cells, cz) for a in (volume_fraction, cut_mask, merge_code))
    f32, i32 = jnp.float32, jnp.int32
    on_chip, far = pl.BlockSpec(memory_space=pltpu.VMEM), pl.BlockSpec(memory_space=pltpu.HBM)

    def vmem(*shape, dtype=f32):
        return pltpu.VMEM((*shape, cz), dtype)

    def swap(value, stride, extent, odd):
        return lax.ppermute(value, AXIS, pairing(stride, extent, devices, odd))

    n = NF * cx
    copies = 2 if two_x else 1
    zp, u, vf, c = call(
        functools.partial(pack_kernel, cx, cy),
        [far] * 4,
        [vmem(2 * cy), vmem(NFIELD * cells), vmem(cells), vmem(cells)],
        [vmem(cells, dtype=i32), vmem(cells, dtype=i32), pltpu.SemaphoreType.DMA((3 + NFIELD,))],
        "pack",
    )(*(pltpu.with_memory_space_constraint(a, pltpu.HBM) for a in (u, vf, mask, code)))
    za, zb = swap(zp, 1, NBZ, False), swap(zp, 1, NBZ, True)
    rows, ring, layers = cy + 8, cy + 24, cx + 4
    cw, ya, yb, *xs = call(
        functools.partial(faces_kernel, cx, cy, two_x),
        [on_chip] * 3,
        [vmem(layers, ring, dtype=i32), vmem(n), vmem(n)] + [vmem(NF * cy)] * copies,
        name="faces",
        flops=1 << 20,
    )(u, vf, c)
    zh, ya, yb = call(
        functools.partial(z_merge_kernel, cx, cy), [on_chip] * 5, [vmem(4 * cy), vmem(n + 8), vmem(n + 8)], name="z_merge"
    )(za, zb, zp, ya, yb)
    kept = [
        vmem(layers, ring, dtype=i32),
        vmem(2 * NF, rows),
        vmem(layers, ring, dtype=i32),
        vmem(NFIELD + 1, layers, ring),
        vmem(NFIELD + 1, layers, ring),
        vmem(NFIELD + 1, layers, ring),
        vmem(layers, cy),
        vmem(NFIELD, layers, ring),
    ]
    scratch = [
        vmem(C2, layers, 8),
        vmem(4, 8),
        vmem(rows, dtype=i32),
        vmem(rows, dtype=i32),
        vmem(2, ring, dtype=i32),
        vmem(9 * NFIELD + 3, ring),
        vmem(rows),
        vmem(NFIELD + 1, rows),
        vmem(NFIELD + 1, rows),
        vmem(NFIELD, rows),
        vmem(NFIELD, rows),
    ]
    yb = swap(yb, NBZ, NBY, True)
    ya = swap(ya, NBZ, NBY, False)
    *state, ended = call(
        functools.partial(early_kernel, cx, cy, nbx),
        [on_chip] * 4,
        kept + [vmem(8)],
        scratch,
        "early",
        flops=1 << 24,
        input_output_aliases={3: 0},
    )(u, vf, zh, cw)
    y_lo, y_hi, *xs = call(
        functools.partial(y_merge_kernel, cx, cy, two_x),
        [on_chip] * (4 + copies),
        [vmem(n + 8), vmem(n + 8)] + [vmem(NF * cy + 56)] * copies,
        name="y_merge",
    )(ended, ya, yb, zh, *xs)
    xs = [swap(x, NBY * NBZ, nbx, odd) for odd, x in enumerate(xs)]
    xa, xb = xs if two_x else xs * 2

    *state, res = call(
        functools.partial(inner_kernel, cx, cy, nbx),
        [on_chip] * (4 + len(kept)),
        kept + [vmem(NFIELD * cells)],
        scratch,
        "inner",
        flops=1 << 26,
        input_output_aliases={4 + i: i for i in range(len(kept))},
    )(u, vf, y_lo, y_hi, *state)
    first = 7
    out, *_ = call(
        functools.partial(outer_kernel, cx, cy, nbx),
        [on_chip] * (first + len(kept)),
        [pltpu.HBM((NFIELD * cells, cz), f32)] + kept,
        scratch + [vmem(NFIELD * cells), pltpu.SemaphoreType.DMA((3 * NFIELD,))],
        "outer",
        flops=1 << 25,
        input_output_aliases={first + i: 1 + i for i in range(len(kept))},
    )(u, vf, y_lo, y_hi, res, xa, xb, *state)
    return out.reshape(conserved.shape)


def solution(mesh):
    return jax.shard_map(
        per_device,
        mesh=mesh,
        in_specs=(
            P(AXIS, None, None, None, None),
            P(AXIS, None, None, None),
            P(AXIS, None, None, None),
            P(AXIS, None, None, None),
        ),
        out_specs=P(AXIS, None, None, None, None),
        check_vma=False,
    )
```

```python
import functools
import types

import jax
import jax.numpy as jnp
from jax import lax
from jax.experimental import pallas as pl
from jax.experimental.pallas import tpu as pltpu
from jax.sharding import PartitionSpec as P

NBY = 4
NBZ = 4
AXIS = "boxes"

NFIELD = 5
VF = 5
C1 = 6
C2 = 7
NF = 8
ZU, ZD, YU, YD, XU, XD = 16, 256, 4, 4096, 1 << 28, 1 << 29
LOW = (1 << 24) - 1
EDGE = 13.0


def pairing(stride, extent, devices, odd):
    pairs = []
    for i in range(devices):
        c = i // stride % extent
        partner = ((c + 1) ^ 1) - 1 if odd else c ^ 1
        pairs.append((i, i + (partner % extent - c) * stride))
    return pairs


def lanes_of(shape):
    return lax.broadcasted_iota(jnp.int32, shape, len(shape) - 1)


def roll(value, shift, axis=1):
    if isinstance(shift, int):
        shift %= value.shape[axis]
        if shift == 0:
            return value
    else:
        shift &= value.shape[axis] - 1
    return pltpu.roll(value, shift, axis)


def place():
    me = lax.axis_index(AXIS)
    return me // (NBY * NBZ), me // NBZ % NBY, me % NBZ


def decode(code):
    qx = (code * 57) >> 9
    rest = code - 9 * qx
    qy = (rest * 11) >> 5
    qz = rest - 3 * qy
    word = 1 + jnp.where(qz == 2, ZU, 0) + jnp.where(qz == 0, ZD, 0)
    word = word * jnp.where(qy == 2, 1 + YU, jnp.where(qy == 0, 1 + YD, 1))
    return word | jnp.where(qx == 2, XU, jnp.where(qx == 0, XD, 0))


def on(word, bits):
    return (word & bits) == bits


ALL, OWN, RIM = "all", "own", "rim"


def ring_store(ref, lead, value, part=ALL):
    def put(first, rows):
        ref[(*lead, slice(first, first + rows.shape[0]), slice(None))] = rows

    if part == RIM:
        put(8, value[16:])
        put(ref.shape[-2] - 24, value[:16])
        put(0, value[8:16])
    else:
        put(8, value)
        if part == ALL:
            put(0, value[-8:])


def ring_load(ref, lead, step, part=ALL):
    n = ref.shape[-2] - 16

    def get(first, last):
        return ref[(*lead, slice(first + step, last + step), slice(None))]

    if part == OWN:
        return get(8, n)
    if part == RIM:
        spans = [(n - 8, n), (0, 16)] if step > 0 else [(n - 8, n + 8), (8, 16)]
    else:
        spans = [(8, n), (0, 8)] if step > 0 else [(8, n + 8)]
    return jnp.concatenate([get(*span) for span in spans], axis=0)


def cut(value, part):
    if part == ALL:
        return value
    n = value.shape[0] - 8
    return value[:n] if part == OWN else jnp.concatenate([value[n - 8 :], value[:8]], axis=0)


def pack_kernel(cx, cy, u_in, vf_in, mask_in, code_in, zp, u, vf, c, mask, code, sems):
    copies = [
        pltpu.make_async_copy(mask_in, mask, sems.at[0]),
        pltpu.make_async_copy(code_in, code, sems.at[1]),
        pltpu.make_async_copy(vf_in, vf, sems.at[2]),
    ]
    for f in range(NFIELD):
        rows = pl.ds(f * cx * cy, cx * cy)
        copies.append(pltpu.make_async_copy(u_in.at[rows, :], u.at[rows, :], sems.at[3 + f]))
    for copy in copies:
        copy.start()
    lane = lanes_of((cy, 128))
    slot = ((lane + 1) & 127) >> 1
    low_lane = (lane & 1) == 0
    copies[0].wait()
    copies[1].wait()
    for x in range(cx):
        rows = pl.ds(x * cy, cy)
        c[rows, :] = jnp.where(mask[rows, :] == 1, code[rows, :], 13).astype(jnp.float32)
    for g in (1, 0):
        acc = jnp.zeros((cy, 128), jnp.float32)
        for k in (3, 2, 1, 0):
            f = 4 * g + k
            if f <= VF:
                copies[3 + f if f < VF else 2].wait()
            for x in range(cx):
                m = cx * k + x
                rows = pl.ds(x * cy, cy)
                if f < NFIELD:
                    part = roll(u[pl.ds((f * cx + x) * cy, cy), :], 2 * m)
                elif f < C2:
                    part = roll((vf if f == VF else c)[rows, :], 2 * m)
                else:
                    part = jnp.where(low_lane, roll(c[rows, :], 2 * m - 1), roll(c[rows, :], 2 * m + 1))
                acc = jnp.where(slot == m, part, acc)
        zp[g * cy : (g + 1) * cy, :] = acc


def faces_kernel(cx, cy, two_x, u, vf, c, cw, y_a, y_b, *xs):
    bx, by, bz = place()
    for x in range(cx):
        cw[x + 2, 8 : 8 + cy, :] = decode(c[x * cy : (x + 1) * cy, :].astype(jnp.int32))

    def y_face(out, high):
        rim = jnp.where(high, cy - 1, 0)
        second = jnp.where(high, cy - 2, 1)

        def column(ref, base, row):
            return ref[pl.ds(base + row, cx, stride=cy), :]

        for f in range(NFIELD):
            out[f * cx : (f + 1) * cx, :] = column(u, f * cx * cy, rim)
        out[VF * cx : (VF + 1) * cx, :] = column(vf, 0, rim)
        out[C1 * cx : (C1 + 1) * cx, :] = column(c, 0, rim)
        out[C2 * cx : (C2 + 1) * cx, :] = column(c, 0, second)

    y_face(y_a, by % 2 == 0)
    y_face(y_b, by % 2 == 1)

    def x_face(out, high):
        rim = jnp.where(high, cx - 1, 0) * cy
        second = jnp.where(high, cx - 2, 1) * cy

        def rows(base, start):
            return pl.ds(pl.multiple_of(base + start, 8), cy)

        for f in range(NFIELD):
            out[f * cy : (f + 1) * cy, :] = u[rows(f * cx * cy, rim), :]
        out[VF * cy : (VF + 1) * cy, :] = vf[rows(0, rim), :]
        out[C1 * cy : (C1 + 1) * cy, :] = c[rows(0, rim), :]
        out[C2 * cy : (C2 + 1) * cy, :] = c[rows(0, second), :]

    x_face(xs[0], bx % 2 == 0)
    if two_x:
        x_face(xs[1], bx % 2 == 1)


def z_merge_kernel(cx, cy, r_a, r_b, zp, ya_in, yb_in, zh, y_a, y_b):
    bx, by, bz = place()
    odd = bz % 2 == 1
    lane = lanes_of((cy, 128))
    low_lane = (lane & 1) == 0
    codes = (lane >= 63) & (lane <= 126)
    for g in range(2):
        rows = slice(g * cy, (g + 1) * cy)
        a, b = r_a[rows, :], r_b[rows, :]
        edge = jnp.where(codes, EDGE, 0.0) if g else jnp.zeros((cy, 128), jnp.float32)
        low = jnp.where(bz > 0, roll(jnp.where(odd, a, b), 1), edge)
        high = jnp.where(bz < NBZ - 1, roll(jnp.where(odd, b, a), -1), edge)
        zh[rows, :] = jnp.where(low_lane, low, high)
    zh[2 * cy :, :] = zp[...]
    n = NF * cx

    def finish(out, main, high):
        out[:n, :] = main[...]
        rim = jnp.where(high, cy - 1, 0)
        second = jnp.where(high, cy - 2, 1)
        for g in range(4):
            out[n + 2 * g : n + 2 * g + 1, :] = zh[pl.ds(g * cy + rim, 1), :]
            out[n + 2 * g + 1 : n + 2 * g + 2, :] = zh[pl.ds(g * cy + second, 1), :]

    finish(y_a, ya_in, by % 2 == 0)
    finish(y_b, yb_in, by % 2 == 1)


def z_edge_rows(cx):
    n = NF * cx
    row = lax.broadcasted_iota(jnp.int32, (n + 8, 128), 0)
    lane = lanes_of((n + 8, 128))
    codes = ((row >= C1 * cx) & (row < n)) | ((row >= n) & ((row & 2) != 0) & (lane >= 63) & (lane <= 126))
    return jnp.where(codes, EDGE, 0.0)


def y_merge_kernel(cx, cy, two_x, ended, r_a, r_b, zh, *refs):
    copies = 2 if two_x else 1
    mains, (y_lo, y_hi), xs = refs[:copies], refs[copies : copies + 2], refs[copies + 2 :]
    bx, by, bz = place()
    odd = by % 2 == 1
    edge = z_edge_rows(cx)
    a, b = r_a[...], r_b[...]
    y_lo[...] = jnp.where(by > 0, jnp.where(odd, a, b), edge)
    y_hi[...] = jnp.where(by < NBY - 1, jnp.where(odd, b, a), edge)
    n = NF * cx

    def x_rim(out, main, high):
        rim = jnp.where(high, cx - 1, 0)
        second = jnp.where(high, cx - 2, 1)
        at = NF * cy
        out[:at, :] = main[...]
        lane = lanes_of((8, 128))
        spot = (lane - jnp.where(high, 2 * cx - 5, 2 * cx - 1)) & (2 * cx - 1)
        for half in range(2):
            tile = jnp.zeros((8, 128), jnp.float32)
            for t in range(cy // 8):
                for g in range(2):
                    start, row = 8 * t + 4 * g, (2 * half + g) * cy + 8 * t
                    tile = jnp.where((spot >= start) & (spot < start + 4), roll(zh[row : row + 8, :], start), tile)
            out[at : at + 8, :] = tile
            at += 8
        low, up = y_lo[n : n + 8, :], y_hi[n : n + 8, :]
        out[at : at + 8, :] = jnp.where(spot < 4, low, roll(up, 4))
        at += 8
        for y in (y_lo, y_hi):
            for f in range(NF):
                out[at : at + 1, :] = y[pl.ds(f * cx + rim, 1), :]
                at += 1
            for f in (C1, C2):
                out[at : at + 1, :] = y[pl.ds(f * cx + second, 1), :]
                at += 1
        out[at:, :] = jnp.zeros((out.shape[0] - at, 128), jnp.float32)

    x_rim(xs[0], mains[0], bx % 2 == 0)
    if two_x:
        x_rim(xs[1], mains[1], bx % 2 == 1)


def y_rows(r, x):
    cx = r.cx
    for f in range(C2):
        r.ht[f, x + 2, 0:1, :] = r.y_hi[pl.ds(f * cx + x, 1), :]
        r.ht[f, x + 2, 7:8, :] = r.y_lo[pl.ds(f * cx + x, 1), :]
    r.ht[C1, x + 2, 1:2, :] = r.y_hi[pl.ds(C2 * cx + x, 1), :]
    r.ht[C1, x + 2, 6:7, :] = r.y_lo[pl.ds(C2 * cx + x, 1), :]


def set_words(r, own, layer):
    both = jnp.concatenate([own, r.ht[C1, layer]], axis=0)
    ring_store(r.cw, (layer,), decode(both.astype(jnp.int32)))


def set_halo_words(r, layer):
    words = decode(r.ht[C1, layer].astype(jnp.int32))
    r.cw[layer, 0:8, :] = words
    r.cw[layer, 8 + r.cy : 16 + r.cy, :] = words


def z_halo(r, f, own):
    g, k = f // 4, f % 4
    return roll(own(g), 4 - 2 * r.cx * k)


def spread_counts(r, planes, slot):
    mid = up = down = jnp.zeros(r.lane.shape, jnp.int32)
    for word, bits in planes:
        v = 1 + ((word & YU) << 6) + ((word & YD) << 4)
        if bits is not None:
            v = jnp.where((word & bits) != 0, v, 0)
        mid = mid + v
        up = up + jnp.where((word & XU) != 0, v, 0)
        down = down + jnp.where((word & XD) != 0, v, 0)
    total = mid + roll(up, 2) + roll(down, -2)
    ring_store(r.tmp_i, (slot,), total, r.part)
    before, after = (ring_load(r.tmp_i, (slot,), step, r.part) for step in (-1, 1))
    return (total & 255) + ((before >> 8) & 255) + ((after >> 16) & 255)


def z_counts(r):
    rows = slice(0, r.lane.shape[0])
    outer1, outer2, inner1, inner2 = (decode(r.zf[f, rows].astype(jnp.int32)) for f in (C1, C2, NF + C1, NF + C2))
    r.ow[rows], r.iw[rows] = outer1, inner1
    planes = ((outer1, None), (outer2, r.inward), (inner1, r.outward)), ((inner1, None), (outer1, r.inward), (inner2, r.outward))
    for first, out, plane in zip((0, NF), (r.zw, r.zi), planes):
        inverse = 1.0 / spread_counts(r, plane, first // NF).astype(jnp.float32)
        weight = r.zf[first + VF, rows] * inverse
        out[0, rows] = weight
        for f in range(NFIELD):
            out[f + 1, rows] = weight * r.zf[first + f, rows]
    r.ci[rows] = inverse


def sum_x(mid, left, right):
    total = (mid & LOW) + jnp.where((left & XU) != 0, left & LOW, 0)
    return total + jnp.where((right & XD) != 0, right & LOW, 0)


def weigh(r, group, part):
    n = r.cy
    lane = lanes_of(({ALL: n + 8, OWN: n, RIM: 24}[part], 128))
    edge_lane = (lane == 0) | (lane == 127)
    totals = []
    for layer, _ in group:
        if part == RIM:
            total = sum_x(*(r.cw[layer + d, 8 + n : 16 + n, :] for d in (0, -1, 1)))
            r.xt[layer, 8 + n : 16 + n, :] = total
            r.xt[layer, 0:8, :] = total
        else:
            ring_store(r.xt, (layer,), sum_x(*(ring_load(r.cw, (layer + d,), 0, part) for d in (0, -1, 1))), part)
    for layer, _ in group:
        total, before, after = (ring_load(r.xt, (layer,), step, part) for step in (0, -1, 1))
        total = (total & 0x333) + ((before >> 2) & 0x333) + ((after >> 12) & 0x333)
        totals.append((total, roll(total, 1), roll(total, -1), roll(cut(r.ci[...], part), -2 * layer)))
    for (layer, field), (total, below, above, edge) in zip(group, totals):
        count = (total & 15) + ((below >> 4) & 15) + ((above >> 8) & 15)
        inverse = jnp.where(edge_lane, edge, 1.0 / count.astype(jnp.float32))
        if part == RIM:
            r.rc[layer, n - 8 :], r.rc[layer, 0:8] = inverse[:8], inverse[16:]
        else:
            r.rc[layer] = inverse[:n]
        ring_store(r.h0, (0, layer), field(VF, part) * inverse, part)
    for layer, field in group:
        weight = ring_load(r.h0, (0, layer), 0, part)
        for f in range(NFIELD + 1):
            w = weight
            if f:
                w = weight * field(f - 1, part)
                ring_store(r.h0, (f, layer), w, part)
            ring_store(r.hm, (f, layer), w + roll(w, 1), part)
            ring_store(r.hp, (f, layer), w + roll(w, -1), part)


def own_field(r, x, f, part):
    base = (f * r.cx + x if f < NFIELD else x) * r.cy
    ref = r.u if f < NFIELD else r.vf

    def rows(first, count):
        start = base + first
        return ref[pl.ds(start if isinstance(start, int) else pl.multiple_of(start, 8), count), :]

    if part == OWN:
        return rows(0, r.cy)
    if part == RIM:
        return jnp.concatenate([rows(r.cy - 8, 8), r.ht[f, x + 2], rows(0, 8)], axis=0)
    return jnp.concatenate([rows(0, r.cy), r.ht[f, x + 2]], axis=0)


def z_averages(r, deposit=True):
    tmp = r.tmp_f

    def pick(word, up, down, values):
        mid, plus, minus = values
        return mid + jnp.where((word & up) != 0, plus, jnp.where((word & down) != 0, minus, 0.0))

    rows = slice(0, r.lane.shape[0])
    sums, inner_sums = [], []
    for f in range(NFIELD + 1):
        both = r.zw[f, rows] + r.zi[f, rows]
        for i, value in enumerate((both, roll(both, -2), roll(both, 2))):
            ring_store(tmp, (3 * f + i,), value, r.part)
        around = [[ring_load(tmp, (3 * f + i,), step, r.part) for step in (0, 1, -1)] for i in range(3)]
        for word, out in ((r.ow[rows], sums), (r.iw[rows], inner_sums))[1 - deposit :]:
            out.append(pick(word, XU, XD, [pick(word, YU, YD, line) for line in around]))
    inverse = 1.0 / inner_sums[0]
    for f in range(NFIELD):
        r.ai[f, rows] = inner_sums[f + 1] * inverse
    if not deposit:
        return
    word = r.ow[...]
    inverse = 1.0 / sums[0]
    first = 3 * NFIELD + 3
    for f in range(NFIELD):
        v = jnp.where((word & r.inward) != 0, sums[f + 1] * inverse, 0.0)
        totals = []
        for i, bits in enumerate((0, XU, XD)):
            w = jnp.where((word & bits) != 0, v, 0.0) if bits else v
            slot = first + 6 * f + 2 * i
            ring_store(tmp, (slot,), jnp.where((word & YU) != 0, w, 0.0))
            ring_store(tmp, (slot + 1,), jnp.where((word & YD) != 0, w, 0.0))
            totals.append(w + ring_load(tmp, (slot,), -1) + ring_load(tmp, (slot + 1,), 1))
        r.dz[f] = totals[0] + roll(totals[1], 2) + roll(totals[2], -2)


def average(r, layer, rows_of=None):
    rows = r.cy + 8
    tiles = rows // 8
    lane = lanes_of((8, 128))
    for t in range(tiles) if rows_of is None else rows_of:
        at = 8 + 8 * t
        word = r.cw[layer, at : at + 8, :]
        zu, zd = (word & ZU) != 0, (word & ZD) != 0
        yu, yd = (word & YU) != 0, (word & YD) != 0
        xu, xd = (word & XU) != 0, (word & XD) != 0
        sums = []
        for f in range(NFIELD + 1):
            parts = []
            for d in (0, 1, -1):
                line = []
                for e in (0, 1, -1):
                    base = 0 if t == tiles - 1 and e == 1 else at
                    at_e = slice(base + e, base + e + 8)
                    v0, vm, vp = (h[f, layer + d, at_e, :] for h in (r.h0, r.hm, r.hp))
                    line.append(jnp.where(zu, vp, jnp.where(zd, vm, v0)))
                parts.append(line[0] + jnp.where(yu, line[1], jnp.where(yd, line[2], 0.0)))
            sums.append(parts[0] + jnp.where(xu, parts[1], jnp.where(xd, parts[2], 0.0)))
        inverse = 1.0 / sums[0]
        leaves = ((lane == 0) & zd) | ((lane == 127) & zu)
        for f in range(NFIELD):
            column = roll(r.ai[f, 8 * t : 8 * t + 8, :], -2 * layer)
            a = jnp.where(leaves, column, sums[f + 1] * inverse)
            r.av[f, layer, at : at + 8, :] = a
            if t == tiles - 1:
                r.av[f, layer, 0:8, :] = a


def redistribute(r, x, out):
    cx, cy = r.cx, r.cy
    layer = x + 2
    back = -2 * layer
    lane = lanes_of((8, 128))
    first_lane, last_lane = lane == 0, lane == 127
    for t in range(cy // 8):
        at = 8 + 8 * t
        base = [r.av[f, layer, at : at + 8, :] for f in range(NFIELD)]
        word = r.cw[layer, at : at + 8, :]
        up = [jnp.where((word & ZU) != 0, a, 0.0) for a in base]
        down = [jnp.where((word & ZD) != 0, a, 0.0) for a in base]
        for d in (0, 1, -1):
            for e in (0, 1, -1):
                if d == 0 and e == 0:
                    continue
                at_e = slice(at - e, at - e + 8)
                word = r.cw[layer - d, at_e, :]
                bits = (0, XU, XD)[d] | (0, YU, YD)[e]
                here = on(word, bits)
                here_up, here_down = on(word, bits | ZU), on(word, bits | ZD)
                for f in range(NFIELD):
                    a = r.av[f, layer - d, at_e, :]
                    base[f] = base[f] + jnp.where(here, a, 0.0)
                    up[f] = up[f] + jnp.where(here_up, a, 0.0)
                    down[f] = down[f] + jnp.where(here_down, a, 0.0)
        inverse = r.rc[layer, 8 * t : 8 * t + 8, :]
        for f in range(NFIELD):
            halo = roll(r.dz[f, 8 * t : 8 * t + 8, :], back)
            total = base[f] + jnp.where(first_lane, halo, roll(up[f], 1))
            total = total + jnp.where(last_lane, halo, roll(down[f], -1))
            out[pl.ds(pl.multiple_of((f * cx + x) * cy + 8 * t, 8), 8), :] = total * inverse


def common(r, part):
    r.part = part
    r.lane = lanes_of((r.cy + (8 if part == ALL else 0), 128))
    even = (r.lane & 1) == 0
    r.inward = jnp.where(even, ZU, ZD)
    r.outward = jnp.where(even, ZD, ZU)


def z_fields(r, rows, own):
    for f in range(2 * NF):
        value = z_halo(r, f, own)
        if r.outside is not None:
            value = jnp.where(r.outside[: value.shape[0]], EDGE if f % NF >= C1 else 0.0, value)
        r.zf[f, rows] = value


KEPT = ("cw", "zf", "xt", "h0", "hm", "hp", "rc", "av")
SCRATCH = ("ht", "hz", "ow", "iw", "tmp_i", "tmp_f", "ci", "zw", "zi", "ai", "dz")


def plan(cx, nbx, bx):
    if nbx == 2:
        high = bx == 0

        def at(j):
            return jnp.where(high, j + 1, cx + 2 - j)

        return types.SimpleNamespace(
            at=at,
            inner_weigh=[at(j) for j in range(1, cx)],
            inner_average=(1, cx - 2),
            inner_spread=(1, cx - 3),
            outer_weigh=[at(cx)],
            outer_average=[(cx - 1, 3)],
            outer_spread=[(cx - 2, 3)],
            inner_rows=(jnp.where(high, 0, 3), cx - 3),
        )
    return types.SimpleNamespace(
        at=lambda j: j + 1,
        inner_weigh=range(3, cx + 1),
        inner_average=(3, cx - 4),
        inner_spread=(4, cx - 6),
        outer_weigh=[2, cx + 1],
        outer_average=[(0, 3), (cx - 1, 3)],
        outer_spread=[(1, 3), (cx - 2, 3)],
        inner_rows=(3, cx - 6),
    )


def x_lanes(r, high):
    below = (r.lane == 127) | (r.lane <= 2)
    above = (r.lane >= 2 * r.cx + 3) & (r.lane <= 2 * r.cx + 6)
    if isinstance(high, bool):
        return above if high else below
    return (above & high) | (below & jnp.logical_not(high))


def each(span, step):
    def body(j, _):
        step(j)
        return 0

    lax.fori_loop(span[0], span[0] + span[1], body, 0)


def set_outside(r, nbx, bx):
    r.outside = x_lanes(r, bx > 0) if nbx == 2 else None


def early_kernel(cx, cy, nbx, *refs):
    names = ("u", "vf", "zh", "cw_in", *KEPT, "ended", *SCRATCH)
    r = types.SimpleNamespace(cx=cx, cy=cy, **dict(zip(names, refs)))
    common(r, OWN)
    bx, by, bz = place()
    todo = plan(cx, nbx, bx)
    set_outside(r, nbx, bx)
    z_fields(r, slice(0, cy), lambda g: r.zh[g * cy : (g + 1) * cy, :])
    if nbx == 2:
        edge = todo.at(0)
        ring_store(r.cw, (edge,), jnp.ones((cy + 8, 128), jnp.int32))
        for f in range(NFIELD + 1):
            for h in (r.h0, r.hm, r.hp):
                ring_store(h, (f, edge), jnp.zeros((cy + 8, 128), jnp.float32))
    z_counts(r)
    weigh(r, [(layer, functools.partial(own_field, r, layer - 2)) for layer in todo.inner_weigh], OWN)
    z_averages(r, deposit=False)
    each(todo.inner_average, lambda j: average(r, todo.at(j), range(1, cy // 8 - 1)))
    r.ended[...] = r.ci[0:8]


def inner_kernel(cx, cy, nbx, *refs):
    kept_in = len(KEPT)
    names = ("u", "vf", "y_lo", "y_hi")
    rest = refs[len(names) + kept_in :]
    r = types.SimpleNamespace(cx=cx, cy=cy, **dict(zip(names, refs)))
    r.__dict__.update(zip((*KEPT, "res", *SCRATCH), rest))
    common(r, ALL)
    bx, by, bz = place()
    todo = plan(cx, nbx, bx)
    set_outside(r, nbx, bx)
    r.ht[...] = jnp.zeros(r.ht.shape, jnp.float32)
    for x in range(cx):
        y_rows(r, x)
        set_halo_words(r, x + 2)
    n = NF * cx
    for g in range(4):
        for i, row in enumerate((0, 1)):
            r.hz[g, row : row + 1, :] = r.y_hi[n + 2 * g + i : n + 2 * g + i + 1, :]
            r.hz[g, 7 - row : 8 - row, :] = r.y_lo[n + 2 * g + i : n + 2 * g + i + 1, :]
    z_fields(r, slice(cy, cy + 8), lambda g: r.hz[g])
    z_counts(r)
    weigh(r, [(layer, functools.partial(own_field, r, layer - 2)) for layer in todo.inner_weigh], RIM)
    z_averages(r)
    each(todo.inner_average, lambda j: average(r, todo.at(j), (0, cy // 8 - 1, cy // 8)))
    each(todo.inner_spread, lambda j: redistribute(r, todo.at(j) - 2, r.res))


def outer_kernel(cx, cy, nbx, *refs):
    kept_in = len(KEPT)
    names = ("u", "vf", "y_lo", "y_hi", "res", "xa", "xb")
    ins = refs[: len(names)]
    rest = refs[len(names) + kept_in :]
    r = types.SimpleNamespace(cx=cx, cy=cy, **dict(zip(names, ins)))
    r.__dict__.update(zip(("out", *KEPT, *SCRATCH, "rim", "sems"), rest))
    size = cx * cy
    bx, by, bz = place()
    todo = plan(cx, nbx, bx)

    def copy(src, first, count, f, semaphore):
        start = pl.multiple_of(f * size + first * cy, 8)
        part = pl.ds(start, count * cy)
        return pltpu.make_async_copy(src.at[part, :], r.out.at[part, :], r.sems.at[semaphore])

    each((0, NFIELD), lambda f: copy(r.res, *todo.inner_rows, f, f).start())

    def finish_layer(j, first, turn):
        x = todo.at(j) - 2
        redistribute(r, x, r.rim)
        for f in range(NFIELD):
            copy(r.rim, x, 1, f, (turn + j - first) * NFIELD + f).start()

    common(r, ALL)
    x_odd = bx % 2 == 1

    if nbx == 2:
        sides = [(bx == 0, True, lambda first, count: r.xa[first : first + count, :])]
    else:

        def message(high):
            def rows(first, count):
                a, b = r.xa[first : first + count, :], r.xb[first : first + count, :]
                return jnp.where(x_odd, b, a) if high else jnp.where(x_odd, a, b)

            return rows

        sides = [(False, bx > 0, message(False)), (True, bx < nbx - 1, message(True))]

    def choose(high, a, b):
        return (a if high else b) if isinstance(high, bool) else jnp.where(high, a, b)

    def present_or(present, value, edge):
        return value if present is True else jnp.where(present, value, edge)

    zrow = NF * cy
    edges = zrow + 16
    halo = []
    for high, present, part in sides:
        layer, second, own = (choose(high, a, b) for a, b in ((cx + 2, 1), (cx + 3, 0), (cx - 1, 0)))
        y_rows(r, own)

        def raw(f, present=present, part=part):
            return present_or(present, part(f * cy, cy), EDGE if f >= C1 else 0.0)

        for y, row1, row2 in ((0, 7, 6), (1, 0, 1)):
            base = edges + 8 + 10 * y

            def rim(i, edge, base=base, present=present, part=part):
                return present_or(present, part(base + i, 1), edge)

            for f in range(C1):
                r.ht[f, layer, row1 : row1 + 1, :] = rim(f, 0.0)
            r.ht[C1, layer, row1 : row1 + 1, :] = rim(C1, EDGE)
            r.ht[C1, layer, row2 : row2 + 1, :] = rim(C2, EDGE)
            r.ht[C1, second, row1 : row1 + 1, :] = rim(NF, EDGE)
            r.ht[C1, second, row2 : row2 + 1, :] = rim(NF + 1, EDGE)
        set_words(r, raw(C1), layer)
        set_words(r, raw(C2), second)
        halo.append((layer, lambda f, part, raw=raw, layer=layer: jnp.concatenate([raw(f), r.ht[f, layer]], axis=0)))

        edge_rows = part(edges, 8)
        upper_rows = roll(edge_rows, -4)
        for g in range(4):
            for i, row in enumerate((0, 1)):
                at = 2 * g + i
                r.hz[g, row : row + 1, :] = upper_rows[at : at + 1]
                r.hz[g, 7 - row : 8 - row, :] = edge_rows[at : at + 1]
        lanes = x_lanes(r, high)
        for f in range(2 * NF):
            g, k = f // 4, f % 4
            shift = 4 - 2 * cx * k + choose(high, 2 * cx, -2 * cx)
            tile = part(zrow + 8 * (g // 2), 8)
            tiles = [roll(tile, shift - 8 * t - 4 * (g % 2)) for t in range(cy // 8)]
            value = jnp.concatenate([*tiles, roll(r.hz[g], shift)], axis=0)
            r.zf[f] = jnp.where(lanes, present_or(present, value, EDGE if f % NF >= C1 else 0.0), r.zf[f])
    z_counts(r)
    weigh(r, [(layer, functools.partial(own_field, r, layer - 2)) for layer in todo.outer_weigh] + halo, ALL)
    z_averages(r)
    for span in todo.outer_average:
        each(span, lambda j: average(r, todo.at(j)))
    turn = 1
    for first, count in todo.outer_spread:
        each((first, count), lambda j: finish_layer(j, first, turn))
        turn += count
    turn = 1
    for first, count in todo.outer_spread:
        for j in range(first, first + count):
            for f in range(NFIELD):
                copy(r.rim, todo.at(j) - 2, 1, f, turn * NFIELD + f).wait()
            turn += 1
    for f in range(NFIELD):
        copy(r.res, *todo.inner_rows, f, f).wait()


def call(kernel, ins, outs, scratch=(), name=None, grant=8, flops=0, **kwargs):
    return pl.pallas_call(
        kernel,
        in_specs=ins,
        out_specs=tuple(pl.BlockSpec(memory_space=o.memory_space) for o in outs),
        out_shape=tuple(outs),
        scratch_shapes=scratch,
        name=name,
        cost_estimate=pl.CostEstimate(flops=flops, transcendentals=0, bytes_accessed=0),
        compiler_params=pltpu.CompilerParams(vmem_limit_bytes=grant << 20),
        **kwargs,
    )


def per_device(conserved, volume_fraction, cut_mask, merge_code):
    _, cx, cy, cz = cut_mask.shape
    devices = lax.axis_size(AXIS)
    nbx = devices // (NBY * NBZ)
    two_x = nbx > 2
    cells = cx * cy
    u = conserved.reshape(NFIELD * cells, cz)
    vf, mask, code = (a.reshape(cells, cz) for a in (volume_fraction, cut_mask, merge_code))
    f32, i32 = jnp.float32, jnp.int32
    on_chip, far = pl.BlockSpec(memory_space=pltpu.VMEM), pl.BlockSpec(memory_space=pltpu.HBM)

    def vmem(*shape, dtype=f32):
        return pltpu.VMEM((*shape, cz), dtype)

    def swap(value, stride, extent, odd):
        return lax.ppermute(value, AXIS, pairing(stride, extent, devices, odd))

    n = NF * cx
    copies = 2 if two_x else 1
    zp, u, vf, c = call(
        functools.partial(pack_kernel, cx, cy),
        [far] * 4,
        [vmem(2 * cy), vmem(NFIELD * cells), vmem(cells), vmem(cells)],
        [vmem(cells, dtype=i32), vmem(cells, dtype=i32), pltpu.SemaphoreType.DMA((3 + NFIELD,))],
        "pack",
    )(*(pltpu.with_memory_space_constraint(a, pltpu.HBM) for a in (u, vf, mask, code)))
    za, zb = swap(zp, 1, NBZ, False), swap(zp, 1, NBZ, True)
    rows, ring, layers = cy + 8, cy + 24, cx + 4
    cw, ya, yb, *xs = call(
        functools.partial(faces_kernel, cx, cy, two_x),
        [on_chip] * 3,
        [vmem(layers, ring, dtype=i32), vmem(n), vmem(n)] + [vmem(NF * cy)] * copies,
        name="faces",
        flops=1 << 20,
    )(u, vf, c)
    zh, ya, yb = call(
        functools.partial(z_merge_kernel, cx, cy), [on_chip] * 5, [vmem(4 * cy), vmem(n + 8), vmem(n + 8)], name="z_merge"
    )(za, zb, zp, ya, yb)
    kept = [
        vmem(layers, ring, dtype=i32),
        vmem(2 * NF, rows),
        vmem(layers, ring, dtype=i32),
        vmem(NFIELD + 1, layers, ring),
        vmem(NFIELD + 1, layers, ring),
        vmem(NFIELD + 1, layers, ring),
        vmem(layers, cy),
        vmem(NFIELD, layers, ring),
    ]
    scratch = [
        vmem(C2, layers, 8),
        vmem(4, 8),
        vmem(rows, dtype=i32),
        vmem(rows, dtype=i32),
        vmem(2, ring, dtype=i32),
        vmem(9 * NFIELD + 3, ring),
        vmem(rows),
        vmem(NFIELD + 1, rows),
        vmem(NFIELD + 1, rows),
        vmem(NFIELD, rows),
        vmem(NFIELD, rows),
    ]
    yb = swap(yb, NBZ, NBY, True)
    ya = swap(ya, NBZ, NBY, False)
    *state, ended = call(
        functools.partial(early_kernel, cx, cy, nbx),
        [on_chip] * 4,
        kept + [vmem(8)],
        scratch,
        "early",
        flops=1 << 24,
        input_output_aliases={3: 0},
    )(u, vf, zh, cw)
    y_lo, y_hi, *xs = call(
        functools.partial(y_merge_kernel, cx, cy, two_x),
        [on_chip] * (4 + copies),
        [vmem(n + 8), vmem(n + 8)] + [vmem(NF * cy + 48)] * copies,
        name="y_merge",
    )(ended, ya, yb, zh, *xs)
    xs = [swap(x, NBY * NBZ, nbx, odd) for odd, x in enumerate(xs)]
    xa, xb = xs if two_x else xs * 2

    *state, res = call(
        functools.partial(inner_kernel, cx, cy, nbx),
        [on_chip] * (4 + len(kept)),
        kept + [vmem(NFIELD * cells)],
        scratch,
        "inner",
        flops=1 << 26,
        input_output_aliases={4 + i: i for i in range(len(kept))},
    )(u, vf, y_lo, y_hi, *state)
    first = 7
    out, *_ = call(
        functools.partial(outer_kernel, cx, cy, nbx),
        [on_chip] * (first + len(kept)),
        [pltpu.HBM((NFIELD * cells, cz), f32)] + kept,
        scratch + [vmem(NFIELD * cells), pltpu.SemaphoreType.DMA((7 * NFIELD,))],
        "outer",
        flops=1 << 25,
        input_output_aliases={first + i: 1 + i for i in range(len(kept))},
    )(u, vf, y_lo, y_hi, res, xa, xb, *state)
    return out.reshape(conserved.shape)


def solution(mesh):
    return jax.shard_map(
        per_device,
        mesh=mesh,
        in_specs=(
            P(AXIS, None, None, None, None),
            P(AXIS, None, None, None),
            P(AXIS, None, None, None),
            P(AXIS, None, None, None),
        ),
        out_specs=P(AXIS, None, None, None, None),
        check_vma=False,
    )
```

```python
import functools
import types

import jax
import jax.numpy as jnp
from jax import lax
from jax.experimental import pallas as pl
from jax.experimental.pallas import tpu as pltpu
from jax.sharding import PartitionSpec as P

NBY = 4
NBZ = 4
AXIS = "boxes"

NFIELD = 5
VF = 5
C1 = 6
C2 = 7
NF = 8
ZU, ZD, YU, YD, XU, XD = 16, 256, 4, 4096, 1 << 28, 1 << 29
LOW = (1 << 24) - 1
EDGE = 13.0


def pairing(stride, extent, devices, odd):
    pairs = []
    for i in range(devices):
        c = i // stride % extent
        partner = ((c + 1) ^ 1) - 1 if odd else c ^ 1
        pairs.append((i, i + (partner % extent - c) * stride))
    return pairs


def lanes_of(shape):
    return lax.broadcasted_iota(jnp.int32, shape, len(shape) - 1)


def roll(value, shift, axis=1):
    if isinstance(shift, int):
        shift %= value.shape[axis]
        if shift == 0:
            return value
    else:
        shift &= value.shape[axis] - 1
    return pltpu.roll(value, shift, axis)


def place():
    me = lax.axis_index(AXIS)
    return me // (NBY * NBZ), me // NBZ % NBY, me % NBZ


def decode(code):
    qx = (code * 57) >> 9
    rest = code - 9 * qx
    qy = (rest * 11) >> 5
    qz = rest - 3 * qy
    word = 1 + jnp.where(qz == 2, ZU, 0) + jnp.where(qz == 0, ZD, 0)
    word = word * jnp.where(qy == 2, 1 + YU, jnp.where(qy == 0, 1 + YD, 1))
    return word | jnp.where(qx == 2, XU, jnp.where(qx == 0, XD, 0))


def on(word, bits):
    return (word & bits) == bits


ALL, OWN, RIM = "all", "own", "rim"


def ring_store(ref, lead, value, part=ALL):
    def put(first, rows):
        ref[(*lead, slice(first, first + rows.shape[0]), slice(None))] = rows

    if part == RIM:
        put(8, value[16:])
        put(ref.shape[-2] - 24, value[:16])
        put(0, value[8:16])
    else:
        put(8, value)
        if part == ALL:
            put(0, value[-8:])


def ring_load(ref, lead, step, part=ALL):
    n = ref.shape[-2] - 16

    def get(first, last):
        return ref[(*lead, slice(first + step, last + step), slice(None))]

    if part == OWN:
        return get(8, n)
    if part == RIM:
        spans = [(n - 8, n), (0, 16)] if step > 0 else [(n - 8, n + 8), (8, 16)]
    else:
        spans = [(8, n), (0, 8)] if step > 0 else [(8, n + 8)]
    return jnp.concatenate([get(*span) for span in spans], axis=0)


def cut(value, part):
    if part == ALL:
        return value
    n = value.shape[0] - 8
    return value[:n] if part == OWN else jnp.concatenate([value[n - 8 :], value[:8]], axis=0)


def pack_kernel(cx, cy, u_in, vf_in, mask_in, code_in, zp, z_a, z_b, u, vf, c, mask, code, sems):
    copies = [
        pltpu.make_async_copy(mask_in, mask, sems.at[0]),
        pltpu.make_async_copy(code_in, code, sems.at[1]),
        pltpu.make_async_copy(vf_in, vf, sems.at[2]),
    ]
    for f in range(NFIELD):
        rows = pl.ds(f * cx * cy, cx * cy)
        copies.append(pltpu.make_async_copy(u_in.at[rows, :], u.at[rows, :], sems.at[3 + f]))
    for copy in copies:
        copy.start()
    lane = lanes_of((cy, 128))
    slot = ((lane + 1) & 127) >> 1
    low_lane = (lane & 1) == 0
    copies[0].wait()
    copies[1].wait()
    for x in range(cx):
        rows = pl.ds(x * cy, cy)
        c[rows, :] = jnp.where(mask[rows, :] == 1, code[rows, :], 13).astype(jnp.float32)
    for g in (1, 0):
        acc = jnp.zeros((cy, 128), jnp.float32)
        for k in (3, 2, 1, 0):
            f = 4 * g + k
            if f <= VF:
                copies[3 + f if f < VF else 2].wait()
            for x in range(cx):
                m = cx * k + x
                rows = pl.ds(x * cy, cy)
                if f < NFIELD:
                    part = roll(u[pl.ds((f * cx + x) * cy, cy), :], 2 * m)
                elif f < C2:
                    part = roll((vf if f == VF else c)[rows, :], 2 * m)
                else:
                    part = jnp.where(low_lane, roll(c[rows, :], 2 * m - 1), roll(c[rows, :], 2 * m + 1))
                acc = jnp.where(slot == m, part, acc)
        zp[g * cy : (g + 1) * cy, :] = acc
        if g:
            second = acc
    high = jnp.where(low_lane, roll(second, 1), acc)
    low = jnp.where(low_lane, acc, roll(second, -1))
    odd = place()[2] % 2 == 1
    z_a[...] = jnp.where(odd, low, high)
    z_b[...] = jnp.where(odd, high, low)


def faces_kernel(cx, cy, two_x, u, vf, c, cw, y_a, y_b, *xs):
    bx, by, bz = place()
    for x in range(cx):
        cw[x + 2, 8 : 8 + cy, :] = decode(c[x * cy : (x + 1) * cy, :].astype(jnp.int32))

    def y_face(out, high):
        rim = jnp.where(high, cy - 1, 0)
        second = jnp.where(high, cy - 2, 1)

        def column(ref, base, row):
            return ref[pl.ds(base + row, cx, stride=cy), :]

        for f in range(NFIELD):
            out[f * cx : (f + 1) * cx, :] = column(u, f * cx * cy, rim)
        out[VF * cx : (VF + 1) * cx, :] = column(vf, 0, rim)
        out[C1 * cx : (C1 + 1) * cx, :] = column(c, 0, rim)
        out[C2 * cx : (C2 + 1) * cx, :] = column(c, 0, second)

    y_face(y_a, by % 2 == 0)
    y_face(y_b, by % 2 == 1)

    def x_face(out, high):
        rim = jnp.where(high, cx - 1, 0) * cy
        second = jnp.where(high, cx - 2, 1) * cy

        def rows(base, start):
            return pl.ds(pl.multiple_of(base + start, 8), cy)

        for f in range(NFIELD):
            out[f * cy : (f + 1) * cy, :] = u[rows(f * cx * cy, rim), :]
        out[VF * cy : (VF + 1) * cy, :] = vf[rows(0, rim), :]
        out[C1 * cy : (C1 + 1) * cy, :] = c[rows(0, rim), :]
        out[C2 * cy : (C2 + 1) * cy, :] = c[rows(0, second), :]

    x_face(xs[0], bx % 2 == 0)
    if two_x:
        x_face(xs[1], bx % 2 == 1)


def z_merge_kernel(cx, cy, r_a, r_b, zp, ya_in, yb_in, zh, y_a, y_b):
    bx, by, bz = place()
    odd = bz % 2 == 1
    lane = lanes_of((cy, 128))
    low_lane = (lane & 1) == 0
    codes = (lane >= 63) & (lane <= 126)
    a, b = r_a[...], r_b[...]
    below, above = jnp.where(odd, a, b), jnp.where(odd, b, a)
    for g in range(2):
        edge = jnp.where(codes, EDGE, 0.0) if g else jnp.zeros((cy, 128), jnp.float32)
        low = jnp.where(bz > 0, below if g else roll(below, 1), edge)
        high = jnp.where(bz < NBZ - 1, above if g else roll(above, -1), edge)
        zh[g * cy : (g + 1) * cy, :] = jnp.where(low_lane, low, high)
    zh[2 * cy :, :] = zp[...]
    n = NF * cx

    def finish(out, main, high):
        out[:n, :] = main[...]
        rim = jnp.where(high, cy - 1, 0)
        second = jnp.where(high, cy - 2, 1)
        for g in range(4):
            out[n + 2 * g : n + 2 * g + 1, :] = zh[pl.ds(g * cy + rim, 1), :]
            out[n + 2 * g + 1 : n + 2 * g + 2, :] = zh[pl.ds(g * cy + second, 1), :]

    finish(y_a, ya_in, by % 2 == 0)
    finish(y_b, yb_in, by % 2 == 1)


def z_edge_rows(cx):
    n = NF * cx
    row = lax.broadcasted_iota(jnp.int32, (n + 8, 128), 0)
    lane = lanes_of((n + 8, 128))
    codes = ((row >= C1 * cx) & (row < n)) | ((row >= n) & ((row & 2) != 0) & (lane >= 63) & (lane <= 126))
    return jnp.where(codes, EDGE, 0.0)


def y_merge_kernel(cx, cy, two_x, ended, r_a, r_b, zh, *refs):
    copies = 2 if two_x else 1
    mains, (y_lo, y_hi), xs = refs[:copies], refs[copies : copies + 2], refs[copies + 2 :]
    bx, by, bz = place()
    odd = by % 2 == 1
    edge = z_edge_rows(cx)
    a, b = r_a[...], r_b[...]
    y_lo[...] = jnp.where(by > 0, jnp.where(odd, a, b), edge)
    y_hi[...] = jnp.where(by < NBY - 1, jnp.where(odd, b, a), edge)
    n = NF * cx

    def x_rim(out, main, high):
        rim = jnp.where(high, cx - 1, 0)
        second = jnp.where(high, cx - 2, 1)
        at = NF * cy
        out[:at, :] = main[...]
        lane = lanes_of((8, 128))
        spot = (lane - jnp.where(high, 2 * cx - 5, 2 * cx - 1)) & (2 * cx - 1)
        for half in range(2):
            tile = jnp.zeros((8, 128), jnp.float32)
            for t in range(cy // 8):
                for g in range(2):
                    start, row = 8 * t + 4 * g, (2 * half + g) * cy + 8 * t
                    tile = jnp.where((spot >= start) & (spot < start + 4), roll(zh[row : row + 8, :], start), tile)
            out[at : at + 8, :] = tile
            at += 8
        low, up = y_lo[n : n + 8, :], y_hi[n : n + 8, :]
        out[at : at + 8, :] = jnp.where(spot < 4, low, roll(up, 4))
        at += 8
        for y in (y_lo, y_hi):
            for f in range(NF):
                out[at : at + 1, :] = y[pl.ds(f * cx + rim, 1), :]
                at += 1
            for f in (C1, C2):
                out[at : at + 1, :] = y[pl.ds(f * cx + second, 1), :]
                at += 1
        out[at:, :] = jnp.zeros((out.shape[0] - at, 128), jnp.float32)

    x_rim(xs[0], mains[0], bx % 2 == 0)
    if two_x:
        x_rim(xs[1], mains[1], bx % 2 == 1)


def y_rows(r, x):
    cx = r.cx
    for f in range(C2):
        r.ht[f, x + 2, 0:1, :] = r.y_hi[pl.ds(f * cx + x, 1), :]
        r.ht[f, x + 2, 7:8, :] = r.y_lo[pl.ds(f * cx + x, 1), :]
    r.ht[C1, x + 2, 1:2, :] = r.y_hi[pl.ds(C2 * cx + x, 1), :]
    r.ht[C1, x + 2, 6:7, :] = r.y_lo[pl.ds(C2 * cx + x, 1), :]


def set_words(r, own, layer):
    both = jnp.concatenate([own, r.ht[C1, layer]], axis=0)
    ring_store(r.cw, (layer,), decode(both.astype(jnp.int32)))


def set_halo_words(r, layer):
    words = decode(r.ht[C1, layer].astype(jnp.int32))
    r.cw[layer, 0:8, :] = words
    r.cw[layer, 8 + r.cy : 16 + r.cy, :] = words


def z_halo(r, f, own):
    g, k = f // 4, f % 4
    return roll(own(g), 4 - 2 * r.cx * k)


def spread_counts(r, planes, slot):
    mid = up = down = jnp.zeros(r.lane.shape, jnp.int32)
    for word, bits in planes:
        v = 1 + ((word & YU) << 6) + ((word & YD) << 4)
        if bits is not None:
            v = jnp.where((word & bits) != 0, v, 0)
        mid = mid + v
        up = up + jnp.where((word & XU) != 0, v, 0)
        down = down + jnp.where((word & XD) != 0, v, 0)
    total = mid + roll(up, 2) + roll(down, -2)
    ring_store(r.tmp_i, (slot,), total, r.part)
    before, after = (ring_load(r.tmp_i, (slot,), step, r.part) for step in (-1, 1))
    return (total & 255) + ((before >> 8) & 255) + ((after >> 16) & 255)


def z_counts(r):
    rows = slice(0, r.lane.shape[0])
    outer1, outer2, inner1, inner2 = (decode(r.zf[f, rows].astype(jnp.int32)) for f in (C1, C2, NF + C1, NF + C2))
    r.ow[rows], r.iw[rows] = outer1, inner1
    planes = ((outer1, None), (outer2, r.inward), (inner1, r.outward)), ((inner1, None), (outer1, r.inward), (inner2, r.outward))
    for first, out, plane in zip((0, NF), (r.zw, r.zi), planes):
        inverse = 1.0 / spread_counts(r, plane, first // NF).astype(jnp.float32)
        weight = r.zf[first + VF, rows] * inverse
        out[0, rows] = weight
        for f in range(NFIELD):
            out[f + 1, rows] = weight * r.zf[first + f, rows]
    r.ci[rows] = inverse


def sum_x(mid, left, right):
    total = (mid & LOW) + jnp.where((left & XU) != 0, left & LOW, 0)
    return total + jnp.where((right & XD) != 0, right & LOW, 0)


def weigh(r, group, part):
    n = r.cy
    lane = lanes_of(({ALL: n + 8, OWN: n, RIM: 24}[part], 128))
    edge_lane = (lane == 0) | (lane == 127)
    totals = []
    for layer, _ in group:
        if part == RIM:
            total = sum_x(*(r.cw[layer + d, 8 + n : 16 + n, :] for d in (0, -1, 1)))
            r.xt[layer, 8 + n : 16 + n, :] = total
            r.xt[layer, 0:8, :] = total
        else:
            ring_store(r.xt, (layer,), sum_x(*(ring_load(r.cw, (layer + d,), 0, part) for d in (0, -1, 1))), part)
    for layer, _ in group:
        total, before, after = (ring_load(r.xt, (layer,), step, part) for step in (0, -1, 1))
        total = (total & 0x333) + ((before >> 2) & 0x333) + ((after >> 12) & 0x333)
        totals.append((total, roll(total, 1), roll(total, -1), roll(cut(r.ci[...], part), -2 * layer)))
    for (layer, field), (total, below, above, edge) in zip(group, totals):
        count = (total & 15) + ((below >> 4) & 15) + ((above >> 8) & 15)
        inverse = jnp.where(edge_lane, edge, 1.0 / count.astype(jnp.float32))
        if part == RIM:
            r.rc[layer, n - 8 :], r.rc[layer, 0:8] = inverse[:8], inverse[16:]
        else:
            r.rc[layer] = inverse[:n]
        ring_store(r.h0, (0, layer), field(VF, part) * inverse, part)
    for layer, field in group:
        weight = ring_load(r.h0, (0, layer), 0, part)
        for f in range(NFIELD + 1):
            w = weight
            if f:
                w = weight * field(f - 1, part)
                ring_store(r.h0, (f, layer), w, part)
            ring_store(r.hm, (f, layer), w + roll(w, 1), part)
            ring_store(r.hp, (f, layer), w + roll(w, -1), part)


def own_field(r, x, f, part):
    base = (f * r.cx + x if f < NFIELD else x) * r.cy
    ref = r.u if f < NFIELD else r.vf

    def rows(first, count):
        start = base + first
        return ref[pl.ds(start if isinstance(start, int) else pl.multiple_of(start, 8), count), :]

    if part == OWN:
        return rows(0, r.cy)
    if part == RIM:
        return jnp.concatenate([rows(r.cy - 8, 8), r.ht[f, x + 2], rows(0, 8)], axis=0)
    return jnp.concatenate([rows(0, r.cy), r.ht[f, x + 2]], axis=0)


def z_averages(r, deposit=True):
    tmp = r.tmp_f

    def pick(word, up, down, values):
        mid, plus, minus = values
        return mid + jnp.where((word & up) != 0, plus, jnp.where((word & down) != 0, minus, 0.0))

    rows = slice(0, r.lane.shape[0])
    sums, inner_sums = [], []
    for f in range(NFIELD + 1):
        both = r.zw[f, rows] + r.zi[f, rows]
        for i, value in enumerate((both, roll(both, -2), roll(both, 2))):
            ring_store(tmp, (3 * f + i,), value, r.part)
        around = [[ring_load(tmp, (3 * f + i,), step, r.part) for step in (0, 1, -1)] for i in range(3)]
        for word, out in ((r.ow[rows], sums), (r.iw[rows], inner_sums))[1 - deposit :]:
            out.append(pick(word, XU, XD, [pick(word, YU, YD, line) for line in around]))
    inverse = 1.0 / inner_sums[0]
    for f in range(NFIELD):
        r.ai[f, rows] = inner_sums[f + 1] * inverse
    if not deposit:
        return
    word = r.ow[...]
    inverse = 1.0 / sums[0]
    first = 3 * NFIELD + 3
    for f in range(NFIELD):
        v = jnp.where((word & r.inward) != 0, sums[f + 1] * inverse, 0.0)
        totals = []
        for i, bits in enumerate((0, XU, XD)):
            w = jnp.where((word & bits) != 0, v, 0.0) if bits else v
            slot = first + 6 * f + 2 * i
            ring_store(tmp, (slot,), jnp.where((word & YU) != 0, w, 0.0))
            ring_store(tmp, (slot + 1,), jnp.where((word & YD) != 0, w, 0.0))
            totals.append(w + ring_load(tmp, (slot,), -1) + ring_load(tmp, (slot + 1,), 1))
        r.dz[f] = totals[0] + roll(totals[1], 2) + roll(totals[2], -2)


def average(r, layer, rows_of=None):
    rows = r.cy + 8
    tiles = rows // 8
    lane = lanes_of((8, 128))
    for t in range(tiles) if rows_of is None else rows_of:
        at = 8 + 8 * t
        word = r.cw[layer, at : at + 8, :]
        zu, zd = (word & ZU) != 0, (word & ZD) != 0
        yu, yd = (word & YU) != 0, (word & YD) != 0
        xu, xd = (word & XU) != 0, (word & XD) != 0
        sums = []
        for f in range(NFIELD + 1):
            parts = []
            for d in (0, 1, -1):
                line = []
                for e in (0, 1, -1):
                    base = 0 if t == tiles - 1 and e == 1 else at
                    at_e = slice(base + e, base + e + 8)
                    v0, vm, vp = (h[f, layer + d, at_e, :] for h in (r.h0, r.hm, r.hp))
                    line.append(jnp.where(zu, vp, jnp.where(zd, vm, v0)))
                parts.append(line[0] + jnp.where(yu, line[1], jnp.where(yd, line[2], 0.0)))
            sums.append(parts[0] + jnp.where(xu, parts[1], jnp.where(xd, parts[2], 0.0)))
        inverse = 1.0 / sums[0]
        leaves = ((lane == 0) & zd) | ((lane == 127) & zu)
        for f in range(NFIELD):
            column = roll(r.ai[f, 8 * t : 8 * t + 8, :], -2 * layer)
            a = jnp.where(leaves, column, sums[f + 1] * inverse)
            r.av[f, layer, at : at + 8, :] = a
            if t == tiles - 1:
                r.av[f, layer, 0:8, :] = a


def redistribute(r, x, out):
    cx, cy = r.cx, r.cy
    layer = x + 2
    back = -2 * layer
    lane = lanes_of((8, 128))
    first_lane, last_lane = lane == 0, lane == 127
    for t in range(cy // 8):
        at = 8 + 8 * t
        base = [r.av[f, layer, at : at + 8, :] for f in range(NFIELD)]
        word = r.cw[layer, at : at + 8, :]
        up = [jnp.where((word & ZU) != 0, a, 0.0) for a in base]
        down = [jnp.where((word & ZD) != 0, a, 0.0) for a in base]
        for d in (0, 1, -1):
            for e in (0, 1, -1):
                if d == 0 and e == 0:
                    continue
                at_e = slice(at - e, at - e + 8)
                word = r.cw[layer - d, at_e, :]
                bits = (0, XU, XD)[d] | (0, YU, YD)[e]
                here = on(word, bits)
                here_up, here_down = on(word, bits | ZU), on(word, bits | ZD)
                for f in range(NFIELD):
                    a = r.av[f, layer - d, at_e, :]
                    base[f] = base[f] + jnp.where(here, a, 0.0)
                    up[f] = up[f] + jnp.where(here_up, a, 0.0)
                    down[f] = down[f] + jnp.where(here_down, a, 0.0)
        inverse = r.rc[layer, 8 * t : 8 * t + 8, :]
        for f in range(NFIELD):
            halo = roll(r.dz[f, 8 * t : 8 * t + 8, :], back)
            total = base[f] + jnp.where(first_lane, halo, roll(up[f], 1))
            total = total + jnp.where(last_lane, halo, roll(down[f], -1))
            out[f, pl.ds(pl.multiple_of(x * cy + 8 * t, 8), 8), :] = total * inverse


def common(r, part):
    r.part = part
    r.lane = lanes_of((r.cy + (8 if part == ALL else 0), 128))
    even = (r.lane & 1) == 0
    r.inward = jnp.where(even, ZU, ZD)
    r.outward = jnp.where(even, ZD, ZU)


def z_fields(r, rows, own):
    for f in range(2 * NF):
        value = z_halo(r, f, own)
        if r.outside is not None:
            value = jnp.where(r.outside[: value.shape[0]], EDGE if f % NF >= C1 else 0.0, value)
        r.zf[f, rows] = value


KEPT = ("cw", "zf", "xt", "h0", "hm", "hp", "rc", "av")
SCRATCH = ("ht", "hz", "ow", "iw", "tmp_i", "tmp_f", "ci", "zw", "zi", "ai", "dz")


def plan(cx, nbx, bx):
    if nbx == 2:
        high = bx == 0

        def at(j):
            return jnp.where(high, j + 1, cx + 2 - j)

        return types.SimpleNamespace(
            at=at,
            inner_weigh=[at(j) for j in range(1, cx)],
            inner_average=(1, cx - 2),
            inner_spread=(1, cx - 3),
            outer_weigh=[at(cx)],
            outer_average=[(cx - 1, 3)],
            outer_spread=[(cx - 2, 3)],
            inner_rows=(jnp.where(high, 0, 3), cx - 3),
        )
    return types.SimpleNamespace(
        at=lambda j: j + 1,
        inner_weigh=range(3, cx + 1),
        inner_average=(3, cx - 4),
        inner_spread=(4, cx - 6),
        outer_weigh=[2, cx + 1],
        outer_average=[(0, 3), (cx - 1, 3)],
        outer_spread=[(1, 3), (cx - 2, 3)],
        inner_rows=(3, cx - 6),
    )


def x_lanes(r, high):
    below = (r.lane == 127) | (r.lane <= 2)
    above = (r.lane >= 2 * r.cx + 3) & (r.lane <= 2 * r.cx + 6)
    if isinstance(high, bool):
        return above if high else below
    return (above & high) | (below & jnp.logical_not(high))


def each(span, step):
    def body(j, _):
        step(j)
        return 0

    lax.fori_loop(span[0], span[0] + span[1], body, 0)


def set_outside(r, nbx, bx):
    r.outside = x_lanes(r, bx > 0) if nbx == 2 else None


def early_kernel(cx, cy, nbx, *refs):
    names = ("u", "vf", "zh", "cw_in", *KEPT, "ended", *SCRATCH)
    r = types.SimpleNamespace(cx=cx, cy=cy, **dict(zip(names, refs)))
    common(r, OWN)
    bx, by, bz = place()
    todo = plan(cx, nbx, bx)
    set_outside(r, nbx, bx)
    z_fields(r, slice(0, cy), lambda g: r.zh[g * cy : (g + 1) * cy, :])
    if nbx == 2:
        edge = todo.at(0)
        ring_store(r.cw, (edge,), jnp.ones((cy + 8, 128), jnp.int32))
        for f in range(NFIELD + 1):
            for h in (r.h0, r.hm, r.hp):
                ring_store(h, (f, edge), jnp.zeros((cy + 8, 128), jnp.float32))
    z_counts(r)
    weigh(r, [(layer, functools.partial(own_field, r, layer - 2)) for layer in todo.inner_weigh], OWN)
    z_averages(r, deposit=False)
    each(todo.inner_average, lambda j: average(r, todo.at(j), range(1, cy // 8 - 1)))
    r.ended[...] = r.ci[0:8]


def inner_kernel(cx, cy, nbx, *refs):
    kept_in = len(KEPT)
    names = ("u", "vf", "y_lo", "y_hi")
    rest = refs[len(names) + kept_in :]
    r = types.SimpleNamespace(cx=cx, cy=cy, **dict(zip(names, refs)))
    r.__dict__.update(zip((*KEPT, "res", *SCRATCH), rest))
    common(r, ALL)
    bx, by, bz = place()
    todo = plan(cx, nbx, bx)
    set_outside(r, nbx, bx)
    r.ht[...] = jnp.zeros(r.ht.shape, jnp.float32)
    for x in range(cx):
        y_rows(r, x)
        set_halo_words(r, x + 2)
    n = NF * cx
    for g in range(4):
        for i, row in enumerate((0, 1)):
            r.hz[g, row : row + 1, :] = r.y_hi[n + 2 * g + i : n + 2 * g + i + 1, :]
            r.hz[g, 7 - row : 8 - row, :] = r.y_lo[n + 2 * g + i : n + 2 * g + i + 1, :]
    z_fields(r, slice(cy, cy + 8), lambda g: r.hz[g])
    z_counts(r)
    weigh(r, [(layer, functools.partial(own_field, r, layer - 2)) for layer in todo.inner_weigh], RIM)
    z_averages(r)
    each(todo.inner_average, lambda j: average(r, todo.at(j), (0, cy // 8 - 1, cy // 8)))
    each(todo.inner_spread, lambda j: redistribute(r, todo.at(j) - 2, r.res))


def outer_kernel(cx, cy, nbx, *refs):
    kept_in = len(KEPT)
    names = ("u", "vf", "y_lo", "y_hi", "res", "xa", "xb")
    ins = refs[: len(names)]
    rest = refs[len(names) + kept_in :]
    r = types.SimpleNamespace(cx=cx, cy=cy, **dict(zip(names, ins)))
    r.__dict__.update(zip(("out", *KEPT, *SCRATCH, "rim", "sems"), rest))
    bx, by, bz = place()
    todo = plan(cx, nbx, bx)

    def copy(src, first, count, semaphore):
        part = pl.ds(pl.multiple_of(first * cy, 8), count * cy)
        return pltpu.make_async_copy(src.at[:, part, :], r.out.at[:, part, :], r.sems.at[semaphore])

    each((0, 2), lambda i: pl.when(i == 0)(lambda: copy(r.res, *todo.inner_rows, 0).start()))

    def finish_layer(j, first, turn):
        x = todo.at(j) - 2
        redistribute(r, x, r.rim)
        copy(r.rim, x, 1, turn + j - first).start()

    common(r, ALL)
    x_odd = bx % 2 == 1

    if nbx == 2:
        sides = [(bx == 0, True, lambda first, count: r.xa[first : first + count, :])]
    else:

        def message(high):
            def rows(first, count):
                a, b = r.xa[first : first + count, :], r.xb[first : first + count, :]
                return jnp.where(x_odd, b, a) if high else jnp.where(x_odd, a, b)

            return rows

        sides = [(False, bx > 0, message(False)), (True, bx < nbx - 1, message(True))]

    def choose(high, a, b):
        return (a if high else b) if isinstance(high, bool) else jnp.where(high, a, b)

    def present_or(present, value, edge):
        return value if present is True else jnp.where(present, value, edge)

    zrow = NF * cy
    edges = zrow + 16
    halo = []
    for high, present, part in sides:
        layer, second, own = (choose(high, a, b) for a, b in ((cx + 2, 1), (cx + 3, 0), (cx - 1, 0)))
        y_rows(r, own)

        def raw(f, present=present, part=part):
            return present_or(present, part(f * cy, cy), EDGE if f >= C1 else 0.0)

        for y, row1, row2 in ((0, 7, 6), (1, 0, 1)):
            base = edges + 8 + 10 * y

            def rim(i, edge, base=base, present=present, part=part):
                return present_or(present, part(base + i, 1), edge)

            for f in range(C1):
                r.ht[f, layer, row1 : row1 + 1, :] = rim(f, 0.0)
            r.ht[C1, layer, row1 : row1 + 1, :] = rim(C1, EDGE)
            r.ht[C1, layer, row2 : row2 + 1, :] = rim(C2, EDGE)
            r.ht[C1, second, row1 : row1 + 1, :] = rim(NF, EDGE)
            r.ht[C1, second, row2 : row2 + 1, :] = rim(NF + 1, EDGE)
        set_words(r, raw(C1), layer)
        set_words(r, raw(C2), second)
        halo.append((layer, lambda f, part, raw=raw, layer=layer: jnp.concatenate([raw(f), r.ht[f, layer]], axis=0)))

        edge_rows = part(edges, 8)
        upper_rows = roll(edge_rows, -4)
        for g in range(4):
            for i, row in enumerate((0, 1)):
                at = 2 * g + i
                r.hz[g, row : row + 1, :] = upper_rows[at : at + 1]
                r.hz[g, 7 - row : 8 - row, :] = edge_rows[at : at + 1]
        lanes = x_lanes(r, high)
        for f in range(2 * NF):
            g, k = f // 4, f % 4
            shift = 4 - 2 * cx * k + choose(high, 2 * cx, -2 * cx)
            tile = part(zrow + 8 * (g // 2), 8)
            tiles = [roll(tile, shift - 8 * t - 4 * (g % 2)) for t in range(cy // 8)]
            value = jnp.concatenate([*tiles, roll(r.hz[g], shift)], axis=0)
            r.zf[f] = jnp.where(lanes, present_or(present, value, EDGE if f % NF >= C1 else 0.0), r.zf[f])
    z_counts(r)
    weigh(r, [(layer, functools.partial(own_field, r, layer - 2)) for layer in todo.outer_weigh] + halo, ALL)
    z_averages(r)
    for span in todo.outer_average:
        each(span, lambda j: average(r, todo.at(j)))
    turn = 1
    for first, count in todo.outer_spread:
        each((first, count), lambda j: finish_layer(j, first, turn))
        turn += count
    turn = 1
    for first, count in todo.outer_spread:
        for j in range(first, first + count):
            copy(r.rim, todo.at(j) - 2, 1, turn).wait()
            turn += 1
    copy(r.res, *todo.inner_rows, 0).wait()


def call(kernel, ins, outs, scratch=(), name=None, grant=8, flops=0, **kwargs):
    return pl.pallas_call(
        kernel,
        in_specs=ins,
        out_specs=tuple(pl.BlockSpec(memory_space=o.memory_space) for o in outs),
        out_shape=tuple(outs),
        scratch_shapes=scratch,
        name=name,
        cost_estimate=pl.CostEstimate(flops=flops, transcendentals=0, bytes_accessed=0),
        compiler_params=pltpu.CompilerParams(vmem_limit_bytes=grant << 20),
        **kwargs,
    )


def per_device(conserved, volume_fraction, cut_mask, merge_code):
    _, cx, cy, cz = cut_mask.shape
    devices = lax.axis_size(AXIS)
    nbx = devices // (NBY * NBZ)
    two_x = nbx > 2
    cells = cx * cy
    u = conserved.reshape(NFIELD * cells, cz)
    vf, mask, code = (a.reshape(cells, cz) for a in (volume_fraction, cut_mask, merge_code))
    f32, i32 = jnp.float32, jnp.int32
    on_chip, far = pl.BlockSpec(memory_space=pltpu.VMEM), pl.BlockSpec(memory_space=pltpu.HBM)

    def vmem(*shape, dtype=f32):
        return pltpu.VMEM((*shape, cz), dtype)

    def swap(value, stride, extent, odd):
        return lax.ppermute(value, AXIS, pairing(stride, extent, devices, odd))

    n = NF * cx
    copies = 2 if two_x else 1
    zp, za, zb, u, vf, c = call(
        functools.partial(pack_kernel, cx, cy),
        [far] * 4,
        [vmem(2 * cy), vmem(cy), vmem(cy), vmem(NFIELD * cells), vmem(cells), vmem(cells)],
        [vmem(cells, dtype=i32), vmem(cells, dtype=i32), pltpu.SemaphoreType.DMA((3 + NFIELD,))],
        "pack",
    )(*(pltpu.with_memory_space_constraint(a, pltpu.HBM) for a in (u, vf, mask, code)))
    za, zb = swap(za, 1, NBZ, False), swap(zb, 1, NBZ, True)
    rows, ring, layers = cy + 8, cy + 24, cx + 4
    cw, ya, yb, *xs = call(
        functools.partial(faces_kernel, cx, cy, two_x),
        [on_chip] * 3,
        [vmem(layers, ring, dtype=i32), vmem(n), vmem(n)] + [vmem(NF * cy)] * copies,
        name="faces",
        flops=1 << 20,
    )(u, vf, c)
    zh, ya, yb = call(
        functools.partial(z_merge_kernel, cx, cy), [on_chip] * 5, [vmem(4 * cy), vmem(n + 8), vmem(n + 8)], name="z_merge"
    )(za, zb, zp, ya, yb)
    kept = [
        vmem(layers, ring, dtype=i32),
        vmem(2 * NF, rows),
        vmem(layers, ring, dtype=i32),
        vmem(NFIELD + 1, layers, ring),
        vmem(NFIELD + 1, layers, ring),
        vmem(NFIELD + 1, layers, ring),
        vmem(layers, cy),
        vmem(NFIELD, layers, ring),
    ]
    scratch = [
        vmem(C2, layers, 8),
        vmem(4, 8),
        vmem(rows, dtype=i32),
        vmem(rows, dtype=i32),
        vmem(2, ring, dtype=i32),
        vmem(9 * NFIELD + 3, ring),
        vmem(rows),
        vmem(NFIELD + 1, rows),
        vmem(NFIELD + 1, rows),
        vmem(NFIELD, rows),
        vmem(NFIELD, rows),
    ]
    yb = swap(yb, NBZ, NBY, True)
    ya = swap(ya, NBZ, NBY, False)
    *state, ended = call(
        functools.partial(early_kernel, cx, cy, nbx),
        [on_chip] * 4,
        kept + [vmem(8)],
        scratch,
        "early",
        flops=1 << 24,
        input_output_aliases={3: 0},
    )(u, vf, zh, cw)
    y_lo, y_hi, *xs = call(
        functools.partial(y_merge_kernel, cx, cy, two_x),
        [on_chip] * (4 + copies),
        [vmem(n + 8), vmem(n + 8)] + [vmem(NF * cy + 48)] * copies,
        name="y_merge",
    )(ended, ya, yb, zh, *xs)
    xs = [swap(x, NBY * NBZ, nbx, odd) for odd, x in enumerate(xs)]
    xa, xb = xs if two_x else xs * 2

    *state, res = call(
        functools.partial(inner_kernel, cx, cy, nbx),
        [on_chip] * (4 + len(kept)),
        kept + [vmem(NFIELD, cells)],
        scratch,
        "inner",
        flops=1 << 26,
        input_output_aliases={4 + i: i for i in range(len(kept))},
    )(u, vf, y_lo, y_hi, *state)
    first = 7
    out, *_ = call(
        functools.partial(outer_kernel, cx, cy, nbx),
        [on_chip] * (first + len(kept)),
        [pltpu.HBM((NFIELD, cells, cz), f32)] + kept,
        scratch + [vmem(NFIELD, cells), pltpu.SemaphoreType.DMA((7,))],
        "outer",
        flops=1 << 25,
        input_output_aliases={first + i: 1 + i for i in range(len(kept))},
    )(u, vf, y_lo, y_hi, res, xa, xb, *state)
    return out.reshape(conserved.shape)


def solution(mesh):
    return jax.shard_map(
        per_device,
        mesh=mesh,
        in_specs=(
            P(AXIS, None, None, None, None),
            P(AXIS, None, None, None),
            P(AXIS, None, None, None),
            P(AXIS, None, None, None),
        ),
        out_specs=P(AXIS, None, None, None, None),
        check_vma=False,
    )
```

```python
import functools
import types

import jax
import jax.numpy as jnp
from jax import lax
from jax.experimental import pallas as pl
from jax.experimental.pallas import tpu as pltpu
from jax.sharding import PartitionSpec as P


NBY = 4
NBZ = 4
AXIS = "boxes"

NFIELD = 5
VF = 5
C1 = 6
C2 = 7
NF = 8
ZU, ZD, YU, YD, XU, XD = 16, 256, 4, 4096, 1 << 28, 1 << 29
LOW = (1 << 24) - 1
EDGE = 13.0


def pairing(stride, extent, devices, odd):
    pairs = []
    for i in range(devices):
        c = i // stride % extent
        partner = ((c + 1) ^ 1) - 1 if odd else c ^ 1
        pairs.append((i, i + (partner % extent - c) * stride))
    return pairs


def lanes_of(shape):
    return lax.broadcasted_iota(jnp.int32, shape, len(shape) - 1)


def roll(value, shift, axis=1):
    if isinstance(shift, int):
        shift %= value.shape[axis]
        if shift == 0:
            return value
    else:
        shift &= value.shape[axis] - 1
    return pltpu.roll(value, shift, axis)


def place():
    me = lax.axis_index(AXIS)
    return me // (NBY * NBZ), me // NBZ % NBY, me % NBZ


def decode(code):
    qx = (code * 57) >> 9
    rest = code - 9 * qx
    qy = (rest * 11) >> 5
    qz = rest - 3 * qy
    word = 1 + jnp.where(qz == 2, ZU, 0) + jnp.where(qz == 0, ZD, 0)
    word = word * jnp.where(qy == 2, 1 + YU, jnp.where(qy == 0, 1 + YD, 1))
    return word | jnp.where(qx == 2, XU, jnp.where(qx == 0, XD, 0))


def on(word, bits):
    return (word & bits) == bits


ALL, OWN, RIM = "all", "own", "rim"


def ring_store(ref, lead, value, part=ALL):
    def put(first, rows):
        ref[(*lead, slice(first, first + rows.shape[0]), slice(None))] = rows

    if part == RIM:
        put(8, value[16:])
        put(ref.shape[-2] - 24, value[:16])
        put(0, value[8:16])
    else:
        put(8, value)
        if part == ALL:
            put(0, value[-8:])


def ring_load(ref, lead, step, part=ALL):
    n = ref.shape[-2] - 16

    def get(first, last):
        return ref[(*lead, slice(first + step, last + step), slice(None))]

    if part == OWN:
        return get(8, n)
    if part == RIM:
        spans = [(n - 8, n), (0, 16)] if step > 0 else [(n - 8, n + 8), (8, 16)]
    else:
        spans = [(8, n), (0, 8)] if step > 0 else [(8, n + 8)]
    return jnp.concatenate([get(*span) for span in spans], axis=0)


def cut(value, part):
    if part == ALL:
        return value
    n = value.shape[0] - 8
    return value[:n] if part == OWN else jnp.concatenate([value[n - 8 :], value[:8]], axis=0)


def pack_kernel(cx, cy, u_in, vf_in, mask_in, code_in, zp, z_a, z_b, u, vf, c, mask, code, sems):
    copies = [
        pltpu.make_async_copy(mask_in, mask, sems.at[0]),
        pltpu.make_async_copy(code_in, code, sems.at[1]),
        pltpu.make_async_copy(vf_in, vf, sems.at[2]),
    ]
    for f in range(NFIELD):
        rows = pl.ds(f * cx * cy, cx * cy)
        copies.append(pltpu.make_async_copy(u_in.at[rows, :], u.at[rows, :], sems.at[3 + f]))
    for copy in copies[:3] + copies[:2:-1]:
        copy.start()
    lane = lanes_of((cy, 128))
    slot = ((lane + 1) & 127) >> 1
    low_lane = (lane & 1) == 0
    copies[0].wait()
    copies[1].wait()
    for x in range(cx):
        rows = pl.ds(x * cy, cy)
        c[rows, :] = jnp.where(mask[rows, :] == 1, code[rows, :], 13).astype(jnp.float32)
    for g in (1, 0):
        acc = jnp.zeros((cy, 128), jnp.float32)
        for k in (3, 2, 1, 0):
            f = 4 * g + k
            if f <= VF:
                copies[3 + f if f < VF else 2].wait()
            for x in range(cx):
                m = cx * k + x
                rows = pl.ds(x * cy, cy)
                if f < NFIELD:
                    part = roll(u[pl.ds((f * cx + x) * cy, cy), :], 2 * m)
                elif f < C2:
                    part = roll((vf if f == VF else c)[rows, :], 2 * m)
                else:
                    part = jnp.where(low_lane, roll(c[rows, :], 2 * m - 1), roll(c[rows, :], 2 * m + 1))
                acc = jnp.where(slot == m, part, acc)
        zp[g * cy : (g + 1) * cy, :] = acc
        if g:
            second = acc
    high = jnp.where(low_lane, roll(second, 1), acc)
    low = jnp.where(low_lane, acc, roll(second, -1))
    odd = place()[2] % 2 == 1
    z_a[...] = jnp.where(odd, low, high)
    z_b[...] = jnp.where(odd, high, low)


def faces_kernel(cx, cy, two_x, u, vf, c, cw, y_a, y_b, *xs):
    bx, by, _ = place()
    for x in range(cx):
        cw[x + 2, 8 : 8 + cy, :] = decode(c[x * cy : (x + 1) * cy, :].astype(jnp.int32))

    def y_face(out, high):
        rim = jnp.where(high, cy - 1, 0)
        second = jnp.where(high, cy - 2, 1)

        def column(ref, base, row):
            return ref[pl.ds(base + row, cx, stride=cy), :]

        for f in range(NFIELD):
            out[f * cx : (f + 1) * cx, :] = column(u, f * cx * cy, rim)
        out[VF * cx : (VF + 1) * cx, :] = column(vf, 0, rim)
        out[C1 * cx : (C1 + 1) * cx, :] = column(c, 0, rim)
        out[C2 * cx : (C2 + 1) * cx, :] = column(c, 0, second)

    y_face(y_a, by % 2 == 0)
    y_face(y_b, by % 2 == 1)

    def x_face(out, high):
        rim = jnp.where(high, cx - 1, 0) * cy
        second = jnp.where(high, cx - 2, 1) * cy

        def rows(base, start):
            return pl.ds(pl.multiple_of(base + start, 8), cy)

        for f in range(NFIELD):
            out[f * cy : (f + 1) * cy, :] = u[rows(f * cx * cy, rim), :]
        out[VF * cy : (VF + 1) * cy, :] = vf[rows(0, rim), :]
        out[C1 * cy : (C1 + 1) * cy, :] = c[rows(0, rim), :]
        out[C2 * cy : (C2 + 1) * cy, :] = c[rows(0, second), :]

    x_face(xs[0], bx % 2 == 0)
    if two_x:
        x_face(xs[1], bx % 2 == 1)


def z_merge_kernel(cx, cy, r_a, r_b, zp, ya_in, yb_in, zh, y_a, y_b):
    _, by, bz = place()
    odd = bz % 2 == 1
    lane = lanes_of((cy, 128))
    low_lane = (lane & 1) == 0
    codes = (lane >= 63) & (lane <= 126)
    a, b = r_a[...], r_b[...]
    below, above = jnp.where(odd, a, b), jnp.where(odd, b, a)
    for g in range(2):
        edge = jnp.where(codes, EDGE, 0.0) if g else jnp.zeros((cy, 128), jnp.float32)
        low = jnp.where(bz > 0, below if g else roll(below, 1), edge)
        high = jnp.where(bz < NBZ - 1, above if g else roll(above, -1), edge)
        zh[g * cy : (g + 1) * cy, :] = jnp.where(low_lane, low, high)
    zh[2 * cy :, :] = zp[...]
    n = NF * cx

    def finish(out, main, high):
        out[:n, :] = main[...]
        rim = jnp.where(high, cy - 1, 0)
        second = jnp.where(high, cy - 2, 1)
        for g in range(4):
            out[n + 2 * g : n + 2 * g + 1, :] = zh[pl.ds(g * cy + rim, 1), :]
            out[n + 2 * g + 1 : n + 2 * g + 2, :] = zh[pl.ds(g * cy + second, 1), :]

    finish(y_a, ya_in, by % 2 == 0)
    finish(y_b, yb_in, by % 2 == 1)


def z_edge_rows(cx):
    n = NF * cx
    row = lax.broadcasted_iota(jnp.int32, (n + 8, 128), 0)
    lane = lanes_of((n + 8, 128))
    codes = ((row >= C1 * cx) & (row < n)) | ((row >= n) & ((row & 2) != 0) & (lane >= 63) & (lane <= 126))
    return jnp.where(codes, EDGE, 0.0)


def y_merge_kernel(cx, cy, two_x, ended, r_a, r_b, zh, *refs):
    copies = 2 if two_x else 1
    mains, (y_lo, y_hi), xs = refs[:copies], refs[copies : copies + 2], refs[copies + 2 :]
    bx, by, _ = place()
    odd = by % 2 == 1
    edge = z_edge_rows(cx)
    a, b = r_a[...], r_b[...]
    y_lo[...] = jnp.where(by > 0, jnp.where(odd, a, b), edge)
    y_hi[...] = jnp.where(by < NBY - 1, jnp.where(odd, b, a), edge)
    n = NF * cx

    def x_rim(out, main, high):
        rim = jnp.where(high, cx - 1, 0)
        second = jnp.where(high, cx - 2, 1)
        at = NF * cy
        out[:at, :] = main[...]
        lane = lanes_of((8, 128))
        spot = (lane - jnp.where(high, 2 * cx - 5, 2 * cx - 1)) & (2 * cx - 1)
        for half in range(2):
            tile = jnp.zeros((8, 128), jnp.float32)
            for t in range(cy // 8):
                for g in range(2):
                    start, row = 8 * t + 4 * g, (2 * half + g) * cy + 8 * t
                    tile = jnp.where((spot >= start) & (spot < start + 4), roll(zh[row : row + 8, :], start), tile)
            out[at : at + 8, :] = tile
            at += 8
        low, up = y_lo[n : n + 8, :], y_hi[n : n + 8, :]
        out[at : at + 8, :] = jnp.where(spot < 4, low, roll(up, 4))
        at += 8
        for y in (y_lo, y_hi):
            for f in range(NF):
                out[at : at + 1, :] = y[pl.ds(f * cx + rim, 1), :]
                at += 1
            for f in (C1, C2):
                out[at : at + 1, :] = y[pl.ds(f * cx + second, 1), :]
                at += 1
        out[at:, :] = jnp.zeros((out.shape[0] - at, 128), jnp.float32)

    x_rim(xs[0], mains[0], bx % 2 == 0)
    if two_x:
        x_rim(xs[1], mains[1], bx % 2 == 1)


def y_rows(r, x):
    cx = r.cx
    for f in range(C2):
        r.ht[f, x + 2, 0:1, :] = r.y_hi[pl.ds(f * cx + x, 1), :]
        r.ht[f, x + 2, 7:8, :] = r.y_lo[pl.ds(f * cx + x, 1), :]
    r.ht[C1, x + 2, 1:2, :] = r.y_hi[pl.ds(C2 * cx + x, 1), :]
    r.ht[C1, x + 2, 6:7, :] = r.y_lo[pl.ds(C2 * cx + x, 1), :]


def set_words(r, own, layer):
    both = jnp.concatenate([own, r.ht[C1, layer]], axis=0)
    ring_store(r.cw, (layer,), decode(both.astype(jnp.int32)))


def set_halo_words(r, layer):
    words = decode(r.ht[C1, layer].astype(jnp.int32))
    r.cw[layer, 0:8, :] = words
    r.cw[layer, 8 + r.cy : 16 + r.cy, :] = words


def z_halo(r, f, own):
    g, k = f // 4, f % 4
    return roll(own(g), 4 - 2 * r.cx * k)


def spread_counts(r, planes, slot):
    mid = up = down = jnp.zeros(r.lane.shape, jnp.int32)
    for word, bits in planes:
        v = 1 + ((word & YU) << 6) + ((word & YD) << 4)
        if bits is not None:
            v = jnp.where((word & bits) != 0, v, 0)
        mid = mid + v
        up = up + jnp.where((word & XU) != 0, v, 0)
        down = down + jnp.where((word & XD) != 0, v, 0)
    total = mid + roll(up, 2) + roll(down, -2)
    ring_store(r.tmp_i, (slot,), total, r.part)
    before, after = (ring_load(r.tmp_i, (slot,), step, r.part) for step in (-1, 1))
    return (total & 255) + ((before >> 8) & 255) + ((after >> 16) & 255)


def z_counts(r):
    rows = slice(0, r.lane.shape[0])
    outer1, outer2, inner1, inner2 = (decode(r.zf[f, rows].astype(jnp.int32)) for f in (C1, C2, NF + C1, NF + C2))
    r.ow[rows], r.iw[rows] = outer1, inner1
    planes = ((outer1, None), (outer2, r.inward), (inner1, r.outward)), ((inner1, None), (outer1, r.inward), (inner2, r.outward))
    for first, out, plane in zip((0, NF), (r.zw, r.zi), planes):
        inverse = 1.0 / spread_counts(r, plane, first // NF).astype(jnp.float32)
        weight = r.zf[first + VF, rows] * inverse
        out[0, rows] = weight
        for f in range(NFIELD):
            out[f + 1, rows] = weight * r.zf[first + f, rows]
    r.ci[rows] = inverse


def sum_x(mid, left, right):
    total = (mid & LOW) + jnp.where((left & XU) != 0, left & LOW, 0)
    return total + jnp.where((right & XD) != 0, right & LOW, 0)


def weigh(r, group, part):
    n = r.cy
    lane = lanes_of(({ALL: n + 8, OWN: n, RIM: 24}[part], 128))
    edge_lane = (lane == 0) | (lane == 127)
    totals = []
    for layer, _ in group:
        if part == RIM:
            total = sum_x(*(r.cw[layer + d, 8 + n : 16 + n, :] for d in (0, -1, 1)))
            r.xt[layer, 8 + n : 16 + n, :] = total
            r.xt[layer, 0:8, :] = total
        else:
            ring_store(r.xt, (layer,), sum_x(*(ring_load(r.cw, (layer + d,), 0, part) for d in (0, -1, 1))), part)
    for layer, _ in group:
        total, before, after = (ring_load(r.xt, (layer,), step, part) for step in (0, -1, 1))
        total = (total & 0x333) + ((before >> 2) & 0x333) + ((after >> 12) & 0x333)
        totals.append((total, roll(total, 1), roll(total, -1), roll(cut(r.ci[...], part), -2 * layer)))
    for (layer, field), (total, below, above, edge) in zip(group, totals):
        count = (total & 15) + ((below >> 4) & 15) + ((above >> 8) & 15)
        inverse = jnp.where(edge_lane, edge, 1.0 / count.astype(jnp.float32))
        if part == RIM:
            r.rc[layer, n - 8 :], r.rc[layer, 0:8] = inverse[:8], inverse[16:]
        else:
            r.rc[layer] = inverse[:n]
        ring_store(r.h0, (0, layer), field(VF, part) * inverse, part)
    for layer, field in group:
        weight = ring_load(r.h0, (0, layer), 0, part)
        for f in range(NFIELD + 1):
            w = weight
            if f:
                w = weight * field(f - 1, part)
                ring_store(r.h0, (f, layer), w, part)
            ring_store(r.hm, (f, layer), w + roll(w, 1), part)
            ring_store(r.hp, (f, layer), w + roll(w, -1), part)


def own_field(r, x, f, part):
    base = (f * r.cx + x if f < NFIELD else x) * r.cy
    ref = r.u if f < NFIELD else r.vf

    def rows(first, count):
        start = base + first
        return ref[pl.ds(start if isinstance(start, int) else pl.multiple_of(start, 8), count), :]

    if part == OWN:
        return rows(0, r.cy)
    if part == RIM:
        return jnp.concatenate([rows(r.cy - 8, 8), r.ht[f, x + 2], rows(0, 8)], axis=0)
    return jnp.concatenate([rows(0, r.cy), r.ht[f, x + 2]], axis=0)


def z_averages(r, deposit=True):
    tmp = r.tmp_f

    def pick(word, up, down, values):
        mid, plus, minus = values
        return mid + jnp.where((word & up) != 0, plus, jnp.where((word & down) != 0, minus, 0.0))

    rows = slice(0, r.lane.shape[0])
    sums, inner_sums = [], []
    for f in range(NFIELD + 1):
        both = r.zw[f, rows] + r.zi[f, rows]
        for i, value in enumerate((both, roll(both, -2), roll(both, 2))):
            ring_store(tmp, (3 * f + i,), value, r.part)
        around = [[ring_load(tmp, (3 * f + i,), step, r.part) for step in (0, 1, -1)] for i in range(3)]
        for word, out in ((r.ow[rows], sums), (r.iw[rows], inner_sums))[1 - deposit :]:
            out.append(pick(word, XU, XD, [pick(word, YU, YD, line) for line in around]))
    inverse = 1.0 / inner_sums[0]
    for f in range(NFIELD):
        r.ai[f, rows] = inner_sums[f + 1] * inverse
    if not deposit:
        return
    word = r.ow[...]
    inverse = 1.0 / sums[0]
    first = 3 * NFIELD + 3
    for f in range(NFIELD):
        v = jnp.where((word & r.inward) != 0, sums[f + 1] * inverse, 0.0)
        totals = []
        for i, bits in enumerate((0, XU, XD)):
            w = jnp.where((word & bits) != 0, v, 0.0) if bits else v
            slot = first + 6 * f + 2 * i
            ring_store(tmp, (slot,), jnp.where((word & YU) != 0, w, 0.0))
            ring_store(tmp, (slot + 1,), jnp.where((word & YD) != 0, w, 0.0))
            totals.append(w + ring_load(tmp, (slot,), -1) + ring_load(tmp, (slot + 1,), 1))
        r.dz[f] = totals[0] + roll(totals[1], 2) + roll(totals[2], -2)


def average(r, layer, rows_of=None):
    rows = r.cy + 8
    tiles = rows // 8
    lane = lanes_of((8, 128))
    for t in range(tiles) if rows_of is None else rows_of:
        at = 8 + 8 * t
        word = r.cw[layer, at : at + 8, :]
        zu, zd = (word & ZU) != 0, (word & ZD) != 0
        yu, yd = (word & YU) != 0, (word & YD) != 0
        xu, xd = (word & XU) != 0, (word & XD) != 0
        sums = []
        for f in range(NFIELD + 1):
            parts = []
            for d in (0, 1, -1):
                line = []
                for e in (0, 1, -1):
                    base = 0 if t == tiles - 1 and e == 1 else at
                    at_e = slice(base + e, base + e + 8)
                    v0, vm, vp = (h[f, layer + d, at_e, :] for h in (r.h0, r.hm, r.hp))
                    line.append(jnp.where(zu, vp, jnp.where(zd, vm, v0)))
                parts.append(line[0] + jnp.where(yu, line[1], jnp.where(yd, line[2], 0.0)))
            sums.append(parts[0] + jnp.where(xu, parts[1], jnp.where(xd, parts[2], 0.0)))
        inverse = 1.0 / sums[0]
        leaves = ((lane == 0) & zd) | ((lane == 127) & zu)
        for f in range(NFIELD):
            column = roll(r.ai[f, 8 * t : 8 * t + 8, :], -2 * layer)
            a = jnp.where(leaves, column, sums[f + 1] * inverse)
            r.av[f, layer, at : at + 8, :] = a
            if t == tiles - 1:
                r.av[f, layer, 0:8, :] = a


def redistribute(r, x, out):
    cy = r.cy
    layer = x + 2
    back = -2 * layer
    lane = lanes_of((8, 128))
    first_lane, last_lane = lane == 0, lane == 127
    for t in range(cy // 8):
        at = 8 + 8 * t
        base = [r.av[f, layer, at : at + 8, :] for f in range(NFIELD)]
        word = r.cw[layer, at : at + 8, :]
        up = [jnp.where((word & ZU) != 0, a, 0.0) for a in base]
        down = [jnp.where((word & ZD) != 0, a, 0.0) for a in base]
        for d in (0, 1, -1):
            for e in (0, 1, -1):
                if d == 0 and e == 0:
                    continue
                at_e = slice(at - e, at - e + 8)
                word = r.cw[layer - d, at_e, :]
                bits = (0, XU, XD)[d] | (0, YU, YD)[e]
                here = on(word, bits)
                here_up, here_down = on(word, bits | ZU), on(word, bits | ZD)
                for f in range(NFIELD):
                    a = r.av[f, layer - d, at_e, :]
                    base[f] = base[f] + jnp.where(here, a, 0.0)
                    up[f] = up[f] + jnp.where(here_up, a, 0.0)
                    down[f] = down[f] + jnp.where(here_down, a, 0.0)
        inverse = r.rc[layer, 8 * t : 8 * t + 8, :]
        for f in range(NFIELD):
            halo = roll(r.dz[f, 8 * t : 8 * t + 8, :], back)
            total = base[f] + jnp.where(first_lane, halo, roll(up[f], 1))
            total = total + jnp.where(last_lane, halo, roll(down[f], -1))
            out[f, pl.ds(pl.multiple_of(x * cy + 8 * t, 8), 8), :] = total * inverse


def common(r, part):
    r.part = part
    r.lane = lanes_of((r.cy + (8 if part == ALL else 0), 128))
    even = (r.lane & 1) == 0
    r.inward = jnp.where(even, ZU, ZD)
    r.outward = jnp.where(even, ZD, ZU)


def z_fields(r, rows, own):
    for f in range(2 * NF):
        value = z_halo(r, f, own)
        if r.outside is not None:
            value = jnp.where(r.outside[: value.shape[0]], EDGE if f % NF >= C1 else 0.0, value)
        r.zf[f, rows] = value


KEPT = ("cw", "zf", "xt", "h0", "hm", "hp", "rc", "av")
SCRATCH = ("ht", "hz", "ow", "iw", "tmp_i", "tmp_f", "ci", "zw", "zi", "ai", "dz")


def plan(cx, nbx, bx):
    if nbx == 2:
        high = bx == 0

        def at(j):
            return jnp.where(high, j + 1, cx + 2 - j)

        return types.SimpleNamespace(
            at=at,
            inner_weigh=[at(j) for j in range(1, cx)],
            inner_average=(1, cx - 2),
            inner_spread=(1, cx - 3),
            outer_weigh=[at(cx)],
            outer_average=[(cx - 1, 3)],
            outer_spread=[(cx - 2, 3)],
            inner_rows=(jnp.where(high, 0, 3), cx - 3),
        )
    return types.SimpleNamespace(
        at=lambda j: j + 1,
        inner_weigh=range(3, cx + 1),
        inner_average=(3, cx - 4),
        inner_spread=(4, cx - 6),
        outer_weigh=[2, cx + 1],
        outer_average=[(0, 3), (cx - 1, 3)],
        outer_spread=[(1, 3), (cx - 2, 3)],
        inner_rows=(3, cx - 6),
    )


def x_lanes(r, high):
    below = (r.lane == 127) | (r.lane <= 2)
    above = (r.lane >= 2 * r.cx + 3) & (r.lane <= 2 * r.cx + 6)
    if isinstance(high, bool):
        return above if high else below
    return (above & high) | (below & jnp.logical_not(high))


def each(span, step):
    def body(j, _):
        step(j)
        return 0

    lax.fori_loop(span[0], span[0] + span[1], body, 0)


def set_outside(r, nbx, bx):
    r.outside = x_lanes(r, bx > 0) if nbx == 2 else None


def early_kernel(cx, cy, nbx, *refs):
    names = ("u", "vf", "zh", "cw_in", *KEPT, "ended", *SCRATCH)
    r = types.SimpleNamespace(cx=cx, cy=cy, **dict(zip(names, refs)))
    common(r, OWN)
    bx, _, _ = place()
    todo = plan(cx, nbx, bx)
    set_outside(r, nbx, bx)
    z_fields(r, slice(0, cy), lambda g: r.zh[g * cy : (g + 1) * cy, :])
    if nbx == 2:
        edge = todo.at(0)
        ring_store(r.cw, (edge,), jnp.ones((cy + 8, 128), jnp.int32))
        for f in range(NFIELD + 1):
            for h in (r.h0, r.hm, r.hp):
                ring_store(h, (f, edge), jnp.zeros((cy + 8, 128), jnp.float32))
    z_counts(r)
    weigh(r, [(layer, functools.partial(own_field, r, layer - 2)) for layer in todo.inner_weigh], OWN)
    z_averages(r, deposit=False)
    each(todo.inner_average, lambda j: average(r, todo.at(j), range(1, cy // 8 - 1)))
    r.ended[...] = r.ci[0:8]


def inner_kernel(cx, cy, nbx, *refs):
    kept_in = len(KEPT)
    names = ("u", "vf", "y_lo", "y_hi")
    rest = refs[len(names) + kept_in :]
    r = types.SimpleNamespace(cx=cx, cy=cy, **dict(zip(names, refs)))
    r.__dict__.update(zip((*KEPT, "res", *SCRATCH), rest))
    common(r, ALL)
    bx, _, _ = place()
    todo = plan(cx, nbx, bx)
    set_outside(r, nbx, bx)
    r.ht[...] = jnp.zeros(r.ht.shape, jnp.float32)
    for x in range(cx):
        y_rows(r, x)
        set_halo_words(r, x + 2)
    n = NF * cx
    for g in range(4):
        for i, row in enumerate((0, 1)):
            r.hz[g, row : row + 1, :] = r.y_hi[n + 2 * g + i : n + 2 * g + i + 1, :]
            r.hz[g, 7 - row : 8 - row, :] = r.y_lo[n + 2 * g + i : n + 2 * g + i + 1, :]
    z_fields(r, slice(cy, cy + 8), lambda g: r.hz[g])
    z_counts(r)
    weigh(r, [(layer, functools.partial(own_field, r, layer - 2)) for layer in todo.inner_weigh], RIM)
    z_averages(r)
    each(todo.inner_average, lambda j: average(r, todo.at(j), (0, cy // 8 - 1, cy // 8)))
    each(todo.inner_spread, lambda j: redistribute(r, todo.at(j) - 2, r.res))


def outer_kernel(cx, cy, nbx, *refs):
    kept_in = len(KEPT)
    names = ("u", "vf", "y_lo", "y_hi", "res", "xa", "xb")
    ins = refs[: len(names)]
    rest = refs[len(names) + kept_in :]
    r = types.SimpleNamespace(cx=cx, cy=cy, **dict(zip(names, ins)))
    r.__dict__.update(zip(("out", *KEPT, *SCRATCH, "rim", "sems"), rest))
    bx, _, _ = place()
    todo = plan(cx, nbx, bx)

    def copy(src, first, count, semaphore):
        part = pl.ds(pl.multiple_of(first * cy, 8), count * cy)
        return pltpu.make_async_copy(src.at[:, part, :], r.out.at[:, part, :], r.sems.at[semaphore])

    each((0, 2), lambda i: pl.when(i == 0)(lambda: copy(r.res, *todo.inner_rows, 0).start()))

    def finish_layer(j, first, turn):
        x = todo.at(j) - 2
        redistribute(r, x, r.rim)
        copy(r.rim, x, 1, turn + j - first).start()

    common(r, ALL)
    x_odd = bx % 2 == 1

    if nbx == 2:
        sides = [(bx == 0, True, lambda first, count: r.xa[first : first + count, :])]
    else:

        def message(high):
            def rows(first, count):
                a, b = r.xa[first : first + count, :], r.xb[first : first + count, :]
                return jnp.where(x_odd, b, a) if high else jnp.where(x_odd, a, b)

            return rows

        sides = [(False, bx > 0, message(False)), (True, bx < nbx - 1, message(True))]

    def choose(high, a, b):
        return (a if high else b) if isinstance(high, bool) else jnp.where(high, a, b)

    def present_or(present, value, edge):
        return value if present is True else jnp.where(present, value, edge)

    zrow = NF * cy
    edges = zrow + 16
    halo = []
    for high, present, part in sides:
        layer, second, own = (choose(high, a, b) for a, b in ((cx + 2, 1), (cx + 3, 0), (cx - 1, 0)))
        y_rows(r, own)

        def raw(f, present=present, part=part):
            return present_or(present, part(f * cy, cy), EDGE if f >= C1 else 0.0)

        for y, row1, row2 in ((0, 7, 6), (1, 0, 1)):
            base = edges + 8 + 10 * y

            def rim(i, edge, base=base, present=present, part=part):
                return present_or(present, part(base + i, 1), edge)

            for f in range(C1):
                r.ht[f, layer, row1 : row1 + 1, :] = rim(f, 0.0)
            r.ht[C1, layer, row1 : row1 + 1, :] = rim(C1, EDGE)
            r.ht[C1, layer, row2 : row2 + 1, :] = rim(C2, EDGE)
            r.ht[C1, second, row1 : row1 + 1, :] = rim(NF, EDGE)
            r.ht[C1, second, row2 : row2 + 1, :] = rim(NF + 1, EDGE)
        set_words(r, raw(C1), layer)
        set_words(r, raw(C2), second)
        halo.append((layer, lambda f, part, raw=raw, layer=layer: jnp.concatenate([raw(f), r.ht[f, layer]], axis=0)))

        edge_rows = part(edges, 8)
        upper_rows = roll(edge_rows, -4)
        for g in range(4):
            for i, row in enumerate((0, 1)):
                at = 2 * g + i
                r.hz[g, row : row + 1, :] = upper_rows[at : at + 1]
                r.hz[g, 7 - row : 8 - row, :] = edge_rows[at : at + 1]
        lanes = x_lanes(r, high)
        for f in range(2 * NF):
            g, k = f // 4, f % 4
            shift = 4 - 2 * cx * k + choose(high, 2 * cx, -2 * cx)
            tile = part(zrow + 8 * (g // 2), 8)
            tiles = [roll(tile, shift - 8 * t - 4 * (g % 2)) for t in range(cy // 8)]
            value = jnp.concatenate([*tiles, roll(r.hz[g], shift)], axis=0)
            r.zf[f] = jnp.where(lanes, present_or(present, value, EDGE if f % NF >= C1 else 0.0), r.zf[f])
    z_counts(r)
    weigh(r, [(layer, functools.partial(own_field, r, layer - 2)) for layer in todo.outer_weigh] + halo, ALL)
    z_averages(r)
    for span in todo.outer_average:
        each(span, lambda j: average(r, todo.at(j)))
    turn = 1
    for first, count in todo.outer_spread:
        each((first, count), lambda j: finish_layer(j, first, turn))
        turn += count
    turn = 1
    for first, count in todo.outer_spread:
        for j in range(first, first + count):
            copy(r.rim, todo.at(j) - 2, 1, turn).wait()
            turn += 1
    copy(r.res, *todo.inner_rows, 0).wait()


def call(kernel, ins, outs, scratch=(), grant=8, flops=0, **kwargs):
    return pl.pallas_call(
        kernel,
        in_specs=ins,
        out_specs=tuple(pl.BlockSpec(memory_space=o.memory_space) for o in outs),
        out_shape=tuple(outs),
        scratch_shapes=scratch,
        cost_estimate=pl.CostEstimate(flops=flops, transcendentals=0, bytes_accessed=0),
        compiler_params=pltpu.CompilerParams(vmem_limit_bytes=grant << 20),
        **kwargs,
    )


def per_device(conserved, volume_fraction, cut_mask, merge_code):
    _, cx, cy, cz = cut_mask.shape
    devices = lax.axis_size(AXIS)
    nbx = devices // (NBY * NBZ)
    two_x = nbx > 2
    cells = cx * cy
    u = conserved.reshape(NFIELD * cells, cz)
    vf, mask, code = (a.reshape(cells, cz) for a in (volume_fraction, cut_mask, merge_code))
    f32, i32 = jnp.float32, jnp.int32
    on_chip, far = pl.BlockSpec(memory_space=pltpu.VMEM), pl.BlockSpec(memory_space=pltpu.HBM)

    def vmem(*shape, dtype=f32):
        return pltpu.VMEM((*shape, cz), dtype)

    def swap(value, stride, extent, odd):
        return lax.ppermute(value, AXIS, pairing(stride, extent, devices, odd))

    n = NF * cx
    copies = 2 if two_x else 1
    zp, za, zb, u, vf, c = call(
        functools.partial(pack_kernel, cx, cy),
        [far] * 4,
        [vmem(2 * cy), vmem(cy), vmem(cy), vmem(NFIELD * cells), vmem(cells), vmem(cells)],
        [vmem(cells, dtype=i32), vmem(cells, dtype=i32), pltpu.SemaphoreType.DMA((3 + NFIELD,))],
    )(*(pltpu.with_memory_space_constraint(a, pltpu.HBM) for a in (u, vf, mask, code)))
    za, zb = swap(za, 1, NBZ, False), swap(zb, 1, NBZ, True)
    rows, ring, layers = cy + 8, cy + 24, cx + 4
    cw, ya, yb, *xs = call(
        functools.partial(faces_kernel, cx, cy, two_x),
        [on_chip] * 3,
        [vmem(layers, ring, dtype=i32), vmem(n), vmem(n)] + [vmem(NF * cy)] * copies,
        flops=1 << 20,
    )(u, vf, c)
    zh, ya, yb = call(
        functools.partial(z_merge_kernel, cx, cy), [on_chip] * 5, [vmem(4 * cy), vmem(n + 8), vmem(n + 8)]
    )(za, zb, zp, ya, yb)
    kept = [
        vmem(layers, ring, dtype=i32),
        vmem(2 * NF, rows),
        vmem(layers, ring, dtype=i32),
        vmem(NFIELD + 1, layers, ring),
        vmem(NFIELD + 1, layers, ring),
        vmem(NFIELD + 1, layers, ring),
        vmem(layers, cy),
        vmem(NFIELD, layers, ring),
    ]
    scratch = [
        vmem(C2, layers, 8),
        vmem(4, 8),
        vmem(rows, dtype=i32),
        vmem(rows, dtype=i32),
        vmem(2, ring, dtype=i32),
        vmem(9 * NFIELD + 3, ring),
        vmem(rows),
        vmem(NFIELD + 1, rows),
        vmem(NFIELD + 1, rows),
        vmem(NFIELD, rows),
        vmem(NFIELD, rows),
    ]
    yb = swap(yb, NBZ, NBY, True)
    ya = swap(ya, NBZ, NBY, False)
    *state, ended = call(
        functools.partial(early_kernel, cx, cy, nbx),
        [on_chip] * 4,
        kept + [vmem(8)],
        scratch,
        flops=1 << 24,
        input_output_aliases={3: 0},
    )(u, vf, zh, cw)
    y_lo, y_hi, *xs = call(
        functools.partial(y_merge_kernel, cx, cy, two_x),
        [on_chip] * (4 + copies),
        [vmem(n + 8), vmem(n + 8)] + [vmem(NF * cy + 48)] * copies,
    )(ended, ya, yb, zh, *xs)
    xs = [swap(x, NBY * NBZ, nbx, odd) for odd, x in enumerate(xs)]
    xa, xb = xs if two_x else xs * 2

    *state, res = call(
        functools.partial(inner_kernel, cx, cy, nbx),
        [on_chip] * (4 + len(kept)),
        kept + [vmem(NFIELD, cells)],
        scratch,
        flops=1 << 26,
        input_output_aliases={4 + i: i for i in range(len(kept))},
    )(u, vf, y_lo, y_hi, *state)
    first = 7
    out, *_ = call(
        functools.partial(outer_kernel, cx, cy, nbx),
        [on_chip] * (first + len(kept)),
        [pltpu.HBM((NFIELD, cells, cz), f32)] + kept,
        scratch + [vmem(NFIELD, cells), pltpu.SemaphoreType.DMA((7,))],
        flops=1 << 25,
        input_output_aliases={first + i: 1 + i for i in range(len(kept))},
    )(u, vf, y_lo, y_hi, res, xa, xb, *state)
    return out.reshape(conserved.shape)


def solution(mesh):
    return jax.shard_map(
        per_device,
        mesh=mesh,
        in_specs=(
            P(AXIS, None, None, None, None),
            P(AXIS, None, None, None),
            P(AXIS, None, None, None),
            P(AXIS, None, None, None),
        ),
        out_specs=P(AXIS, None, None, None, None),
        check_vma=False,
    )
```
